256 devices in a mesh: row: 16 (over x_lo, y, core), col: 16 (over z, x_hi).
Axes of the slice: x: 4 (x_hi: 2, x_lo: 2; x = x_hi * 2 + x_lo), y: 4, z: 8, core: 2. Of those that a mesh axis runs over, the one named last changes fastest.
Arguments:
- labels: int32 [16, 512, 2048], P(None, 'row', 'col'), may hold values from 0 to 11
- pressure: float32 [16, 512, 2048], P(None, 'row', 'col'), may hold values from -6 to 6
- velocity_x: float32 [16, 512, 2048], P(None, 'row', 'col'), may hold values from -6 to 6
- velocity_y: float32 [16, 512, 2048], P(None, 'row', 'col'), may hold values from -6 to 6
- velocity_z: float32 [16, 512, 2048], P(None, 'row', 'col'), may hold values from -6 to 6
- speed_table: float32 [12], replicated, may hold values from 0.8 to 2
- density_table: float32 [12], replicated, may hold values from 0.9 to 1.9
- filter_taps: float32 [33], replicated, may hold values from -0.2 to 0.8, as said below
- layer_width: int32 [4], replicated, may hold values from 10 to 40
Outputs:
- pressure_next: float32 [16, 512, 2048], P(None, 'row', 'col')
- velocity_x_next: float32 [16, 512, 2048], P(None, 'row', 'col')
- velocity_y_next: float32 [16, 512, 2048], P(None, 'row', 'col')
- velocity_z_next: float32 [16, 512, 2048], P(None, 'row', 'col')
The draws below stay inside these ranges and needn't reach their ends.
Inputs may be any that keep to these rules, and one draw needn't show every extreme that they name: `filter_taps`: tap k weighs the cell k - 16 positions away.
All inputs are finite; a program needn't handle non-finite values.
Results may differ from the reference program's by a relative error of at most 0.000068.
Values sent between devices are 32-bit elements; how exact they have to be, the bound alone decides.
A program may use at most 64 MiB of HBM per device.

```python
import math
import jax
import jax.numpy as jnp

NZ = 16
TAPS = 33
LABELS = 12
NX = 2048
NY = 512


def draw_filter_taps(key, part):
    offsets = jnp.arange(TAPS, dtype=jnp.float32) - TAPS // 2
    cutoff = 0.3
    lowpass = 2.0 * cutoff * jnp.sinc(2.0 * cutoff * offsets)
    tapering = 0.42 + 0.5 * jnp.cos(math.pi * offsets / (TAPS // 2 + 1)) + 0.08 * jnp.cos(2.0 * math.pi * offsets / (TAPS // 2 + 1))
    jitter = jax.random.uniform(key, (TAPS,), jnp.float32, -0.25, 0.25)
    return (lowpass * tapering * (1.0 + jitter)).astype(jnp.float32)


def place_ends(array, own_key, low, high):
    longest = array.shape.index(max(array.shape))
    spots = []
    for shift in (0, 1):
        where = [jax.random.randint(jax.random.fold_in(own_key, axis), (), 0, length) for axis, length in enumerate(array.shape)]
        where[longest] = (where[longest] + shift) % array.shape[longest]
        spots.append(tuple(where))
    return array.at[spots[0]].set(low).at[spots[1]].set(high)


def steps_of(key, extent, shards, least, top_value):
    def one(dim, parts):
        heights = jax.random.uniform(jax.random.fold_in(jax.random.fold_in(key, 6), dim), (parts,), jnp.float32, least / len(shards), top_value / len(shards))
        return jnp.repeat(jnp.exp(heights), extent[dim] // parts).reshape((-1,) + (1,) * (len(extent) - dim - 1))

    factor_of = one(*shards[0])
    for cut in shards[1:]:
        factor_of = factor_of * one(*cut)
    return factor_of


def scatter_about(own_key, shape, width, most, cuts=(), kind=jnp.bfloat16):
    values = jax.random.normal(own_key, shape, jnp.float32) * width
    if len(cuts) > 0:
        values = steps_of(own_key, shape, cuts, -0.22, 0.18) * values
    return jnp.clip(values, min=-most, max=most).astype(kind)


def setup_inputs(seed: int = 0) -> dict:
    arg_keys = jax.random.split(jax.random.key(seed), 10)
    labels = place_ends(jax.random.randint(arg_keys[0], (NZ, NY, NX), 0, LABELS), jax.random.fold_in(arg_keys[0], 1), 0, LABELS - 1).astype(jnp.int32)
    pressure = scatter_about(arg_keys[1], (NZ, NY, NX), 1.0, 6.0, ((1, 16), (2, 16)), jnp.float32)
    velocity_x = scatter_about(arg_keys[2], (NZ, NY, NX), 1.0, 6.0, ((1, 16), (2, 16)), jnp.float32)
    velocity_y = scatter_about(arg_keys[3], (NZ, NY, NX), 1.0, 6.0, ((1, 16), (2, 16)), jnp.float32)
    velocity_z = scatter_about(arg_keys[4], (NZ, NY, NX), 1.0, 6.0, ((1, 16), (2, 16)), jnp.float32)
    speed_table = jnp.clip(jnp.exp(jax.random.uniform(arg_keys[5], (LABELS,), jnp.float32, math.log(0.8), math.log(2.0))), 0.8, 2.0)
    density_table = jnp.clip(jax.random.uniform(arg_keys[6], (LABELS,), jnp.float32, 0.9, 1.9), 0.9, 1.9)
    filter_taps = draw_filter_taps(jax.random.fold_in(arg_keys[9], 71), 0)
    layer_width = place_ends(jax.random.randint(arg_keys[8], (4,), 10, 41), jax.random.fold_in(arg_keys[8], 1), 10, 40).astype(jnp.int32)
    return {"labels": labels, "pressure": pressure, "velocity_x": velocity_x, "velocity_y": velocity_y, "velocity_z": velocity_z, "speed_table": speed_table, "density_table": density_table, "filter_taps": filter_taps, "layer_width": layer_width}


time_step = 0.15
reference_speed = 2.0
absorption = 6.0

def smooth(field, filter_taps, axis_id):
    reach = filter_taps.shape[0] // 2
    summed = jnp.zeros(field.shape, jnp.float32)
    for tap_id in range(filter_taps.shape[0]):
        summed = summed + filter_taps[tap_id] * jnp.roll(field, reach - tap_id, axis=axis_id)
    return summed

def wavenumbers(length):
    indices = jnp.arange(length, dtype=jnp.int32)
    signed = jnp.where(indices < length // 2, indices, indices - length)
    return signed.astype(jnp.float32) * (2.0 * math.pi / length)

def absorber(length, low_width, high_width):
    position = jnp.arange(length, dtype=jnp.int32)
    low_part = jnp.maximum(low_width - position, 0).astype(jnp.float32) / low_width.astype(jnp.float32)
    high_part = jnp.maximum(position - (length - 1 - high_width), 0).astype(jnp.float32) / high_width.astype(jnp.float32)
    damping = absorption * reference_speed * (low_part ** 4 + high_part ** 4)
    return jnp.exp(-0.5 * time_step * damping)

def reference(labels, pressure, velocity_x, velocity_y, velocity_z, speed_table, density_table, filter_taps, layer_width):
    buoyancy = (1.0 / density_table)[labels]
    modulus = (density_table * speed_table * speed_table)[labels]
    buoyancy = smooth(smooth(buoyancy, filter_taps, 2), filter_taps, 1)
    modulus = smooth(smooth(modulus, filter_taps, 2), filter_taps, 1)
    wave_x = wavenumbers(NX)[None, None, :]
    wave_y = wavenumbers(NY)[None, :, None]
    wave_z = wavenumbers(NZ)[:, None, None]
    correction = jnp.sinc(reference_speed * time_step * jnp.sqrt(wave_x * wave_x + wave_y * wave_y + wave_z * wave_z) / (2.0 * math.pi))
    damp_x = absorber(NX, layer_width[0], layer_width[1])[None, None, :]
    damp_y = absorber(NY, layer_width[2], layer_width[3])[None, :, None]
    spectrum = jnp.fft.fftn(pressure)

    def gradient(wavenum):
        return jnp.real(jnp.fft.ifftn(1j * wavenum * correction * jnp.exp(0.5j * wavenum) * spectrum))

    def inward(wavenum, field):
        return jnp.real(jnp.fft.ifftn(1j * wavenum * correction * jnp.exp(-0.5j * wavenum) * jnp.fft.fftn(field)))
    next_x = damp_x * (damp_x * velocity_x - time_step * buoyancy * gradient(wave_x))
    next_y = damp_y * (damp_y * velocity_y - time_step * buoyancy * gradient(wave_y))
    next_z = velocity_z - time_step * buoyancy * gradient(wave_z)
    divergence = inward(wave_x, next_x) + inward(wave_y, next_y) + inward(wave_z, next_z)
    damp_both = damp_x * damp_y
    pressure_next = damp_both * (damp_both * pressure - time_step * modulus * divergence)
    return (pressure_next, next_x, next_y, next_z)
```

```python
import functools
import math

import jax
import jax.numpy as jnp
import numpy as np
from jax import lax
from jax.experimental import pallas as pl
from jax.experimental.pallas import tpu as pltpu
from jax.sharding import PartitionSpec as P

time_step = 0.15
reference_speed = 2.0
absorption = 6.0
highest = lax.Precision.HIGHEST
MESH = pl.DeviceIdType.MESH

NZ, NY, NX = 16, 512, 2048
ROWS, COLS = 16, 16
YB, XB = NY // ROWS, NX // COLS
SLOTS = 8
f32, bf16 = jnp.float32, jnp.bfloat16


def split_table(table):
    high = table.astype(np.float32).astype(bf16)
    low = (table - high.astype(np.float64)).astype(np.float32).astype(bf16)
    return np.stack([high, low])


def row_tables():
    slot = np.arange(NY // 2)
    y = np.arange(NY)
    angle = 2.0 * np.pi * ((slot[:, None] * y[None, :]) % NY) / NY
    real, imag = np.cos(angle), -np.sin(angle)
    imag[0] = np.where(y % 2 == 0, 1.0, -1.0)
    order = lambda t: t.reshape(NY // 2 // SLOTS, SLOTS, NY)
    forward = np.stack([order(real), order(imag)], axis=1).reshape(NY, NY)
    weight = np.where(slot == 0, 1.0, 2.0) / NY
    inverse = np.stack([order(real * weight[:, None]), order(imag * weight[:, None])], axis=1)
    inverse = inverse.reshape(NY, NY).T
    wave = 2.0 * np.pi * slot / NY
    same = -wave * np.sin(0.5 * wave)
    cross = wave * np.cos(0.5 * wave)
    same_imag = same.copy()
    same_imag[0] = -np.pi
    wide = lambda v: np.broadcast_to(v.reshape(-1, SLOTS, 1), (NY // 2 // SLOTS, SLOTS, XB))
    derivative = np.stack([wide(same), wide(same_imag), wide(cross)]).astype(np.float32)
    return split_table(forward), split_table(inverse), derivative


def column_tables():
    x = np.arange(XB)
    angle = 2.0 * np.pi * ((x[:, None] * x[None, :]) % XB) / XB
    c, s = np.cos(angle), np.sin(angle)
    forward = np.block([[c, -s], [s, c]])
    inverse = np.block([[c, s], [-s, c]]) / NX
    kc = np.arange(COLS)
    twist = 2.0 * np.pi * (kc[:, None] * x[None, :]) / NX
    index = kc[:, None] + COLS * x[None, :]
    wave = 2.0 * np.pi * np.where(index < NX // 2, index, index - NX) / NX
    same = wave * np.sin(0.5 * wave)
    cross = wave * np.cos(0.5 * wave)
    small = np.stack([np.cos(twist), np.sin(twist), wave * wave, same, cross]).astype(np.float32)
    return split_table(forward), split_table(inverse), small


def scaled(value, factor):
    if abs(factor - 1.0) < 1e-12:
        return value
    if abs(factor + 1.0) < 1e-12:
        return -value
    return value * np.float32(factor)


def weighted(terms):
    total = None
    for value, factor in terms:
        if abs(factor) < 1e-12:
            continue
        if total is None:
            total = scaled(value, factor)
        elif abs(factor + 1.0) < 1e-12:
            total = total - value
        else:
            total = total + scaled(value, factor)
    return total


def cos16(n):
    return math.cos(2.0 * math.pi * (n % 16) / 16)


def sin16(n):
    return math.sin(2.0 * math.pi * (n % 16) / 16)


def depth_forward(p):
    even = [p[0]] + [p[n] + p[16 - n] for n in range(1, 8)] + [p[8]]
    odd = [None] + [p[n] - p[16 - n] for n in range(1, 8)]
    plus = [even[n] + even[8 - n] for n in range(4)] + [even[4]]
    minus = [even[n] - even[8 - n] for n in range(4)]
    odd_plus = [None] + [odd[n] + odd[8 - n] for n in range(1, 4)] + [odd[4]]
    odd_minus = [None] + [odd[n] - odd[8 - n] for n in range(1, 4)]

    def real_of(k):
        side = plus if k % 2 == 0 else minus
        return weighted([(side[n], cos16(k * n)) for n in range(len(side))])

    def imag_of(k):
        if k % 2 == 0:
            return weighted([(odd_minus[n], -sin16(k * n)) for n in range(1, 4)])
        return weighted([(odd_plus[n], -sin16(k * n)) for n in range(1, 5)])

    out = [real_of(0), real_of(8)]
    for k in range(1, 8):
        out += [real_of(k), imag_of(k)]
    return out


def depth_inverse(m):
    real = [m[0]] + [m[2 * k] for k in range(1, 8)] + [m[1]]
    imag = [None] + [m[2 * k + 1] for k in range(1, 8)]
    weight = [1.0 / 16] + [2.0 / 16] * 7 + [1.0 / 16]

    def terms(values, ids, n, wave):
        return weighted([(values[k], weight[k] * wave(k * n)) for k in ids])

    out = [None] * 16
    for n in range(0, 5):
        ce = terms(real, range(0, 9, 2), n, cos16)
        co = terms(real, range(1, 9, 2), n, cos16)
        so = terms(imag, range(1, 8, 2), n, lambda v: -sin16(v))
        se = terms(imag, range(2, 8, 2), n, lambda v: -sin16(v))
        near = ce if co is None else ce + co
        far = ce if co is None else ce - co
        if n == 0:
            out[0], out[8] = near, far
            continue
        if se is None:
            d_near, d_far = so, so
        else:
            d_near, d_far = so + se, so - se
        out[n], out[16 - n] = near + d_near, near - d_near
        if n < 4:
            out[8 - n], out[8 + n] = far + d_far, far - d_far
    return out


def depth_derivative(m, sign):
    out = [jnp.zeros_like(m[0]), m[1] * np.float32(-sign * math.pi)]
    for k in range(1, 8):
        wave = 2.0 * math.pi * k / 16
        a = np.float32(-sign * wave * math.sin(0.5 * wave))
        b = np.float32(wave * math.cos(0.5 * wave))
        out += [m[2 * k] * a - m[2 * k + 1] * b, m[2 * k + 1] * a + m[2 * k] * b]
    return out


def short_transform(values, sign):
    count = len(values)
    if count == 1:
        return values
    even = short_transform(values[0::2], sign)
    odd = short_transform(values[1::2], sign)
    out = [None] * count
    for k in range(count // 2):
        angle = sign * 2.0 * math.pi * k / count
        c, s = math.cos(angle), math.sin(angle)
        re, im = odd[k]
        if k == 0:
            tr, ti = re, im
        elif abs(c) < 1e-9:
            tr, ti = (-im, re) if s > 0 else (im, -re)
        elif abs(abs(c) - abs(s)) < 1e-9:
            h = np.float32(abs(c))
            cs, ss = (1 if c > 0 else -1), (1 if s > 0 else -1)
            first = re if cs > 0 else -re
            tr = (first - im if ss > 0 else first + im) * h
            second = im if cs > 0 else -im
            ti = (second + re if ss > 0 else second - re) * h
        else:
            tr = re * np.float32(c) - im * np.float32(s)
            ti = re * np.float32(s) + im * np.float32(c)
        er, ei = even[k]
        out[k] = (er + tr, ei + ti)
        out[k + count // 2] = (er - tr, ei - ti)
    return out


def halves(value):
    high = value.astype(bf16)
    low = (value - high.astype(f32)).astype(bf16)
    return high, low


def mm(a, b):
    return jnp.dot(a, b, preferred_element_type=f32)


def step_kernel(
    p_ref, vx_ref, vy_ref, vz_ref, b_ref, m_ref, dx_ref, dy_ref,
    fy_ref, gy_ref, yd_ref, wx_ref, ux_ref, xt_ref,
    po_ref, vxo_ref, vyo_ref, vzo_ref,
    row_out, row_in, col_out, col_in, bcol_out, bcol_in, brow_out, brow_in,
    kappa, xb, xs,
    send_sem, recv_sem,
):
    r, c = lax.axis_index("row"), lax.axis_index("col")
    j, h = r // 2, r % 2
    q = h * COLS + c

    barrier = pltpu.get_barrier_semaphore()

    def greet_row(i, carry):
        pl.semaphore_signal(barrier, inc=1, device_id=((r + i) % ROWS, c), device_id_type=MESH)
        return carry

    def greet_plane(i, carry):
        t = (q + i) % (2 * COLS)
        pl.semaphore_signal(
            barrier, inc=1, device_id=(2 * j + t // COLS, t % COLS), device_id_type=MESH
        )
        return carry

    lax.fori_loop(1, ROWS, greet_row, 0)
    lax.fori_loop(1, 2 * COLS, greet_plane, 0)

    def row_copy(src, dst, sem, i):
        t = (r + i) % ROWS
        return pltpu.make_async_remote_copy(
            src_ref=src.at[t], dst_ref=dst.at[r], send_sem=send_sem.at[sem],
            recv_sem=recv_sem.at[sem], device_id=(t, c), device_id_type=MESH,
        )

    def plane_copy(src, dst, sem, i):
        t = (q + i) % (2 * COLS)
        return pltpu.make_async_remote_copy(
            src_ref=src.at[t], dst_ref=dst.at[q], send_sem=send_sem.at[sem],
            recv_sem=recv_sem.at[sem], device_id=(2 * j + t // COLS, t % COLS),
            device_id_type=MESH,
        )

    def start_all(copy_of, src, dst, sem, count, own):
        def body(i, carry):
            copy_of(src, dst, sem, i).start()
            return carry

        lax.fori_loop(1, count, body, 0)
        dst[own] = src[own]

    def whole(src, dst, sem, count):
        span = pl.ds(0, count - 1)
        return pltpu.make_async_remote_copy(
            src_ref=src.at[span], dst_ref=dst.at[span], send_sem=send_sem.at[sem],
            recv_sem=recv_sem.at[sem], device_id=((r + 1) % ROWS, c), device_id_type=MESH,
        )

    def send_row(f):
        start_all(row_copy, row_out.at[f], row_in.at[f], f, ROWS, r)

    def send_col(f):
        start_all(plane_copy, col_out.at[f], col_in.at[f], 4 + f, 2 * COLS, q)

    def send_bcol(f):
        start_all(plane_copy, bcol_out.at[f], bcol_in.at[f], 7 + f, 2 * COLS, q)

    def send_brow(f):
        start_all(row_copy, brow_out.at[f], brow_in.at[f], 10 + f, ROWS, r)

    def all_of(kind, f):
        src, dst, base, count = {
            "row": (row_out, row_in, 0, ROWS),
            "col": (col_out, col_in, 4, 2 * COLS),
            "bcol": (bcol_out, bcol_in, 7, 2 * COLS),
            "brow": (brow_out, brow_in, 10, ROWS),
        }[kind]
        return whole(src.at[f], dst.at[f], base + f, count)

    def arrived(kind, f):
        all_of(kind, f).wait_recv()

    def load(ref, rows):
        return [ref[z, rows, :] for z in range(NZ)]

    def store(ref, rows, planes):
        for z in range(NZ):
            ref[z, rows, :] = planes[z]

    def chunks(body):
        def step(i, carry):
            body(pl.ds(pl.multiple_of(i * 8, 8), 8))
            return carry

        lax.fori_loop(0, YB // 8, step, 0)

    def pressure_planes(rows):
        store(row_out.at[0], rows, depth_forward(load(p_ref, rows)))

    chunks(pressure_planes)

    lane_rows = lax.broadcasted_iota(jnp.int32, (SLOTS, XB), 0)
    slot = q * SLOTS + lane_rows
    one, zero = jnp.ones((SLOTS, XB), f32), jnp.zeros((SLOTS, XB), f32)
    first = jnp.where(slot == 0, one, zero)
    flat = jnp.where(jnp.full((SLOTS, XB), j, jnp.int32) == 0, one, zero)
    general = (1.0 - first) * (1.0 - flat)
    half_general = 0.5 * general
    first_deep = first * (1.0 - flat)
    first_flat = first * flat
    rest_flat = flat * (1.0 - first)
    own_imag = first_deep + rest_flat
    not_first = 1.0 - first
    not_flat = 1.0 - flat

    pi2 = np.float32(math.pi * math.pi)
    ky = slot.astype(f32) * np.float32(2.0 * math.pi / NY)
    kz = jnp.full((SLOTS, XB), j, jnp.int32).astype(f32) * np.float32(2.0 * math.pi / NZ)
    low = ky * ky + kz * kz
    top = low + pi2 * (first_deep + flat)
    extra = pi2 + jnp.where(lane_rows == 0, zero, pi2 * one)
    scale = np.float32((0.5 * reference_speed * time_step) ** 2)

    def fill_kappa(kc, carry):
        kx2 = xt_ref[2, pl.ds(kc, 1), :]
        for g, part in enumerate((low, top, extra)):
            v2 = scale * (kx2 + part)
            series = 1.0 + v2 * np.float32(-1.0 / 110.0)
            series = 1.0 + v2 * np.float32(-1.0 / 72.0) * series
            series = 1.0 + v2 * np.float32(-1.0 / 42.0) * series
            series = 1.0 + v2 * np.float32(-1.0 / 20.0) * series
            kappa[g, kc] = 1.0 + v2 * np.float32(-1.0 / 6.0) * series
        return carry

    lax.fori_loop(0, COLS, fill_kappa, 0)

    pl.semaphore_wait(barrier, ROWS - 1 + 2 * COLS - 1)
    send_row(0)

    def lines(ref, f):
        return ref[f].reshape(NY, XB)

    def row_product(table, values):
        parts = [halves(v) for v in values]
        high = [part[0] for part in parts]
        low_part = [part[1] for part in parts]
        if len(values) == 1:
            both = mm(table[0], jnp.concatenate([high[0], low_part[0]], axis=1))
            return [both[:, :XB] + both[:, XB:] + mm(table[1], high[0])]
        high = jnp.concatenate(high, axis=1)
        low_part = jnp.concatenate(low_part, axis=1)
        result = mm(table[0], high) + mm(table[0], low_part) + mm(table[1], high)
        return [result[:, :XB], result[:, XB:]]

    def y_derivative(value, sign):
        parts = value.reshape(NY // 2 // SLOTS, 2, SLOTS, XB)
        re, im = parts[:, 0], parts[:, 1]
        same, same_imag, cross = yd_ref[0], yd_ref[1], yd_ref[2]
        if sign > 0:
            out = [re * same - im * cross, im * same_imag + re * cross]
        else:
            out = [-(re * same + im * cross), re * cross - im * same_imag]
        return jnp.stack(out, axis=1).reshape(NY, XB)

    def x_forward(f):
        for n in range(COLS):
            rr, ri = col_in[f, n, 0:8, :], col_in[f, n, 8:16, :]
            ir, ii = col_in[f, COLS + n, 0:8, :], col_in[f, COLS + n, 8:16, :]
            xb[0, 0, n] = rr - general * ii
            xb[0, 1, n] = not_first * ri + not_flat * ir
            xb[1, 0, n] = general * (rr + ii) + first_deep * ri + flat * ir
            xb[1, 1, n] = general * (ir - ri) + own_imag * ii
            xb[2, 0, n] = first_flat * ri + pltpu.roll(first_flat * ii, 1, 0)
            xb[2, 1, n] = zero

        def group(g, carry):
            values = [(xb[g, 0, n], xb[g, 1, n]) for n in range(COLS)]
            values = short_transform(values, -1.0)
            for kc in range(COLS):
                re, im = values[kc]
                cs, sn = xt_ref[0, kc : kc + 1, :], xt_ref[1, kc : kc + 1, :]
                xs[0, g, kc, :, :XB] = re * cs + im * sn
                xs[0, g, kc, :, XB:] = im * cs - re * sn
            return carry

        lax.fori_loop(0, 3, group, 0)
        high, low_part = halves(xs[0].reshape(3 * COLS * SLOTS, 2 * XB))
        out = mm(high, wx_ref[0]) + mm(low_part, wx_ref[0]) + mm(high, wx_ref[1])
        return out.reshape(3, COLS, SLOTS, 2 * XB)

    def x_derivative(re, im, sign):
        same = xt_ref[3][None, :, None, :]
        cross = xt_ref[4][None, :, None, :]
        if sign > 0:
            return -(re * same + im * cross), re * cross - im * same
        return re * same - im * cross, im * same + re * cross

    def x_inverse(value, f):
        high, low_part = halves(value.reshape(3 * COLS * SLOTS, 2 * XB))
        out = mm(high, ux_ref[0]) + mm(low_part, ux_ref[0]) + mm(high, ux_ref[1])
        xs[0] = out.reshape(3, COLS, SLOTS, 2 * XB)

        def group(g, carry):
            values = []
            for kc in range(COLS):
                re, im = xs[0, g, kc, :, :XB], xs[0, g, kc, :, XB:]
                cs, sn = xt_ref[0, kc : kc + 1, :], xt_ref[1, kc : kc + 1, :]
                values.append((re * cs - im * sn, im * cs + re * sn))
            values = short_transform(values, 1.0)
            for n in range(COLS):
                xb[g, 0, n] = values[n][0]
                xb[g, 1, n] = values[n][1]
            return carry

        lax.fori_loop(0, 3, group, 0)
        for n in range(COLS):
            lr, li = xb[0, 0, n], xb[0, 1, n]
            hr, hi = xb[1, 0, n], xb[1, 1, n]
            xr = xb[2, 0, n]
            bcol_out[f, n, 0:8, :] = lr + half_general * (hr - lr)
            bcol_out[f, n, 8:16, :] = (
                half_general * (li - hi) + first_deep * hr + rest_flat * li + first_flat * xr
            )
            bcol_out[f, COLS + n, 0:8, :] = half_general * (li + hi) + first_deep * li + flat * hr
            bcol_out[f, COLS + n, 8:16, :] = (
                half_general * (hr - lr) + own_imag * hi + first_flat * pltpu.roll(xr, 7, 0)
            )

    arrived("row", 0)
    col_out[0] = row_product(fy_ref, [lines(row_in, 0)])[0].reshape(2 * COLS, 2 * SLOTS, XB)
    send_col(0)

    arrived("col", 0)
    spectrum = x_forward(0)
    re, im = spectrum[..., :XB] * kappa[...], spectrum[..., XB:] * kappa[...]
    dre, dim = x_derivative(re, im, 1)
    x_inverse(jnp.concatenate([dre, dim], axis=-1), 0)
    send_bcol(0)
    x_inverse(jnp.concatenate([re, im], axis=-1), 1)
    send_bcol(1)

    arrived("bcol", 0)
    brow_out[0] = row_product(gy_ref, [lines(bcol_in, 0)])[0].reshape(ROWS, YB, XB)
    send_brow(0)

    dx = dx_ref[0:8, :]

    arrived("brow", 0)

    def update_x(rows):
        grad = depth_inverse(load(brow_in.at[0], rows))
        fresh = []
        for z in range(NZ):
            change = time_step * b_ref[z, rows, :] * grad[z]
            fresh.append(dx * (dx * vx_ref[z, rows, :] - change))
        store(vxo_ref, rows, fresh)
        store(row_out.at[1], rows, depth_forward(fresh))

    chunks(update_x)
    send_row(1)

    arrived("bcol", 1)
    flow = lines(bcol_in, 1)
    plain, slope = row_product(gy_ref, [flow, y_derivative(flow, 1)])
    brow_out[1] = slope.reshape(ROWS, YB, XB)
    send_brow(1)
    brow_out[2] = plain.reshape(ROWS, YB, XB)
    send_brow(2)

    arrived("row", 1)
    col_out[1] = row_product(fy_ref, [lines(row_in, 1)])[0].reshape(2 * COLS, 2 * SLOTS, XB)
    send_col(1)

    arrived("brow", 1)

    def update_y(rows):
        grad = depth_inverse(load(brow_in.at[1], rows))
        dy = dy_ref[rows, :]
        fresh = []
        for z in range(NZ):
            change = time_step * b_ref[z, rows, :] * grad[z]
            fresh.append(dy * (dy * vy_ref[z, rows, :] - change))
        store(vyo_ref, rows, fresh)
        store(row_out.at[2], rows, depth_forward(fresh))

    chunks(update_y)
    send_row(2)

    arrived("brow", 2)

    def update_z(rows):
        grad = depth_inverse(depth_derivative(load(brow_in.at[2], rows), 1))
        fresh = []
        for z in range(NZ):
            fresh.append(vz_ref[z, rows, :] - time_step * b_ref[z, rows, :] * grad[z])
        store(vzo_ref, rows, fresh)
        store(row_out.at[3], rows, depth_derivative(depth_forward(fresh), -1))

    chunks(update_z)
    send_row(3)

    arrived("row", 2)
    arrived("row", 3)
    across, deep = row_product(fy_ref, [lines(row_in, 2), lines(row_in, 3)])
    summed = deep + y_derivative(across, -1)
    col_out[2] = summed.reshape(2 * COLS, 2 * SLOTS, XB)
    send_col(2)

    arrived("col", 1)
    flow_x = x_forward(1)
    tre, tim = x_derivative(flow_x[..., :XB], flow_x[..., XB:], -1)
    arrived("col", 2)
    rest = x_forward(2)
    tre = (tre + rest[..., :XB]) * kappa[...]
    tim = (tim + rest[..., XB:]) * kappa[...]
    x_inverse(jnp.concatenate([tre, tim], axis=-1), 2)
    send_bcol(2)

    arrived("bcol", 2)
    brow_out[3] = row_product(gy_ref, [lines(bcol_in, 2)])[0].reshape(ROWS, YB, XB)
    send_brow(3)

    arrived("brow", 3)

    def update_p(rows):
        divergence = depth_inverse(load(brow_in.at[3], rows))
        both = dx * dy_ref[rows, :]
        for z in range(NZ):
            change = time_step * m_ref[z, rows, :] * divergence[z]
            po_ref[z, rows, :] = both * (both * p_ref[z, rows, :] - change)

    chunks(update_p)

    for kind, number in (("row", 4), ("col", 3), ("bcol", 3), ("brow", 4)):
        for f in range(number):
            all_of(kind, f).wait_send()


def extended(array, sides, width):
    for axis, dim in sides:
        size, length = (lax.axis_size(axis), array.shape[dim])
        up = [(i, (i + 1) % size) for i in range(size)]
        down = [(j, i) for i, j in up]
        last = lax.slice_in_dim(array, length - width, length, axis=dim)
        initial = lax.slice_in_dim(array, 0, width, axis=dim)
        before = lax.ppermute(last, axis, up)
        after = lax.ppermute(initial, axis, down)
        array = jnp.concatenate([before, array, after], axis=dim)
    return array


def band_matrix(filter_taps, extent):
    tap_count = filter_taps.shape[0]
    offset = (
        jnp.arange(extent + tap_count - 1, dtype=jnp.int32)[:, None]
        - jnp.arange(extent, dtype=jnp.int32)[None, :]
    )
    selected = offset[:, :, None] == jnp.arange(tap_count, dtype=jnp.int32)[None, None, :]
    return jnp.sum(jnp.where(selected, filter_taps[None, None, :], 0.0), axis=2)


def absorber(position, length, low_width, high_width):
    low_part = jnp.maximum(low_width - position, 0).astype(f32) / low_width.astype(f32)
    high_part = jnp.maximum(position - (length - 1 - high_width), 0).astype(
        f32
    ) / high_width.astype(f32)
    damping = absorption * reference_speed * (low_part**4 + high_part**4)
    return jnp.exp(-0.5 * time_step * damping)


def on_device(
    labels, pressure, velocity_x, velocity_y, velocity_z,
    speed_table, density_table, filter_taps, layer_width,
):
    planes, height, breadth = pressure.shape
    buoyancy_of = 1.0 / density_table
    modulus_of = density_table * speed_table * speed_table
    buoyancy = jnp.zeros(pressure.shape, f32)
    modulus = jnp.zeros(pressure.shape, f32)
    for label_id in range(speed_table.shape[0]):
        matches = labels == label_id
        buoyancy = jnp.where(matches, buoyancy_of[label_id], buoyancy)
        modulus = jnp.where(matches, modulus_of[label_id], modulus)
    coefficients = jnp.stack([buoyancy, modulus])
    reach = filter_taps.shape[0] // 2
    across = band_matrix(filter_taps, breadth)
    downward = band_matrix(filter_taps, height)
    padded = extended(coefficients, (("col", 3),), reach)
    smoothed = jnp.einsum("fzyj,ji->fzyi", padded, across, precision=highest)
    padded = extended(smoothed, (("row", 2),), reach)
    smoothed = jnp.einsum("fzjx,jy->fzyx", padded, downward, precision=highest)
    buoyancy = smoothed[0]
    modulus = smoothed[1]
    column_ids = lax.axis_index("col") * breadth + jnp.arange(breadth, dtype=jnp.int32)
    row_ids = lax.axis_index("row") * height + jnp.arange(height, dtype=jnp.int32)
    damp_x = absorber(column_ids, NX, layer_width[0], layer_width[1])
    damp_y = absorber(row_ids, NY, layer_width[2], layer_width[3])
    damp_x = jnp.broadcast_to(damp_x[None, :], (8, breadth))
    damp_y = jnp.broadcast_to(damp_y[:, None], (height, breadth))

    fy, gy, yd = row_tables()
    wx, ux, xt = column_tables()
    brick = jax.ShapeDtypeStruct(pressure.shape, f32)
    row_buffer = lambda n: pltpu.VMEM((n, ROWS, YB, XB), f32)
    col_buffer = lambda n: pltpu.VMEM((n, 2 * COLS, 2 * SLOTS, XB), f32)
    return pl.pallas_call(
        step_kernel,
        out_shape=(brick,) * 4,
        in_specs=[pl.BlockSpec(memory_space=pltpu.VMEM)] * 14,
        out_specs=(pl.BlockSpec(memory_space=pltpu.VMEM),) * 4,
        scratch_shapes=[
            row_buffer(4), row_buffer(4), col_buffer(3), col_buffer(3),
            col_buffer(3), col_buffer(3), row_buffer(4), row_buffer(4),
            pltpu.VMEM((3, COLS, SLOTS, XB), f32),
            pltpu.VMEM((3, 2, COLS, SLOTS, XB), f32),
            pltpu.VMEM((1, 3, COLS, SLOTS, 2 * XB), f32),
            pltpu.SemaphoreType.DMA((14,)),
            pltpu.SemaphoreType.DMA((14,)),
        ],
        compiler_params=pltpu.CompilerParams(
            collective_id=0, has_side_effects=True, vmem_limit_bytes=48 * 1024 * 1024
        ),
    )(
        pressure, velocity_x, velocity_y, velocity_z, buoyancy, modulus, damp_x, damp_y,
        jnp.asarray(fy), jnp.asarray(gy), jnp.asarray(yd),
        jnp.asarray(wx), jnp.asarray(ux), jnp.asarray(xt),
    )


def solution(mesh):
    brick = P(None, "row", "col")
    return jax.shard_map(
        on_device,
        mesh=mesh,
        in_specs=(brick,) * 5 + (P(),) * 4,
        out_specs=(brick,) * 4,
        check_vma=False,
    )
```

```python
import functools
import math

import jax
import jax.numpy as jnp
import numpy as np
from jax import lax
from jax.experimental import pallas as pl
from jax.experimental.pallas import tpu as pltpu
from jax.sharding import PartitionSpec as P

time_step = 0.15
reference_speed = 2.0
absorption = 6.0
MESH = pl.DeviceIdType.MESH

NZ, NY, NX = 16, 512, 2048
ROWS, COLS = 16, 16
YB, XB = NY // ROWS, NX // COLS
SLOTS, HALO = 8, 16
VMEM_BYTES = 67043328
TAPS, LABELS = 33, 12
f32, bf16 = jnp.float32, jnp.bfloat16


def split_table(table):
    high = table.astype(np.float32).astype(bf16)
    low = (table - high.astype(np.float64)).astype(np.float32).astype(bf16)
    return np.stack([high, low])


def row_tables():
    slot = np.arange(NY // 2)
    y = np.arange(NY)
    angle = 2.0 * np.pi * ((slot[:, None] * y[None, :]) % NY) / NY
    real, imag = np.cos(angle), -np.sin(angle)
    imag[0] = np.where(y % 2 == 0, 1.0, -1.0)
    order = lambda t: t.reshape(NY // 2 // SLOTS, SLOTS, NY)
    forward = np.stack([order(real), order(imag)], axis=1).reshape(NY, NY)
    weight = np.where(slot == 0, 1.0, 2.0) / NY
    inverse = np.stack([order(real * weight[:, None]), order(imag * weight[:, None])], axis=1)
    inverse = inverse.reshape(NY, NY).T
    wave = 2.0 * np.pi * slot / NY
    same = -wave * np.sin(0.5 * wave)
    cross = wave * np.cos(0.5 * wave)
    same_imag = same.copy()
    same_imag[0] = -np.pi
    wide = lambda v: np.broadcast_to(v.reshape(-1, SLOTS, 1), (NY // 2 // SLOTS, SLOTS, XB))
    derivative = np.stack([wide(same), wide(same_imag), wide(cross)]).astype(np.float32)
    return split_table(forward), split_table(inverse), derivative


def column_tables():
    x = np.arange(XB)
    angle = 2.0 * np.pi * ((x[:, None] * x[None, :]) % XB) / XB
    c, s = np.cos(angle), np.sin(angle)
    forward = np.block([[c, -s], [s, c]])
    inverse = np.block([[c, s], [-s, c]]) / NX
    kc = np.arange(COLS)
    twist = 2.0 * np.pi * (kc[:, None] * x[None, :]) / NX
    index = kc[:, None] + COLS * x[None, :]
    wave = 2.0 * np.pi * np.where(index < NX // 2, index, index - NX) / NX
    same = wave * np.sin(0.5 * wave)
    cross = wave * np.cos(0.5 * wave)
    small = np.stack([np.cos(twist), np.sin(twist), wave * wave, same, cross]).astype(np.float32)
    return split_table(forward), split_table(inverse), small


def scaled(value, factor):
    if abs(factor - 1.0) < 1e-12:
        return value
    if abs(factor + 1.0) < 1e-12:
        return -value
    return value * np.float32(factor)


def weighted(terms):
    total = None
    for value, factor in terms:
        if abs(factor) < 1e-12:
            continue
        if total is None:
            total = scaled(value, factor)
        elif abs(factor + 1.0) < 1e-12:
            total = total - value
        else:
            total = total + scaled(value, factor)
    return total


def cos16(n):
    return math.cos(2.0 * math.pi * (n % 16) / 16)


def sin16(n):
    return math.sin(2.0 * math.pi * (n % 16) / 16)


def depth_forward(p):
    even = [p[0]] + [p[n] + p[16 - n] for n in range(1, 8)] + [p[8]]
    odd = [None] + [p[n] - p[16 - n] for n in range(1, 8)]
    plus = [even[n] + even[8 - n] for n in range(4)] + [even[4]]
    minus = [even[n] - even[8 - n] for n in range(4)]
    odd_plus = [None] + [odd[n] + odd[8 - n] for n in range(1, 4)] + [odd[4]]
    odd_minus = [None] + [odd[n] - odd[8 - n] for n in range(1, 4)]

    def real_of(k):
        side = plus if k % 2 == 0 else minus
        return weighted([(side[n], cos16(k * n)) for n in range(len(side))])

    def imag_of(k):
        if k % 2 == 0:
            return weighted([(odd_minus[n], -sin16(k * n)) for n in range(1, 4)])
        return weighted([(odd_plus[n], -sin16(k * n)) for n in range(1, 5)])

    out = [real_of(0), real_of(8)]
    for k in range(1, 8):
        out += [real_of(k), imag_of(k)]
    return out


def depth_inverse(m):
    real = [m[0]] + [m[2 * k] for k in range(1, 8)] + [m[1]]
    imag = [None] + [m[2 * k + 1] for k in range(1, 8)]
    weight = [1.0 / 16] + [2.0 / 16] * 7 + [1.0 / 16]

    def terms(values, ids, n, wave):
        return weighted([(values[k], weight[k] * wave(k * n)) for k in ids])

    out = [None] * 16
    for n in range(0, 5):
        ce = terms(real, range(0, 9, 2), n, cos16)
        co = terms(real, range(1, 9, 2), n, cos16)
        so = terms(imag, range(1, 8, 2), n, lambda v: -sin16(v))
        se = terms(imag, range(2, 8, 2), n, lambda v: -sin16(v))
        near = ce if co is None else ce + co
        far = ce if co is None else ce - co
        if n == 0:
            out[0], out[8] = near, far
            continue
        if se is None:
            d_near, d_far = so, so
        else:
            d_near, d_far = so + se, so - se
        out[n], out[16 - n] = near + d_near, near - d_near
        if n < 4:
            out[8 - n], out[8 + n] = far + d_far, far - d_far
    return out


def depth_derivative(m, sign):
    out = [jnp.zeros_like(m[0]), m[1] * np.float32(-sign * math.pi)]
    for k in range(1, 8):
        wave = 2.0 * math.pi * k / 16
        a = np.float32(-sign * wave * math.sin(0.5 * wave))
        b = np.float32(wave * math.cos(0.5 * wave))
        out += [m[2 * k] * a - m[2 * k + 1] * b, m[2 * k + 1] * a + m[2 * k] * b]
    return out


def short_transform(values, sign):
    count = len(values)
    if count == 1:
        return values
    even = short_transform(values[0::2], sign)
    odd = short_transform(values[1::2], sign)
    out = [None] * count
    for k in range(count // 2):
        angle = sign * 2.0 * math.pi * k / count
        c, s = math.cos(angle), math.sin(angle)
        re, im = odd[k]
        if k == 0:
            tr, ti = re, im
        elif abs(c) < 1e-9:
            tr, ti = (-im, re) if s > 0 else (im, -re)
        elif abs(abs(c) - abs(s)) < 1e-9:
            h = np.float32(abs(c))
            cs, ss = (1 if c > 0 else -1), (1 if s > 0 else -1)
            first = re if cs > 0 else -re
            tr = (first - im if ss > 0 else first + im) * h
            second = im if cs > 0 else -im
            ti = (second + re if ss > 0 else second - re) * h
        else:
            tr = re * np.float32(c) - im * np.float32(s)
            ti = re * np.float32(s) + im * np.float32(c)
        er, ei = even[k]
        out[k] = (er + tr, ei + ti)
        out[k + count // 2] = (er - tr, ei - ti)
    return out


def halves(value):
    high = value.astype(bf16)
    low = (value - high.astype(f32)).astype(bf16)
    return high, low


def mm(a, b):
    return jnp.dot(a, b, preferred_element_type=f32)


def step_kernel(
    lab_hbm, p_hbm, vx_hbm, vy_hbm, vz_hbm, speed_hbm, density_hbm, taps_hbm, width_hbm,
    fy_hbm, gy_hbm, yd_hbm, wx_hbm, ux_hbm, xt_hbm,
    po_hbm, vxo_hbm, vyo_hbm, vzo_hbm,
    row_out, row_in, col_out, col_in, bcol_out, bcol_in, brow_out, brow_in,
    kappa, xb, xs, coef, lab, edge_out, edge_in, raw, across, edge_band, down, damp,
    lab_ref, p_ref, vx_ref, vy_ref, vz_ref, speed_ref, density_ref, taps_ref, width_ref,
    fy_ref, gy_ref, yd_ref, wx_ref, ux_ref, xt_ref,
    po_ref, vxo_ref, vyo_ref, vzo_ref,
    send_sem, recv_sem, load_sem, store_sem,
):
    fetches = [
        pltpu.make_async_copy(source, target, load_sem.at[n])
        for n, (source, target) in enumerate(
            [
                (p_hbm, p_ref), (lab_hbm, lab_ref), (xt_hbm, xt_ref), (taps_hbm, taps_ref),
                (width_hbm, width_ref), (fy_hbm, fy_ref), (wx_hbm, wx_ref),
                (speed_hbm, speed_ref), (density_hbm, density_ref), (ux_hbm, ux_ref),
                (gy_hbm, gy_ref), (vx_hbm, vx_ref), (yd_hbm, yd_ref), (vy_hbm, vy_ref),
                (vz_hbm, vz_ref),
            ]
        )
    ]
    for fetch in fetches:
        fetch.start()
    writes = [
        pltpu.make_async_copy(source, target, store_sem.at[n])
        for n, (source, target) in enumerate(
            [(vxo_ref, vxo_hbm), (vyo_ref, vyo_hbm), (vzo_ref, vzo_hbm), (po_ref, po_hbm)]
        )
    ]

    def loaded(*numbers):
        for n in numbers:
            fetches[n].wait()

    r, c = lax.axis_index("row"), lax.axis_index("col")
    j, h = r // 2, r % 2
    q = h * COLS + c

    barrier = pltpu.get_barrier_semaphore()

    def greet_row(i, carry):
        pl.semaphore_signal(barrier, inc=1, device_id=((r + i) % ROWS, c), device_id_type=MESH)
        return carry

    def greet_plane(i, carry):
        t = (q + i) % (2 * COLS)
        pl.semaphore_signal(
            barrier, inc=1, device_id=(2 * j + t // COLS, t % COLS), device_id_type=MESH
        )
        return carry

    lax.fori_loop(1, ROWS, greet_row, 0)
    lax.fori_loop(1, 2 * COLS, greet_plane, 0)

    def row_copy(src, dst, sem, i):
        t = (r + i) % ROWS
        return pltpu.make_async_remote_copy(
            src_ref=src.at[t], dst_ref=dst.at[r], send_sem=send_sem.at[sem],
            recv_sem=recv_sem.at[sem], device_id=(t, c), device_id_type=MESH,
        )

    def plane_copy(src, dst, sem, i):
        t = (q + i) % (2 * COLS)
        return pltpu.make_async_remote_copy(
            src_ref=src.at[t], dst_ref=dst.at[q], send_sem=send_sem.at[sem],
            recv_sem=recv_sem.at[sem], device_id=(2 * j + t // COLS, t % COLS),
            device_id_type=MESH,
        )

    def start_all(copy_of, src, dst, sem, count, own):
        def body(i, carry):
            copy_of(src, dst, sem, i).start()
            return carry

        lax.fori_loop(1, count, body, 0)
        dst[own] = src[own]

    def whole(src, dst, sem, count):
        span = pl.ds(0, count - 1)
        return pltpu.make_async_remote_copy(
            src_ref=src.at[span], dst_ref=dst.at[span], send_sem=send_sem.at[sem],
            recv_sem=recv_sem.at[sem], device_id=((r + 1) % ROWS, c), device_id_type=MESH,
        )

    def send_row(f):
        start_all(row_copy, row_out.at[f], row_in.at[f], f, ROWS, r)

    def send_col(f):
        start_all(plane_copy, col_out.at[f], col_in.at[f], 4 + f, 2 * COLS, q)

    def send_bcol(f):
        start_all(plane_copy, bcol_out.at[f], bcol_in.at[f], 7 + f, 2 * COLS, q)

    def send_brow(f):
        start_all(row_copy, brow_out.at[f], brow_in.at[f], 10 + f, ROWS, r)

    def all_of(kind, f):
        src, dst, base, count = {
            "row": (row_out, row_in, 0, ROWS),
            "col": (col_out, col_in, 4, 2 * COLS),
            "bcol": (bcol_out, bcol_in, 7, 2 * COLS),
            "brow": (brow_out, brow_in, 10, ROWS),
        }[kind]
        return whole(src.at[f], dst.at[f], base + f, count)

    def arrived(kind, f):
        all_of(kind, f).wait_recv()

    def load(ref, rows):
        return [ref[z, rows, :] for z in range(NZ)]

    def store(ref, rows, planes):
        for z in range(NZ):
            ref[z, rows, :] = planes[z]

    def chunks(body):
        def step(i, carry):
            body(pl.ds(pl.multiple_of(i * 8, 8), 8))
            return carry

        lax.fori_loop(0, YB // 8, step, 0)

    def pressure_planes(rows):
        store(row_out.at[0], rows, depth_forward(load(p_ref, rows)))

    loaded(0)
    chunks(pressure_planes)

    loaded(1)
    for z in range(NZ):
        lab[z, HALO : HALO + YB, :] = lab_ref[z].astype(f32)

    def y_edges():
        before, after = (r + ROWS - 1) % ROWS, (r + 1) % ROWS
        return [
            pltpu.make_async_remote_copy(
                src_ref=lab.at[:, pl.ds(HALO, HALO), :],
                dst_ref=lab.at[:, pl.ds(HALO + YB, HALO), :],
                send_sem=send_sem.at[14], recv_sem=recv_sem.at[14],
                device_id=(before, c), device_id_type=MESH,
            ),
            pltpu.make_async_remote_copy(
                src_ref=lab.at[:, pl.ds(YB, HALO), :],
                dst_ref=lab.at[:, pl.ds(0, HALO), :],
                send_sem=send_sem.at[15], recv_sem=recv_sem.at[15],
                device_id=(after, c), device_id_type=MESH,
            ),
        ]

    def x_edges():
        before, after = (c + COLS - 1) % COLS, (c + 1) % COLS
        return [
            pltpu.make_async_remote_copy(
                src_ref=edge_out.at[0], dst_ref=edge_in.at[1],
                send_sem=send_sem.at[16], recv_sem=recv_sem.at[16],
                device_id=(r, before), device_id_type=MESH,
            ),
            pltpu.make_async_remote_copy(
                src_ref=edge_out.at[1], dst_ref=edge_in.at[0],
                send_sem=send_sem.at[17], recv_sem=recv_sem.at[17],
                device_id=(r, after), device_id_type=MESH,
            ),
        ]

    def ids(shape, dim):
        return lax.broadcasted_iota(jnp.int32, shape, dim)

    def banded(offset):
        def tap(t, total):
            return jnp.where(offset == t, taps_ref[t], total)

        return lax.fori_loop(0, TAPS, tap, jnp.zeros(offset.shape, f32), unroll=3)

    def fill_bands():
        wide = (XB, XB)
        band = banded(ids(wide, 0) - ids(wide, 1) + HALO)
        none = jnp.zeros(wide, bf16)
        for part, value in enumerate(halves(band)):
            top_rows = jnp.concatenate([value, none], axis=1)
            low_rows = jnp.concatenate([none, value], axis=1)
            across[part] = jnp.concatenate([top_rows, low_rows], axis=0)
        edge_band[0] = banded(ids(wide, 0) % HALO - ids(wide, 1))
        edge_band[1] = banded(ids(wide, 0) % HALO - ids(wide, 1) + XB + HALO)
        tall = (4 * YB, 8 * YB)
        row, line = ids(tall, 0), ids(tall, 1)
        offset = jnp.where(row // YB == line // (2 * YB), line % (2 * YB) - row % YB, -1)
        for part, value in enumerate(halves(banded(offset))):
            down[part] = value

    def fill_damping():
        def absorb(position, length, low_width, high_width):
            size = position.shape
            low_side = jnp.maximum(low_width - position, 0).astype(f32)
            high_side = jnp.maximum(position - (length - 1 - high_width), 0).astype(f32)
            low_side = low_side / jnp.full(size, low_width, jnp.int32).astype(f32)
            high_side = high_side / jnp.full(size, high_width, jnp.int32).astype(f32)
            low_side, high_side = low_side * low_side, high_side * high_side
            total = low_side * low_side + high_side * high_side
            return jnp.exp((-0.5 * time_step * absorption * reference_speed) * total)

        damp[0:8] = absorb(c * XB + ids((8, XB), 1), NX, width_ref[0], width_ref[1])
        damp[8:] = absorb(r * YB + ids((YB, XB), 0), NY, width_ref[2], width_ref[3])

    def pack_edges():
        wide = (XB, XB)
        source, target = ids(wide, 0), ids(wide, 1)
        total = None
        for g in range(8):
            here = target // HALO == g
            first_lanes = here & (source == target % HALO)
            last_lanes = here & (source == target % HALO + XB - HALO)
            select = jnp.concatenate(
                [jnp.where(first_lanes, 1.0, 0.0), jnp.where(last_lanes, 1.0, 0.0)], axis=1
            ).astype(bf16)
            part = mm(lab[2 * g : 2 * g + 2].reshape(XB, XB).astype(bf16), select)
            total = part if total is None else total + part
        edge_out[0] = total[:, :XB]
        edge_out[1] = total[:, XB:]

    def tables():
        density = [jnp.full((8, XB), density_ref[n], f32) for n in range(LABELS)]
        speed = [jnp.full((8, XB), speed_ref[n], f32) for n in range(LABELS)]
        return [1.0 / d for d in density], [d * s * s for d, s in zip(density, speed)]

    def look_up(label, table):
        value = jnp.broadcast_to(table[0][None], label.shape)
        for n in range(1, LABELS):
            value = jnp.where(label == float(n), table[n][None], value)
        return value

    def fill_raw():
        buoyancy_of, modulus_of = tables()

        def plane(z, carry):
            label = lab[z].reshape(8, 8, XB)
            rows = pl.ds(pl.multiple_of(z * 2 * YB, 2 * YB), 2 * YB)
            raw[rows, :XB] = look_up(label, buoyancy_of).reshape(2 * YB, XB)
            raw[rows, XB:] = look_up(label, modulus_of).reshape(2 * YB, XB)
            return carry

        lax.fori_loop(0, NZ, plane, 0)

    def smooth():
        buoyancy_of, modulus_of = tables()
        edges = [edge_in[0].reshape(16, 8, XB), edge_in[1].reshape(16, 8, XB)]
        sides = [
            halves(jnp.concatenate([look_up(e, t).reshape(XB, XB) for e in edges], axis=1))
            for t in (buoyancy_of, modulus_of)
        ]
        group_of = ids((XB, XB), 0) // HALO

        def quarter(i, carry):
            rows = pl.ds(pl.multiple_of(i * 8 * YB, 8 * YB), 8 * YB)
            high, low_part = halves(raw[rows, :])
            main = mm(high, across[0]) + mm(low_part, across[0]) + mm(high, across[1])
            parts = []
            for g in range(2):
                inside = group_of == 2 * i + g
                parts.append(
                    jnp.concatenate(
                        [jnp.where(inside, edge_band[s], 0.0) for s in range(2)], axis=0
                    )
                )
            high, low_part = halves(jnp.concatenate(parts, axis=1))
            columns = []
            for side_high, side_low in sides:
                out = mm(side_high, high) + mm(side_low, high) + mm(side_high, low_part)
                columns.append(jnp.concatenate([out[:, :XB], out[:, XB:]], axis=0))
            high, low_part = halves(main + jnp.concatenate(columns, axis=1))
            out = mm(down[0], high) + mm(down[0], low_part) + mm(down[1], high)
            planes = pl.ds(i * 4, 4)
            coef[0, planes] = out[:, :XB].reshape(4, YB, XB)
            coef[1, planes] = out[:, XB:].reshape(4, YB, XB)
            return carry

        lax.fori_loop(0, 4, quarter, 0)

    lane_rows = lax.broadcasted_iota(jnp.int32, (SLOTS, XB), 0)
    slot = q * SLOTS + lane_rows
    one, zero = jnp.ones((SLOTS, XB), f32), jnp.zeros((SLOTS, XB), f32)
    first = jnp.where(slot == 0, one, zero)
    flat = jnp.where(jnp.full((SLOTS, XB), j, jnp.int32) == 0, one, zero)
    general = (1.0 - first) * (1.0 - flat)
    half_general = 0.5 * general
    first_deep = first * (1.0 - flat)
    first_flat = first * flat
    rest_flat = flat * (1.0 - first)
    own_imag = first_deep + rest_flat
    not_first = 1.0 - first
    not_flat = 1.0 - flat

    pi2 = np.float32(math.pi * math.pi)
    ky = slot.astype(f32) * np.float32(2.0 * math.pi / NY)
    kz = jnp.full((SLOTS, XB), j, jnp.int32).astype(f32) * np.float32(2.0 * math.pi / NZ)
    low = ky * ky + kz * kz
    top = low + pi2 * (first_deep + flat)
    extra = pi2 + jnp.where(lane_rows == 0, zero, pi2 * one)
    scale = np.float32((0.5 * reference_speed * time_step) ** 2)

    def fill_kappa(kc, carry):
        kx2 = xt_ref[2, pl.ds(kc, 1), :]
        for g, part in enumerate((low, top, extra)):
            v2 = scale * (kx2 + part)
            series = 1.0 + v2 * np.float32(-1.0 / 110.0)
            series = 1.0 + v2 * np.float32(-1.0 / 72.0) * series
            series = 1.0 + v2 * np.float32(-1.0 / 42.0) * series
            series = 1.0 + v2 * np.float32(-1.0 / 20.0) * series
            kappa[g, kc] = 1.0 + v2 * np.float32(-1.0 / 6.0) * series
        return carry

    loaded(2)
    lax.fori_loop(0, COLS, fill_kappa, 0)

    pl.semaphore_wait(barrier, ROWS - 1 + 2 * COLS - 1)
    send_row(0)
    for edge in y_edges():
        edge.start()
    loaded(3, 4)
    fill_bands()
    fill_damping()

    def lines(ref, f):
        return ref[f].reshape(NY, XB)

    def row_product(table, values):
        parts = [halves(v) for v in values]
        high = [part[0] for part in parts]
        low_part = [part[1] for part in parts]
        if len(values) == 1:
            both = mm(table[0], jnp.concatenate([high[0], low_part[0]], axis=1))
            return [both[:, :XB] + both[:, XB:] + mm(table[1], high[0])]
        high = jnp.concatenate(high, axis=1)
        low_part = jnp.concatenate(low_part, axis=1)
        result = mm(table[0], high) + mm(table[0], low_part) + mm(table[1], high)
        return [result[:, :XB], result[:, XB:]]

    def y_derivative(value, sign):
        parts = value.reshape(NY // 2 // SLOTS, 2, SLOTS, XB)
        re, im = parts[:, 0], parts[:, 1]
        same, same_imag, cross = yd_ref[0], yd_ref[1], yd_ref[2]
        if sign > 0:
            out = [re * same - im * cross, im * same_imag + re * cross]
        else:
            out = [-(re * same + im * cross), re * cross - im * same_imag]
        return jnp.stack(out, axis=1).reshape(NY, XB)

    def x_forward(f):
        for n in range(COLS):
            rr, ri = col_in[f, n, 0:8, :], col_in[f, n, 8:16, :]
            ir, ii = col_in[f, COLS + n, 0:8, :], col_in[f, COLS + n, 8:16, :]
            xb[0, 0, n] = rr - general * ii
            xb[0, 1, n] = not_first * ri + not_flat * ir
            xb[1, 0, n] = general * (rr + ii) + first_deep * ri + flat * ir
            xb[1, 1, n] = general * (ir - ri) + own_imag * ii
            xb[2, 0, n] = first_flat * ri + pltpu.roll(first_flat * ii, 1, 0)
            xb[2, 1, n] = zero

        def group(g, carry):
            values = [(xb[g, 0, n], xb[g, 1, n]) for n in range(COLS)]
            values = short_transform(values, -1.0)
            for kc in range(COLS):
                re, im = values[kc]
                cs, sn = xt_ref[0, kc : kc + 1, :], xt_ref[1, kc : kc + 1, :]
                xs[0, g, kc, :, :XB] = re * cs + im * sn
                xs[0, g, kc, :, XB:] = im * cs - re * sn
            return carry

        lax.fori_loop(0, 3, group, 0)
        high, low_part = halves(xs[0].reshape(3 * COLS * SLOTS, 2 * XB))
        out = mm(high, wx_ref[0]) + mm(low_part, wx_ref[0]) + mm(high, wx_ref[1])
        return out.reshape(3, COLS, SLOTS, 2 * XB)

    def x_derivative(re, im, sign):
        same = xt_ref[3][None, :, None, :]
        cross = xt_ref[4][None, :, None, :]
        if sign > 0:
            return -(re * same + im * cross), re * cross - im * same
        return re * same - im * cross, im * same + re * cross

    def x_inverse(value, f):
        high, low_part = halves(value.reshape(3 * COLS * SLOTS, 2 * XB))
        out = mm(high, ux_ref[0]) + mm(low_part, ux_ref[0]) + mm(high, ux_ref[1])
        xs[0] = out.reshape(3, COLS, SLOTS, 2 * XB)

        def group(g, carry):
            values = []
            for kc in range(COLS):
                re, im = xs[0, g, kc, :, :XB], xs[0, g, kc, :, XB:]
                cs, sn = xt_ref[0, kc : kc + 1, :], xt_ref[1, kc : kc + 1, :]
                values.append((re * cs - im * sn, im * cs + re * sn))
            values = short_transform(values, 1.0)
            for n in range(COLS):
                xb[g, 0, n] = values[n][0]
                xb[g, 1, n] = values[n][1]
            return carry

        lax.fori_loop(0, 3, group, 0)
        for n in range(COLS):
            lr, li = xb[0, 0, n], xb[0, 1, n]
            hr, hi = xb[1, 0, n], xb[1, 1, n]
            xr = xb[2, 0, n]
            bcol_out[f, n, 0:8, :] = lr + half_general * (hr - lr)
            bcol_out[f, n, 8:16, :] = (
                half_general * (li - hi) + first_deep * hr + rest_flat * li + first_flat * xr
            )
            bcol_out[f, COLS + n, 0:8, :] = half_general * (li + hi) + first_deep * li + flat * hr
            bcol_out[f, COLS + n, 8:16, :] = (
                half_general * (hr - lr) + own_imag * hi + first_flat * pltpu.roll(xr, 7, 0)
            )

    loaded(5)
    arrived("row", 0)
    col_out[0] = row_product(fy_ref, [lines(row_in, 0)])[0].reshape(2 * COLS, 2 * SLOTS, XB)
    send_col(0)

    for edge in y_edges():
        edge.wait_recv()
    pack_edges()
    for edge in x_edges():
        edge.start()
    loaded(7, 8)
    fill_raw()

    loaded(6, 9)
    arrived("col", 0)
    spectrum = x_forward(0)
    re, im = spectrum[..., :XB] * kappa[...], spectrum[..., XB:] * kappa[...]
    dre, dim = x_derivative(re, im, 1)
    x_inverse(jnp.concatenate([dre, dim], axis=-1), 0)
    send_bcol(0)
    x_inverse(jnp.concatenate([re, im], axis=-1), 1)
    send_bcol(1)

    for edge in x_edges():
        edge.wait_recv()
    smooth()
    loaded(10, 11, 12, 13, 14)

    arrived("bcol", 0)
    brow_out[0] = row_product(gy_ref, [lines(bcol_in, 0)])[0].reshape(ROWS, YB, XB)
    send_brow(0)

    dx = damp[0:8]

    arrived("brow", 0)

    def update_x(rows):
        grad = depth_inverse(load(brow_in.at[0], rows))
        fresh = []
        for z in range(NZ):
            change = time_step * coef[0, z, rows, :] * grad[z]
            fresh.append(dx * (dx * vx_ref[z, rows, :] - change))
        store(vxo_ref, rows, fresh)
        store(row_out.at[1], rows, depth_forward(fresh))

    chunks(update_x)
    send_row(1)
    writes[0].start()

    arrived("bcol", 1)
    flow = lines(bcol_in, 1)
    plain, slope = row_product(gy_ref, [flow, y_derivative(flow, 1)])
    brow_out[1] = slope.reshape(ROWS, YB, XB)
    send_brow(1)
    brow_out[2] = plain.reshape(ROWS, YB, XB)
    send_brow(2)

    arrived("row", 1)
    col_out[1] = row_product(fy_ref, [lines(row_in, 1)])[0].reshape(2 * COLS, 2 * SLOTS, XB)
    send_col(1)

    arrived("brow", 1)

    def update_y(rows):
        grad = depth_inverse(load(brow_in.at[1], rows))
        dy = damp[pl.ds(pl.multiple_of(rows.start + 8, 8), 8), :]
        fresh = []
        for z in range(NZ):
            change = time_step * coef[0, z, rows, :] * grad[z]
            fresh.append(dy * (dy * vy_ref[z, rows, :] - change))
        store(vyo_ref, rows, fresh)
        store(row_out.at[2], rows, depth_forward(fresh))

    chunks(update_y)
    send_row(2)
    writes[1].start()

    arrived("brow", 2)

    def update_z(rows):
        grad = depth_inverse(depth_derivative(load(brow_in.at[2], rows), 1))
        fresh = []
        for z in range(NZ):
            fresh.append(vz_ref[z, rows, :] - time_step * coef[0, z, rows, :] * grad[z])
        store(vzo_ref, rows, fresh)
        store(row_out.at[3], rows, depth_derivative(depth_forward(fresh), -1))

    chunks(update_z)
    send_row(3)
    writes[2].start()

    arrived("row", 2)
    arrived("row", 3)
    across, deep = row_product(fy_ref, [lines(row_in, 2), lines(row_in, 3)])
    summed = deep + y_derivative(across, -1)
    col_out[2] = summed.reshape(2 * COLS, 2 * SLOTS, XB)
    send_col(2)

    arrived("col", 1)
    flow_x = x_forward(1)
    tre, tim = x_derivative(flow_x[..., :XB], flow_x[..., XB:], -1)
    arrived("col", 2)
    rest = x_forward(2)
    tre = (tre + rest[..., :XB]) * kappa[...]
    tim = (tim + rest[..., XB:]) * kappa[...]
    x_inverse(jnp.concatenate([tre, tim], axis=-1), 2)
    send_bcol(2)

    arrived("bcol", 2)
    brow_out[3] = row_product(gy_ref, [lines(bcol_in, 2)])[0].reshape(ROWS, YB, XB)
    send_brow(3)

    arrived("brow", 3)

    def update_p(rows):
        divergence = depth_inverse(load(brow_in.at[3], rows))
        both = dx * damp[pl.ds(pl.multiple_of(rows.start + 8, 8), 8), :]
        for z in range(NZ):
            change = time_step * coef[1, z, rows, :] * divergence[z]
            po_ref[z, rows, :] = both * (both * p_ref[z, rows, :] - change)

    chunks(update_p)
    writes[3].start()

    for kind, number in (("row", 4), ("col", 3), ("bcol", 3), ("brow", 4)):
        for f in range(number):
            all_of(kind, f).wait_send()
    for edge in y_edges() + x_edges():
        edge.wait_send()
    for write in writes:
        write.wait()


def write_kernel(a, b, c, d, a_out, b_out, c_out, d_out, held, in_sem, out_sem):
    arrays = ((a, a_out), (b, b_out), (c, c_out), (d, d_out))
    loads = [pltpu.make_async_copy(x, held.at[n], in_sem.at[n]) for n, (x, _) in enumerate(arrays)]
    stores = [pltpu.make_async_copy(held.at[n], y, out_sem.at[n]) for n, (_, y) in enumerate(arrays)]
    for load in loads:
        load.start()
    for load, store in zip(loads, stores):
        load.wait()
        store.start()
    for store in stores:
        store.wait()


def on_device(
    labels, pressure, velocity_x, velocity_y, velocity_z,
    speed_table, density_table, filter_taps, layer_width,
):
    fy, gy, yd = row_tables()
    wx, ux, xt = column_tables()
    brick = jax.ShapeDtypeStruct(pressure.shape, f32)
    row_buffer = lambda n: pltpu.VMEM((n, ROWS, YB, XB), f32)
    col_buffer = lambda n: pltpu.VMEM((n, 2 * COLS, 2 * SLOTS, XB), f32)
    results = pl.pallas_call(
        step_kernel,
        out_shape=(brick,) * 4,
        in_specs=[pl.BlockSpec(memory_space=pl.ANY)] * 15,
        out_specs=(pl.BlockSpec(memory_space=pl.ANY),) * 4,
        scratch_shapes=[
            row_buffer(4), row_buffer(4), col_buffer(3), col_buffer(3),
            col_buffer(3), col_buffer(3), row_buffer(4), row_buffer(4),
            pltpu.VMEM((3, COLS, SLOTS, XB), f32),
            pltpu.VMEM((3, 2, COLS, SLOTS, XB), f32),
            pltpu.VMEM((1, 3, COLS, SLOTS, 2 * XB), f32),
            pltpu.VMEM((2, NZ, YB, XB), f32),
            pltpu.VMEM((NZ, 2 * YB, XB), f32),
            pltpu.VMEM((2, XB, XB), f32),
            pltpu.VMEM((2, XB, XB), f32),
            pltpu.VMEM((NZ * 2 * YB, 2 * XB), f32),
            pltpu.VMEM((2, 2 * XB, 2 * XB), bf16),
            pltpu.VMEM((2, XB, XB), f32),
            pltpu.VMEM((2, 4 * YB, 8 * YB), bf16),
            pltpu.VMEM((8 + YB, XB), f32),
            pltpu.VMEM(labels.shape, jnp.int32),
            *[pltpu.VMEM(pressure.shape, f32)] * 4,
            pltpu.SMEM((LABELS,), f32), pltpu.SMEM((LABELS,), f32),
            pltpu.SMEM((TAPS,), f32), pltpu.SMEM((4,), jnp.int32),
            *[pltpu.VMEM(t.shape, t.dtype) for t in (fy, gy, yd, wx, ux, xt)],
            *[pltpu.VMEM(pressure.shape, f32)] * 4,
            pltpu.SemaphoreType.DMA((18,)),
            pltpu.SemaphoreType.DMA((18,)),
            pltpu.SemaphoreType.DMA((15,)),
            pltpu.SemaphoreType.DMA((4,)),
        ],
        compiler_params=pltpu.CompilerParams(
            collective_id=0, has_side_effects=True, vmem_limit_bytes=VMEM_BYTES
        ),
    )(
        labels, pressure, velocity_x, velocity_y, velocity_z,
        speed_table, density_table, filter_taps, layer_width,
        jnp.asarray(fy), jnp.asarray(gy), jnp.asarray(yd),
        jnp.asarray(wx), jnp.asarray(ux), jnp.asarray(xt),
    )
    return pl.pallas_call(
        write_kernel,
        out_shape=(brick,) * 4,
        in_specs=[pl.BlockSpec(memory_space=pl.ANY)] * 4,
        out_specs=(pl.BlockSpec(memory_space=pl.ANY),) * 4,
        scratch_shapes=[
            pltpu.VMEM((4,) + pressure.shape, f32),
            pltpu.SemaphoreType.DMA((4,)), pltpu.SemaphoreType.DMA((4,)),
        ],
        compiler_params=pltpu.CompilerParams(vmem_limit_bytes=VMEM_BYTES),
    )(*results)


def solution(mesh):
    brick = P(None, "row", "col")
    return jax.shard_map(
        on_device,
        mesh=mesh,
        in_specs=(brick,) * 5 + (P(),) * 4,
        out_specs=(brick,) * 4,
        check_vma=False,
    )
```

```python
import functools
import math

import jax
import jax.numpy as jnp
import numpy as np
from jax import lax
from jax.experimental import pallas as pl
from jax.experimental.pallas import tpu as pltpu
from jax.sharding import PartitionSpec as P

time_step = 0.15
reference_speed = 2.0
absorption = 6.0
MESH = pl.DeviceIdType.MESH

NZ, NY, NX = 16, 512, 2048
ROWS, COLS = 16, 16
YB, XB = NY // ROWS, NX // COLS
SLOTS, HALO = 8, 16
VMEM_BYTES = 67043328
TAPS, LABELS = 33, 12
f32, bf16 = jnp.float32, jnp.bfloat16


def split_table(table):
    high = table.astype(np.float32).astype(bf16)
    low = (table - high.astype(np.float64)).astype(np.float32).astype(bf16)
    return np.stack([high, low])


def row_tables():
    slot = np.arange(NY // 2)
    y = np.arange(NY)
    angle = 2.0 * np.pi * ((slot[:, None] * y[None, :]) % NY) / NY
    real, imag = np.cos(angle), -np.sin(angle)
    imag[0] = np.where(y % 2 == 0, 1.0, -1.0)
    order = lambda t: t.reshape(NY // 2 // SLOTS, SLOTS, NY)
    forward = np.stack([order(real), order(imag)], axis=1).reshape(NY, NY)
    weight = np.where(slot == 0, 1.0, 2.0) / NY
    inverse = np.stack([order(real * weight[:, None]), order(imag * weight[:, None])], axis=1)
    inverse = inverse.reshape(NY, NY).T
    wave = 2.0 * np.pi * slot / NY
    same = -wave * np.sin(0.5 * wave)
    cross = wave * np.cos(0.5 * wave)
    same_imag = same.copy()
    same_imag[0] = -np.pi
    wide = lambda v: np.broadcast_to(v.reshape(-1, SLOTS, 1), (NY // 2 // SLOTS, SLOTS, XB))
    derivative = np.stack([wide(same), wide(same_imag), wide(cross)]).astype(np.float32)
    return split_table(forward), split_table(inverse), derivative


def column_tables():
    x = np.arange(XB)
    angle = 2.0 * np.pi * ((x[:, None] * x[None, :]) % XB) / XB
    c, s = np.cos(angle), np.sin(angle)
    forward = np.block([[c, -s], [s, c]])
    inverse = np.block([[c, s], [-s, c]]) / NX
    kc = np.arange(COLS)
    twist = 2.0 * np.pi * (kc[:, None] * x[None, :]) / NX
    index = kc[:, None] + COLS * x[None, :]
    wave = 2.0 * np.pi * np.where(index < NX // 2, index, index - NX) / NX
    same = wave * np.sin(0.5 * wave)
    cross = wave * np.cos(0.5 * wave)
    small = np.stack([np.cos(twist), np.sin(twist), wave * wave, same, cross]).astype(np.float32)
    return split_table(forward), split_table(inverse), small


def scaled(value, factor):
    if abs(factor - 1.0) < 1e-12:
        return value
    if abs(factor + 1.0) < 1e-12:
        return -value
    return value * np.float32(factor)


def weighted(terms):
    total = None
    for value, factor in terms:
        if abs(factor) < 1e-12:
            continue
        if total is None:
            total = scaled(value, factor)
        elif abs(factor + 1.0) < 1e-12:
            total = total - value
        else:
            total = total + scaled(value, factor)
    return total


def cos16(n):
    return math.cos(2.0 * math.pi * (n % 16) / 16)


def sin16(n):
    return math.sin(2.0 * math.pi * (n % 16) / 16)


def depth_forward(p):
    even = [p[0]] + [p[n] + p[16 - n] for n in range(1, 8)] + [p[8]]
    odd = [None] + [p[n] - p[16 - n] for n in range(1, 8)]
    plus = [even[n] + even[8 - n] for n in range(4)] + [even[4]]
    minus = [even[n] - even[8 - n] for n in range(4)]
    odd_plus = [None] + [odd[n] + odd[8 - n] for n in range(1, 4)] + [odd[4]]
    odd_minus = [None] + [odd[n] - odd[8 - n] for n in range(1, 4)]

    def real_of(k):
        side = plus if k % 2 == 0 else minus
        return weighted([(side[n], cos16(k * n)) for n in range(len(side))])

    def imag_of(k):
        if k % 2 == 0:
            return weighted([(odd_minus[n], -sin16(k * n)) for n in range(1, 4)])
        return weighted([(odd_plus[n], -sin16(k * n)) for n in range(1, 5)])

    out = [real_of(0), real_of(8)]
    for k in range(1, 8):
        out += [real_of(k), imag_of(k)]
    return out


def depth_inverse(m):
    real = [m[0]] + [m[2 * k] for k in range(1, 8)] + [m[1]]
    imag = [None] + [m[2 * k + 1] for k in range(1, 8)]
    weight = [1.0 / 16] + [2.0 / 16] * 7 + [1.0 / 16]

    def terms(values, ids, n, wave):
        return weighted([(values[k], weight[k] * wave(k * n)) for k in ids])

    out = [None] * 16
    for n in range(0, 5):
        ce = terms(real, range(0, 9, 2), n, cos16)
        co = terms(real, range(1, 9, 2), n, cos16)
        so = terms(imag, range(1, 8, 2), n, lambda v: -sin16(v))
        se = terms(imag, range(2, 8, 2), n, lambda v: -sin16(v))
        near = ce if co is None else ce + co
        far = ce if co is None else ce - co
        if n == 0:
            out[0], out[8] = near, far
            continue
        if se is None:
            d_near, d_far = so, so
        else:
            d_near, d_far = so + se, so - se
        out[n], out[16 - n] = near + d_near, near - d_near
        if n < 4:
            out[8 - n], out[8 + n] = far + d_far, far - d_far
    return out


def depth_derivative(m, sign):
    out = [jnp.zeros_like(m[0]), m[1] * np.float32(-sign * math.pi)]
    for k in range(1, 8):
        wave = 2.0 * math.pi * k / 16
        a = np.float32(-sign * wave * math.sin(0.5 * wave))
        b = np.float32(wave * math.cos(0.5 * wave))
        out += [m[2 * k] * a - m[2 * k + 1] * b, m[2 * k + 1] * a + m[2 * k] * b]
    return out


def short_transform(values, sign):
    count = len(values)
    if count == 1:
        return values
    even = short_transform(values[0::2], sign)
    odd = short_transform(values[1::2], sign)
    out = [None] * count
    for k in range(count // 2):
        angle = sign * 2.0 * math.pi * k / count
        c, s = math.cos(angle), math.sin(angle)
        re, im = odd[k]
        if k == 0:
            tr, ti = re, im
        elif abs(c) < 1e-9:
            tr, ti = (-im, re) if s > 0 else (im, -re)
        elif abs(abs(c) - abs(s)) < 1e-9:
            h = np.float32(abs(c))
            cs, ss = (1 if c > 0 else -1), (1 if s > 0 else -1)
            first = re if cs > 0 else -re
            tr = (first - im if ss > 0 else first + im) * h
            second = im if cs > 0 else -im
            ti = (second + re if ss > 0 else second - re) * h
        else:
            tr = re * np.float32(c) - im * np.float32(s)
            ti = re * np.float32(s) + im * np.float32(c)
        er, ei = even[k]
        out[k] = (er + tr, ei + ti)
        out[k + count // 2] = (er - tr, ei - ti)
    return out


def halves(value):
    high = value.astype(bf16)
    low = (value - high.astype(f32)).astype(bf16)
    return high, low


def mm(a, b):
    return jnp.dot(a, b, preferred_element_type=f32)


def step_kernel(
    lab_hbm, p_hbm, vx_hbm, vy_hbm, vz_hbm, speed_hbm, density_hbm, taps_hbm, width_hbm,
    fy_hbm, gy_hbm, yd_hbm, wx_hbm, ux_hbm, xt_hbm,
    po_hbm, vxo_hbm, vyo_hbm, vzo_hbm,
    row_out, row_in, col_out, col_in, bcol_out, bcol_in, brow_out, brow_in,
    kappa, xb, xs, coef, lab, edge_out, edge_in, raw, across, edge_band, down, damp,
    lab_ref, p_ref, vx_ref, vy_ref, vz_ref, speed_ref, density_ref, taps_ref, width_ref,
    fy_ref, gy_ref, yd_ref, wx_ref, ux_ref, xt_ref,
    po_ref, vxo_ref, vyo_ref, vzo_ref,
    send_sem, recv_sem, load_sem, store_sem,
):
    writes = [
        pltpu.make_async_copy(source, target, store_sem.at[n])
        for n, (source, target) in enumerate(
            [(vxo_ref, vxo_hbm), (vyo_ref, vyo_hbm), (vzo_ref, vzo_hbm), (po_ref, po_hbm)]
        )
    ]

    def loaded(*numbers):
        for n in numbers:
            fetches[n].wait()

    r, c = lax.axis_index("row"), lax.axis_index("col")
    j, h = r // 2, r % 2
    q = h * COLS + c

    barrier = pltpu.get_barrier_semaphore()

    x_low, y_chip, core = r // 8, (r // 2) % 4, r % 2
    z_chip, x_high = c // 2, c % 2

    def pick(i, values):
        value = jnp.int32(values[0])
        for n in range(1, len(values)):
            value = jnp.where(i == n, jnp.int32(values[n]), value)
        return value

    def row_partner(i, other):
        x = (x_low + pick(i, (1, 0, 1, 1, 0, 0, 1, 0))) % 2
        y = (y_chip + pick(i, (2, 2, 1, 3, 1, 3, 0, 0))) % 4
        return (x * 4 + y) * 2 + (core + other) % 2

    def plane_partner(i, other):
        z = (z_chip + pick(i, (4, 3, 5, 4, 2, 6, 3, 5, 1, 7, 2, 6, 0, 1, 7, 0))) % 8
        x = (x_high + pick(i, (1, 1, 1, 0, 1, 1, 0, 0, 1, 1, 0, 0, 1, 0, 0, 0))) % 2
        return (core + other) % 2 * COLS + z * 2 + x

    def each_partner(partner, classes, body):
        def step(i, carry):
            body(partner(i, 0))
            body(partner(i, 1))
            return carry

        lax.fori_loop(0, classes - 1, step, 0)
        body(partner(classes - 1, 1))

    def row_device(t):
        return (t, c)

    def plane_device(t):
        return (2 * j + t // COLS, t % COLS)

    def greet(device):
        pl.semaphore_signal(barrier, inc=1, device_id=device, device_id_type=MESH)

    each_partner(plane_partner, COLS, lambda t: greet(plane_device(t)))
    each_partner(row_partner, ROWS // 2, lambda t: greet(row_device(t)))

    fetches = [
        pltpu.make_async_copy(source, target, load_sem.at[n])
        for n, (source, target) in enumerate(
            [
                (p_hbm, p_ref), (lab_hbm, lab_ref), (xt_hbm, xt_ref), (taps_hbm, taps_ref),
                (width_hbm, width_ref), (fy_hbm, fy_ref), (wx_hbm, wx_ref),
                (speed_hbm, speed_ref), (density_hbm, density_ref), (ux_hbm, ux_ref),
                (gy_hbm, gy_ref), (vx_hbm, vx_ref), (yd_hbm, yd_ref), (vy_hbm, vy_ref),
                (vz_hbm, vz_ref),
            ]
        )
    ]
    for fetch in fetches:
        fetch.start()
    def start_all(src, dst, sem, partner, classes, device_of, own):
        def start(t):
            pltpu.make_async_remote_copy(
                src_ref=src.at[t], dst_ref=dst.at[own], send_sem=send_sem.at[sem],
                recv_sem=recv_sem.at[sem], device_id=device_of(t), device_id_type=MESH,
            ).start()

        each_partner(partner, classes, start)
        dst[own] = src[own]

    def row_all(src, dst, sem):
        start_all(src, dst, sem, row_partner, ROWS // 2, row_device, r)

    def plane_all(src, dst, sem):
        start_all(src, dst, sem, plane_partner, COLS, plane_device, q)

    def whole(src, dst, sem, count):
        span = pl.ds(0, count - 1)
        return pltpu.make_async_remote_copy(
            src_ref=src.at[span], dst_ref=dst.at[span], send_sem=send_sem.at[sem],
            recv_sem=recv_sem.at[sem], device_id=((r + 1) % ROWS, c), device_id_type=MESH,
        )

    def send_row(f):
        row_all(row_out.at[f], row_in.at[f], f)

    def send_col(f):
        plane_all(col_out.at[f], col_in.at[f], 4 + f)

    def send_bcol(f):
        plane_all(bcol_out.at[f], bcol_in.at[f], 7 + f)

    def send_brow(f):
        row_all(brow_out.at[f], brow_in.at[f], 10 + f)

    def all_of(kind, f):
        src, dst, base, count = {
            "row": (row_out, row_in, 0, ROWS),
            "col": (col_out, col_in, 4, 2 * COLS),
            "bcol": (bcol_out, bcol_in, 7, 2 * COLS),
            "brow": (brow_out, brow_in, 10, ROWS),
        }[kind]
        return whole(src.at[f], dst.at[f], base + f, count)

    def arrived(kind, f):
        all_of(kind, f).wait_recv()

    def load(ref, rows):
        return [ref[z, rows, :] for z in range(NZ)]

    def store(ref, rows, planes):
        for z in range(NZ):
            ref[z, rows, :] = planes[z]

    def chunks(body):
        def step(i, carry):
            body(pl.ds(pl.multiple_of(i * 8, 8), 8))
            return carry

        lax.fori_loop(0, YB // 8, step, 0)

    def pressure_planes(rows):
        store(row_out.at[0], rows, depth_forward(load(p_ref, rows)))

    loaded(0)
    chunks(pressure_planes)
    pl.semaphore_wait(barrier, ROWS - 1 + 2 * COLS - 1)
    send_row(0)

    loaded(1)
    for z in range(NZ):
        lab[z, HALO : HALO + YB, :] = lab_ref[z].astype(f32)

    def y_edges():
        before, after = (r + ROWS - 1) % ROWS, (r + 1) % ROWS
        return [
            pltpu.make_async_remote_copy(
                src_ref=lab.at[:, pl.ds(HALO, HALO), :],
                dst_ref=lab.at[:, pl.ds(HALO + YB, HALO), :],
                send_sem=send_sem.at[14], recv_sem=recv_sem.at[14],
                device_id=(before, c), device_id_type=MESH,
            ),
            pltpu.make_async_remote_copy(
                src_ref=lab.at[:, pl.ds(YB, HALO), :],
                dst_ref=lab.at[:, pl.ds(0, HALO), :],
                send_sem=send_sem.at[15], recv_sem=recv_sem.at[15],
                device_id=(after, c), device_id_type=MESH,
            ),
        ]

    def x_edges():
        before, after = (c + COLS - 1) % COLS, (c + 1) % COLS
        return [
            pltpu.make_async_remote_copy(
                src_ref=edge_out.at[0], dst_ref=edge_in.at[1],
                send_sem=send_sem.at[16], recv_sem=recv_sem.at[16],
                device_id=(r, before), device_id_type=MESH,
            ),
            pltpu.make_async_remote_copy(
                src_ref=edge_out.at[1], dst_ref=edge_in.at[0],
                send_sem=send_sem.at[17], recv_sem=recv_sem.at[17],
                device_id=(r, after), device_id_type=MESH,
            ),
        ]

    def ids(shape, dim):
        return lax.broadcasted_iota(jnp.int32, shape, dim)

    def banded(offset):
        def tap(t, total):
            return jnp.where(offset == t, taps_ref[t], total)

        return lax.fori_loop(0, TAPS, tap, jnp.zeros(offset.shape, f32), unroll=3)

    def fill_bands():
        wide = (XB, XB)
        band = banded(ids(wide, 0) - ids(wide, 1) + HALO)
        none = jnp.zeros(wide, bf16)
        for part, value in enumerate(halves(band)):
            top_rows = jnp.concatenate([value, none], axis=1)
            low_rows = jnp.concatenate([none, value], axis=1)
            across[part] = jnp.concatenate([top_rows, low_rows], axis=0)
        edge_band[0] = banded(ids(wide, 0) % HALO - ids(wide, 1))
        edge_band[1] = banded(ids(wide, 0) % HALO - ids(wide, 1) + XB + HALO)
        tall = (4 * YB, 8 * YB)
        row, line = ids(tall, 0), ids(tall, 1)
        offset = jnp.where(row // YB == line // (2 * YB), line % (2 * YB) - row % YB, -1)
        for part, value in enumerate(halves(banded(offset))):
            down[part] = value

    def fill_damping():
        def absorb(position, length, low_width, high_width):
            size = position.shape
            low_side = jnp.maximum(low_width - position, 0).astype(f32)
            high_side = jnp.maximum(position - (length - 1 - high_width), 0).astype(f32)
            low_side = low_side / jnp.full(size, low_width, jnp.int32).astype(f32)
            high_side = high_side / jnp.full(size, high_width, jnp.int32).astype(f32)
            low_side, high_side = low_side * low_side, high_side * high_side
            total = low_side * low_side + high_side * high_side
            return jnp.exp((-0.5 * time_step * absorption * reference_speed) * total)

        damp[0:8] = absorb(c * XB + ids((8, XB), 1), NX, width_ref[0], width_ref[1])
        damp[8:] = absorb(r * YB + ids((YB, XB), 0), NY, width_ref[2], width_ref[3])

    def pack_edges():
        wide = (XB, XB)
        source, target = ids(wide, 0), ids(wide, 1)
        total = None
        for g in range(8):
            here = target // HALO == g
            first_lanes = here & (source == target % HALO)
            last_lanes = here & (source == target % HALO + XB - HALO)
            select = jnp.concatenate(
                [jnp.where(first_lanes, 1.0, 0.0), jnp.where(last_lanes, 1.0, 0.0)], axis=1
            ).astype(bf16)
            part = mm(lab[2 * g : 2 * g + 2].reshape(XB, XB).astype(bf16), select)
            total = part if total is None else total + part
        edge_out[0] = total[:, :XB]
        edge_out[1] = total[:, XB:]

    def tables():
        density = [jnp.full((8, XB), density_ref[n], f32) for n in range(LABELS)]
        speed = [jnp.full((8, XB), speed_ref[n], f32) for n in range(LABELS)]
        return [1.0 / d for d in density], [d * s * s for d, s in zip(density, speed)]

    def look_up(label, table):
        value = jnp.broadcast_to(table[0][None], label.shape)
        for n in range(1, LABELS):
            value = jnp.where(label == float(n), table[n][None], value)
        return value

    def fill_raw():
        buoyancy_of, modulus_of = tables()

        def plane(z, carry):
            label = lab[z].reshape(8, 8, XB)
            rows = pl.ds(pl.multiple_of(z * 2 * YB, 2 * YB), 2 * YB)
            raw[rows, :XB] = look_up(label, buoyancy_of).reshape(2 * YB, XB)
            raw[rows, XB:] = look_up(label, modulus_of).reshape(2 * YB, XB)
            return carry

        lax.fori_loop(0, NZ, plane, 0)

    def smooth():
        buoyancy_of, modulus_of = tables()
        edges = [edge_in[0].reshape(16, 8, XB), edge_in[1].reshape(16, 8, XB)]
        sides = [
            halves(jnp.concatenate([look_up(e, t).reshape(XB, XB) for e in edges], axis=1))
            for t in (buoyancy_of, modulus_of)
        ]
        group_of = ids((XB, XB), 0) // HALO

        def quarter(i, carry):
            rows = pl.ds(pl.multiple_of(i * 8 * YB, 8 * YB), 8 * YB)
            high, low_part = halves(raw[rows, :])
            main = mm(high, across[0]) + mm(low_part, across[0]) + mm(high, across[1])
            parts = []
            for g in range(2):
                inside = group_of == 2 * i + g
                parts.append(
                    jnp.concatenate(
                        [jnp.where(inside, edge_band[s], 0.0) for s in range(2)], axis=0
                    )
                )
            high, low_part = halves(jnp.concatenate(parts, axis=1))
            columns = []
            for side_high, side_low in sides:
                out = mm(side_high, high) + mm(side_low, high) + mm(side_high, low_part)
                columns.append(jnp.concatenate([out[:, :XB], out[:, XB:]], axis=0))
            high, low_part = halves(main + jnp.concatenate(columns, axis=1))
            out = mm(down[0], high) + mm(down[0], low_part) + mm(down[1], high)
            planes = pl.ds(i * 4, 4)
            coef[0, planes] = out[:, :XB].reshape(4, YB, XB)
            coef[1, planes] = out[:, XB:].reshape(4, YB, XB)
            return carry

        lax.fori_loop(0, 4, quarter, 0)

    lane_rows = lax.broadcasted_iota(jnp.int32, (SLOTS, XB), 0)
    slot = q * SLOTS + lane_rows
    one, zero = jnp.ones((SLOTS, XB), f32), jnp.zeros((SLOTS, XB), f32)
    first = jnp.where(slot == 0, one, zero)
    flat = jnp.where(jnp.full((SLOTS, XB), j, jnp.int32) == 0, one, zero)
    general = (1.0 - first) * (1.0 - flat)
    half_general = 0.5 * general
    first_deep = first * (1.0 - flat)
    first_flat = first * flat
    rest_flat = flat * (1.0 - first)
    own_imag = first_deep + rest_flat
    not_first = 1.0 - first
    not_flat = 1.0 - flat

    pi2 = np.float32(math.pi * math.pi)
    ky = slot.astype(f32) * np.float32(2.0 * math.pi / NY)
    kz = jnp.full((SLOTS, XB), j, jnp.int32).astype(f32) * np.float32(2.0 * math.pi / NZ)
    low = ky * ky + kz * kz
    top = low + pi2 * (first_deep + flat)
    extra = pi2 + jnp.where(lane_rows == 0, zero, pi2 * one)
    scale = np.float32((0.5 * reference_speed * time_step) ** 2)

    def fill_kappa(kc, carry):
        kx2 = xt_ref[2, pl.ds(kc, 1), :]
        for g, part in enumerate((low, top, extra)):
            v2 = scale * (kx2 + part)
            series = 1.0 + v2 * np.float32(-1.0 / 110.0)
            series = 1.0 + v2 * np.float32(-1.0 / 72.0) * series
            series = 1.0 + v2 * np.float32(-1.0 / 42.0) * series
            series = 1.0 + v2 * np.float32(-1.0 / 20.0) * series
            kappa[g, kc] = 1.0 + v2 * np.float32(-1.0 / 6.0) * series
        return carry

    loaded(2)
    lax.fori_loop(0, COLS, fill_kappa, 0)

    for edge in y_edges():
        edge.start()
    loaded(3, 4)
    fill_bands()
    fill_damping()

    def lines(ref, f):
        return ref[f].reshape(NY, XB)

    def row_product(table, values):
        parts = [halves(v) for v in values]
        high = [part[0] for part in parts]
        low_part = [part[1] for part in parts]
        if len(values) == 1:
            both = mm(table[0], jnp.concatenate([high[0], low_part[0]], axis=1))
            return [both[:, :XB] + both[:, XB:] + mm(table[1], high[0])]
        high = jnp.concatenate(high, axis=1)
        low_part = jnp.concatenate(low_part, axis=1)
        result = mm(table[0], high) + mm(table[0], low_part) + mm(table[1], high)
        return [result[:, :XB], result[:, XB:]]

    def y_derivative(value, sign):
        parts = value.reshape(NY // 2 // SLOTS, 2, SLOTS, XB)
        re, im = parts[:, 0], parts[:, 1]
        same, same_imag, cross = yd_ref[0], yd_ref[1], yd_ref[2]
        if sign > 0:
            out = [re * same - im * cross, im * same_imag + re * cross]
        else:
            out = [-(re * same + im * cross), re * cross - im * same_imag]
        return jnp.stack(out, axis=1).reshape(NY, XB)

    def x_forward(f):
        for n in range(COLS):
            rr, ri = col_in[f, n, 0:8, :], col_in[f, n, 8:16, :]
            ir, ii = col_in[f, COLS + n, 0:8, :], col_in[f, COLS + n, 8:16, :]
            xb[0, 0, n] = rr - general * ii
            xb[0, 1, n] = not_first * ri + not_flat * ir
            xb[1, 0, n] = general * (rr + ii) + first_deep * ri + flat * ir
            xb[1, 1, n] = general * (ir - ri) + own_imag * ii
            xb[2, 0, n] = first_flat * ri + pltpu.roll(first_flat * ii, 1, 0)
            xb[2, 1, n] = zero

        def group(g, carry):
            values = [(xb[g, 0, n], xb[g, 1, n]) for n in range(COLS)]
            values = short_transform(values, -1.0)
            for kc in range(COLS):
                re, im = values[kc]
                cs, sn = xt_ref[0, kc : kc + 1, :], xt_ref[1, kc : kc + 1, :]
                xs[0, g, kc, :, :XB] = re * cs + im * sn
                xs[0, g, kc, :, XB:] = im * cs - re * sn
            return carry

        lax.fori_loop(0, 3, group, 0)
        high, low_part = halves(xs[0].reshape(3 * COLS * SLOTS, 2 * XB))
        out = mm(high, wx_ref[0]) + mm(low_part, wx_ref[0]) + mm(high, wx_ref[1])
        return out.reshape(3, COLS, SLOTS, 2 * XB)

    def x_derivative(re, im, sign):
        same = xt_ref[3][None, :, None, :]
        cross = xt_ref[4][None, :, None, :]
        if sign > 0:
            return -(re * same + im * cross), re * cross - im * same
        return re * same - im * cross, im * same + re * cross

    def x_inverse(value, f):
        high, low_part = halves(value.reshape(3 * COLS * SLOTS, 2 * XB))
        out = mm(high, ux_ref[0]) + mm(low_part, ux_ref[0]) + mm(high, ux_ref[1])
        xs[0] = out.reshape(3, COLS, SLOTS, 2 * XB)

        def group(g, carry):
            values = []
            for kc in range(COLS):
                re, im = xs[0, g, kc, :, :XB], xs[0, g, kc, :, XB:]
                cs, sn = xt_ref[0, kc : kc + 1, :], xt_ref[1, kc : kc + 1, :]
                values.append((re * cs - im * sn, im * cs + re * sn))
            values = short_transform(values, 1.0)
            for n in range(COLS):
                xb[g, 0, n] = values[n][0]
                xb[g, 1, n] = values[n][1]
            return carry

        lax.fori_loop(0, 3, group, 0)
        for n in range(COLS):
            lr, li = xb[0, 0, n], xb[0, 1, n]
            hr, hi = xb[1, 0, n], xb[1, 1, n]
            xr = xb[2, 0, n]
            bcol_out[f, n, 0:8, :] = lr + half_general * (hr - lr)
            bcol_out[f, n, 8:16, :] = (
                half_general * (li - hi) + first_deep * hr + rest_flat * li + first_flat * xr
            )
            bcol_out[f, COLS + n, 0:8, :] = half_general * (li + hi) + first_deep * li + flat * hr
            bcol_out[f, COLS + n, 8:16, :] = (
                half_general * (hr - lr) + own_imag * hi + first_flat * pltpu.roll(xr, 7, 0)
            )

    loaded(5)
    arrived("row", 0)
    col_out[0] = row_product(fy_ref, [lines(row_in, 0)])[0].reshape(2 * COLS, 2 * SLOTS, XB)
    send_col(0)

    for edge in y_edges():
        edge.wait_recv()
    pack_edges()
    for edge in x_edges():
        edge.start()
    loaded(7, 8)
    fill_raw()

    loaded(6, 9)
    arrived("col", 0)
    spectrum = x_forward(0)
    re, im = spectrum[..., :XB] * kappa[...], spectrum[..., XB:] * kappa[...]
    dre, dim = x_derivative(re, im, 1)
    x_inverse(jnp.concatenate([dre, dim], axis=-1), 0)
    send_bcol(0)
    x_inverse(jnp.concatenate([re, im], axis=-1), 1)
    send_bcol(1)

    for edge in x_edges():
        edge.wait_recv()
    smooth()
    loaded(10, 11, 12, 13, 14)

    arrived("bcol", 0)
    brow_out[0] = row_product(gy_ref, [lines(bcol_in, 0)])[0].reshape(ROWS, YB, XB)
    send_brow(0)

    dx = damp[0:8]

    arrived("brow", 0)

    def update_x(rows):
        grad = depth_inverse(load(brow_in.at[0], rows))
        fresh = []
        for z in range(NZ):
            change = time_step * coef[0, z, rows, :] * grad[z]
            fresh.append(dx * (dx * vx_ref[z, rows, :] - change))
        store(vxo_ref, rows, fresh)
        store(row_out.at[1], rows, depth_forward(fresh))

    chunks(update_x)
    send_row(1)
    writes[0].start()

    arrived("bcol", 1)
    flow = lines(bcol_in, 1)
    plain, slope = row_product(gy_ref, [flow, y_derivative(flow, 1)])
    brow_out[1] = slope.reshape(ROWS, YB, XB)
    send_brow(1)
    brow_out[2] = plain.reshape(ROWS, YB, XB)
    send_brow(2)

    arrived("row", 1)
    col_out[1] = row_product(fy_ref, [lines(row_in, 1)])[0].reshape(2 * COLS, 2 * SLOTS, XB)
    send_col(1)

    arrived("brow", 1)

    def update_y(rows):
        grad = depth_inverse(load(brow_in.at[1], rows))
        dy = damp[pl.ds(pl.multiple_of(rows.start + 8, 8), 8), :]
        fresh = []
        for z in range(NZ):
            change = time_step * coef[0, z, rows, :] * grad[z]
            fresh.append(dy * (dy * vy_ref[z, rows, :] - change))
        store(vyo_ref, rows, fresh)
        store(row_out.at[2], rows, depth_forward(fresh))

    chunks(update_y)
    send_row(2)
    writes[1].start()

    arrived("brow", 2)

    def update_z(rows):
        grad = depth_inverse(depth_derivative(load(brow_in.at[2], rows), 1))
        fresh = []
        for z in range(NZ):
            fresh.append(vz_ref[z, rows, :] - time_step * coef[0, z, rows, :] * grad[z])
        store(vzo_ref, rows, fresh)
        store(row_out.at[3], rows, depth_derivative(depth_forward(fresh), -1))

    chunks(update_z)
    send_row(3)
    writes[2].start()

    arrived("row", 2)
    arrived("row", 3)
    across, deep = row_product(fy_ref, [lines(row_in, 2), lines(row_in, 3)])
    summed = deep + y_derivative(across, -1)
    col_out[2] = summed.reshape(2 * COLS, 2 * SLOTS, XB)
    send_col(2)

    arrived("col", 1)
    flow_x = x_forward(1)
    tre, tim = x_derivative(flow_x[..., :XB], flow_x[..., XB:], -1)
    arrived("col", 2)
    rest = x_forward(2)
    tre = (tre + rest[..., :XB]) * kappa[...]
    tim = (tim + rest[..., XB:]) * kappa[...]
    x_inverse(jnp.concatenate([tre, tim], axis=-1), 2)
    send_bcol(2)

    arrived("bcol", 2)
    brow_out[3] = row_product(gy_ref, [lines(bcol_in, 2)])[0].reshape(ROWS, YB, XB)
    send_brow(3)

    arrived("brow", 3)

    def update_p(rows):
        divergence = depth_inverse(load(brow_in.at[3], rows))
        both = dx * damp[pl.ds(pl.multiple_of(rows.start + 8, 8), 8), :]
        for z in range(NZ):
            change = time_step * coef[1, z, rows, :] * divergence[z]
            po_ref[z, rows, :] = both * (both * p_ref[z, rows, :] - change)

    chunks(update_p)
    writes[3].start()

    for kind, number in (("row", 4), ("col", 3), ("bcol", 3), ("brow", 4)):
        for f in range(number):
            all_of(kind, f).wait_send()
    for edge in y_edges() + x_edges():
        edge.wait_send()
    for write in writes:
        write.wait()


def write_kernel(a, b, c, d, a_out, b_out, c_out, d_out, held, in_sem, out_sem):
    arrays = ((a, a_out), (b, b_out), (c, c_out), (d, d_out))
    loads = [pltpu.make_async_copy(x, held.at[n], in_sem.at[n]) for n, (x, _) in enumerate(arrays)]
    stores = [pltpu.make_async_copy(held.at[n], y, out_sem.at[n]) for n, (_, y) in enumerate(arrays)]
    for load in loads:
        load.start()
    for load, store in zip(loads, stores):
        load.wait()
        store.start()
    for store in stores:
        store.wait()


def on_device(
    labels, pressure, velocity_x, velocity_y, velocity_z,
    speed_table, density_table, filter_taps, layer_width,
):
    fy, gy, yd = row_tables()
    wx, ux, xt = column_tables()
    brick = jax.ShapeDtypeStruct(pressure.shape, f32)
    row_buffer = lambda n: pltpu.VMEM((n, ROWS, YB, XB), f32)
    col_buffer = lambda n: pltpu.VMEM((n, 2 * COLS, 2 * SLOTS, XB), f32)
    results = pl.pallas_call(
        step_kernel,
        out_shape=(brick,) * 4,
        in_specs=[pl.BlockSpec(memory_space=pl.ANY)] * 15,
        out_specs=(pl.BlockSpec(memory_space=pl.ANY),) * 4,
        scratch_shapes=[
            row_buffer(4), row_buffer(4), col_buffer(3), col_buffer(3),
            col_buffer(3), col_buffer(3), row_buffer(4), row_buffer(4),
            pltpu.VMEM((3, COLS, SLOTS, XB), f32),
            pltpu.VMEM((3, 2, COLS, SLOTS, XB), f32),
            pltpu.VMEM((1, 3, COLS, SLOTS, 2 * XB), f32),
            pltpu.VMEM((2, NZ, YB, XB), f32),
            pltpu.VMEM((NZ, 2 * YB, XB), f32),
            pltpu.VMEM((2, XB, XB), f32),
            pltpu.VMEM((2, XB, XB), f32),
            pltpu.VMEM((NZ * 2 * YB, 2 * XB), f32),
            pltpu.VMEM((2, 2 * XB, 2 * XB), bf16),
            pltpu.VMEM((2, XB, XB), f32),
            pltpu.VMEM((2, 4 * YB, 8 * YB), bf16),
            pltpu.VMEM((8 + YB, XB), f32),
            pltpu.VMEM(labels.shape, jnp.int32),
            *[pltpu.VMEM(pressure.shape, f32)] * 4,
            pltpu.SMEM((LABELS,), f32), pltpu.SMEM((LABELS,), f32),
            pltpu.SMEM((TAPS,), f32), pltpu.SMEM((4,), jnp.int32),
            *[pltpu.VMEM(t.shape, t.dtype) for t in (fy, gy, yd, wx, ux, xt)],
            *[pltpu.VMEM(pressure.shape, f32)] * 4,
            pltpu.SemaphoreType.DMA((18,)),
            pltpu.SemaphoreType.DMA((18,)),
            pltpu.SemaphoreType.DMA((15,)),
            pltpu.SemaphoreType.DMA((4,)),
        ],
        compiler_params=pltpu.CompilerParams(
            collective_id=0, has_side_effects=True, vmem_limit_bytes=VMEM_BYTES
        ),
    )(
        labels, pressure, velocity_x, velocity_y, velocity_z,
        speed_table, density_table, filter_taps, layer_width,
        jnp.asarray(fy), jnp.asarray(gy), jnp.asarray(yd),
        jnp.asarray(wx), jnp.asarray(ux), jnp.asarray(xt),
    )
    return pl.pallas_call(
        write_kernel,
        out_shape=(brick,) * 4,
        in_specs=[pl.BlockSpec(memory_space=pl.ANY)] * 4,
        out_specs=(pl.BlockSpec(memory_space=pl.ANY),) * 4,
        scratch_shapes=[
            pltpu.VMEM((4,) + pressure.shape, f32),
            pltpu.SemaphoreType.DMA((4,)), pltpu.SemaphoreType.DMA((4,)),
        ],
        compiler_params=pltpu.CompilerParams(vmem_limit_bytes=VMEM_BYTES),
    )(*results)


def solution(mesh):
    brick = P(None, "row", "col")
    return jax.shard_map(
        on_device,
        mesh=mesh,
        in_specs=(brick,) * 5 + (P(),) * 4,
        out_specs=(brick,) * 4,
        check_vma=False,
    )
```

```python
import functools
import math

import jax
import jax.numpy as jnp
import numpy as np
from jax import lax
from jax.experimental import pallas as pl
from jax.experimental.pallas import tpu as pltpu
from jax.sharding import PartitionSpec as P

time_step = 0.15
reference_speed = 2.0
absorption = 6.0
MESH = pl.DeviceIdType.MESH

NZ, NY, NX = 16, 512, 2048
ROWS, COLS = 16, 16
YB, XB = NY // ROWS, NX // COLS
SLOTS, HALO = 4, 16
CHUNK = 2 * COLS * SLOTS
VMEM_BYTES = 67043328
TAPS, LABELS = 33, 12
f32, bf16 = jnp.float32, jnp.bfloat16


def split_table(table):
    high = table.astype(np.float32).astype(bf16)
    low = (table - high.astype(np.float64)).astype(np.float32).astype(bf16)
    return np.stack([high, low])


def row_tables():
    slot = np.arange(NY // 2)
    y = np.arange(NY)
    angle = 2.0 * np.pi * ((slot[:, None] * y[None, :]) % NY) / NY
    real, imag = np.cos(angle), -np.sin(angle)
    imag[0] = np.where(y % 2 == 0, 1.0, -1.0)

    def order(a, b):
        pair = [t.reshape((2 * 2 * COLS, SLOTS) + t.shape[1:]) for t in (a, b)]
        return np.stack(pair, axis=1)

    forward = order(real, imag).reshape(NY, NY)
    weight = np.where(slot == 0, 1.0, 2.0)[:, None] / NY
    inverse = order(real * weight, imag * weight).reshape(NY, NY).T
    wave = 2.0 * np.pi * slot / NY
    same = -wave * np.sin(0.5 * wave)
    cross = wave * np.cos(0.5 * wave)
    same_imag = same.copy()
    same_imag[0] = -np.pi
    tables = [order(same, same_imag), order(-cross, cross)]
    wide = [np.broadcast_to(t.reshape(-1, 2 * SLOTS, 1), (NY // 8, 8, XB)) for t in tables]
    return split_table(forward), split_table(inverse), np.stack(wide).astype(np.float32)


def column_tables():
    x = np.arange(XB)
    angle = 2.0 * np.pi * ((x[:, None] * x[None, :]) % XB) / XB
    c, s = np.cos(angle), np.sin(angle)
    forward = np.block([[c, -s], [s, c]])
    inverse = np.block([[c, s], [-s, c]]) / NX
    kc = np.arange(COLS)
    twist = 2.0 * np.pi * (kc[:, None] * x[None, :]) / NX
    index = kc[:, None] + COLS * x[None, :]
    wave = 2.0 * np.pi * np.where(index < NX // 2, index, index - NX) / NX
    same = wave * np.sin(0.5 * wave)
    cross = wave * np.cos(0.5 * wave)
    small = np.stack([np.cos(twist), np.sin(twist), wave * wave, same, cross]).astype(np.float32)
    return split_table(forward), split_table(inverse), small


def scaled(value, factor):
    if abs(factor - 1.0) < 1e-12:
        return value
    if abs(factor + 1.0) < 1e-12:
        return -value
    return value * np.float32(factor)


def weighted(terms):
    total = None
    for value, factor in terms:
        if abs(factor) < 1e-12:
            continue
        if total is None:
            total = scaled(value, factor)
        elif abs(factor + 1.0) < 1e-12:
            total = total - value
        else:
            total = total + scaled(value, factor)
    return total


def cos16(n):
    return math.cos(2.0 * math.pi * (n % 16) / 16)


def sin16(n):
    return math.sin(2.0 * math.pi * (n % 16) / 16)


def depth_forward(p):
    even = [p[0]] + [p[n] + p[16 - n] for n in range(1, 8)] + [p[8]]
    odd = [None] + [p[n] - p[16 - n] for n in range(1, 8)]
    plus = [even[n] + even[8 - n] for n in range(4)] + [even[4]]
    minus = [even[n] - even[8 - n] for n in range(4)]
    odd_plus = [None] + [odd[n] + odd[8 - n] for n in range(1, 4)] + [odd[4]]
    odd_minus = [None] + [odd[n] - odd[8 - n] for n in range(1, 4)]

    def real_of(k):
        side = plus if k % 2 == 0 else minus
        return weighted([(side[n], cos16(k * n)) for n in range(len(side))])

    def imag_of(k):
        if k % 2 == 0:
            return weighted([(odd_minus[n], -sin16(k * n)) for n in range(1, 4)])
        return weighted([(odd_plus[n], -sin16(k * n)) for n in range(1, 5)])

    out = [real_of(0), real_of(8)]
    for k in range(1, 8):
        out += [real_of(k), imag_of(k)]
    return out


def depth_inverse(m):
    real = [m[0]] + [m[2 * k] for k in range(1, 8)] + [m[1]]
    imag = [None] + [m[2 * k + 1] for k in range(1, 8)]
    weight = [1.0 / 16] + [2.0 / 16] * 7 + [1.0 / 16]

    def terms(values, ids, n, wave):
        return weighted([(values[k], weight[k] * wave(k * n)) for k in ids])

    out = [None] * 16
    for n in range(0, 5):
        ce = terms(real, range(0, 9, 2), n, cos16)
        co = terms(real, range(1, 9, 2), n, cos16)
        so = terms(imag, range(1, 8, 2), n, lambda v: -sin16(v))
        se = terms(imag, range(2, 8, 2), n, lambda v: -sin16(v))
        near = ce if co is None else ce + co
        far = ce if co is None else ce - co
        if n == 0:
            out[0], out[8] = near, far
            continue
        if se is None:
            d_near, d_far = so, so
        else:
            d_near, d_far = so + se, so - se
        out[n], out[16 - n] = near + d_near, near - d_near
        if n < 4:
            out[8 - n], out[8 + n] = far + d_far, far - d_far
    return out


def depth_derivative(m, sign):
    out = [jnp.zeros_like(m[0]), m[1] * np.float32(-sign * math.pi)]
    for k in range(1, 8):
        wave = 2.0 * math.pi * k / 16
        a = np.float32(-sign * wave * math.sin(0.5 * wave))
        b = np.float32(wave * math.cos(0.5 * wave))
        out += [m[2 * k] * a - m[2 * k + 1] * b, m[2 * k + 1] * a + m[2 * k] * b]
    return out


def short_transform(values, sign):
    count = len(values)
    if count == 1:
        return values
    even = short_transform(values[0::2], sign)
    odd = short_transform(values[1::2], sign)
    out = [None] * count
    for k in range(count // 2):
        angle = sign * 2.0 * math.pi * k / count
        c, s = math.cos(angle), math.sin(angle)
        re, im = odd[k]
        if k == 0:
            tr, ti = re, im
        elif abs(c) < 1e-9:
            tr, ti = (-im, re) if s > 0 else (im, -re)
        elif abs(abs(c) - abs(s)) < 1e-9:
            h = np.float32(abs(c))
            cs, ss = (1 if c > 0 else -1), (1 if s > 0 else -1)
            first = re if cs > 0 else -re
            tr = (first - im if ss > 0 else first + im) * h
            second = im if cs > 0 else -im
            ti = (second + re if ss > 0 else second - re) * h
        else:
            tr = re * np.float32(c) - im * np.float32(s)
            ti = re * np.float32(s) + im * np.float32(c)
        er, ei = even[k]
        out[k] = (er + tr, ei + ti)
        out[k + count // 2] = (er - tr, ei - ti)
    return out


def halves(value):
    high = value.astype(bf16)
    low = (value - high.astype(f32)).astype(bf16)
    return high, low


def mm(a, b):
    return jnp.dot(a, b, preferred_element_type=f32)


def step_kernel(
    lab_hbm, p_hbm, vx_hbm, vy_hbm, vz_hbm, speed_hbm, density_hbm, taps_hbm, width_hbm,
    fy_hbm, gy_hbm, yd_hbm, wx_hbm, ux_hbm, xt_hbm,
    po_hbm, vxo_hbm, vyo_hbm, vzo_hbm,
    row_out, row_in, col_out, col_in, bcol_out, bcol_in, brow_out, brow_in,
    kappa, xb, xs, coef, lab, edge_out, edge_in, raw, across, edge_band, down, damp,
    lab_ref, p_ref, vx_ref, vy_ref, vz_ref, speed_ref, density_ref, taps_ref, width_ref,
    fy_ref, gy_ref, yd_ref, wx_ref, ux_ref, xt_ref,
    po_ref, vxo_ref, vyo_ref, vzo_ref,
    send_sem, recv_sem, load_sem, store_sem,
):
    writes = [
        pltpu.make_async_copy(source, target, store_sem.at[n])
        for n, (source, target) in enumerate(
            [(vxo_ref, vxo_hbm), (vyo_ref, vyo_hbm), (vzo_ref, vzo_hbm), (po_ref, po_hbm)]
        )
    ]

    def loaded(*numbers):
        for n in numbers:
            fetches[n].wait()

    r, c = lax.axis_index("row"), lax.axis_index("col")
    j, h = r // 2, r % 2
    q = h * COLS + c

    barrier = pltpu.get_barrier_semaphore()

    x_low, y_chip, core = r // 8, (r // 2) % 4, r % 2
    z_chip, x_high = c // 2, c % 2

    def pick(i, values):
        value = jnp.int32(values[0])
        for n in range(1, len(values)):
            value = jnp.where(i == n, jnp.int32(values[n]), value)
        return value

    def row_partner(i, other):
        x = (x_low + pick(i, (1, 0, 1, 1, 0, 0, 1, 0))) % 2
        y = (y_chip + pick(i, (2, 2, 1, 3, 1, 3, 0, 0))) % 4
        return (x * 4 + y) * 2 + (core + other) % 2

    def plane_partner(i, other):
        z = (z_chip + pick(i, (4, 3, 5, 4, 2, 6, 3, 5, 1, 7, 2, 6, 0, 1, 7, 0))) % 8
        x = (x_high + pick(i, (1, 1, 1, 0, 1, 1, 0, 0, 1, 1, 0, 0, 1, 0, 0, 0))) % 2
        return (core + other) % 2 * COLS + z * 2 + x

    def each_partner(partner, classes, body):
        def step(i, carry):
            body(partner(i, 0))
            body(partner(i, 1))
            return carry

        lax.fori_loop(0, classes - 1, step, 0)
        body(partner(classes - 1, 1))

    def row_device(t):
        return (t, c)

    def plane_device(t):
        return (2 * j + t // COLS, t % COLS)

    def greet(device):
        pl.semaphore_signal(barrier, inc=1, device_id=device, device_id_type=MESH)

    each_partner(plane_partner, COLS, lambda t: greet(plane_device(t)))
    each_partner(row_partner, ROWS // 2, lambda t: greet(row_device(t)))

    fetches = [
        pltpu.make_async_copy(source, target, load_sem.at[n])
        for n, (source, target) in enumerate(
            [
                (p_hbm, p_ref), (lab_hbm, lab_ref), (xt_hbm, xt_ref), (taps_hbm, taps_ref),
                (width_hbm, width_ref), (fy_hbm, fy_ref), (wx_hbm, wx_ref),
                (speed_hbm, speed_ref), (density_hbm, density_ref), (ux_hbm, ux_ref),
                (gy_hbm, gy_ref), (vx_hbm, vx_ref), (yd_hbm, yd_ref), (vy_hbm, vy_ref),
                (vz_hbm, vz_ref),
            ]
        )
    ]
    for fetch in fetches:
        fetch.start()
    def start_all(src, dst, sem, partner, classes, device_of, own):
        def start(t):
            pltpu.make_async_remote_copy(
                src_ref=src.at[t], dst_ref=dst.at[own], send_sem=send_sem.at[sem],
                recv_sem=recv_sem.at[sem], device_id=device_of(t), device_id_type=MESH,
            ).start()

        each_partner(partner, classes, start)
        dst[own] = src[own]

    def row_all(src, dst, sem):
        start_all(src, dst, sem, row_partner, ROWS // 2, row_device, r)

    def plane_all(src, dst, sem):
        start_all(src, dst, sem, plane_partner, COLS, plane_device, q)

    def whole(src, dst, sem, count):
        span = pl.ds(0, count - 1)
        return pltpu.make_async_remote_copy(
            src_ref=src.at[span], dst_ref=dst.at[span], send_sem=send_sem.at[sem],
            recv_sem=recv_sem.at[sem], device_id=((r + 1) % ROWS, c), device_id_type=MESH,
        )

    def send_row(f):
        row_all(row_out.at[f], row_in.at[f], f)

    def send_col(f, u):
        plane_all(col_out.at[f, u], col_in.at[f, u], 4 + 2 * f + u)

    def send_bcol(f, u):
        plane_all(bcol_out.at[f, u], bcol_in.at[f, u], 10 + 2 * f + u)

    def send_brow(f):
        row_all(brow_out.at[f], brow_in.at[f], 16 + f)

    def all_of(kind, f, u=None):
        if kind == "row":
            return whole(row_out.at[f], row_in.at[f], f, ROWS)
        if kind == "brow":
            return whole(brow_out.at[f], brow_in.at[f], 16 + f, ROWS)
        if kind == "col":
            return whole(col_out.at[f, u], col_in.at[f, u], 4 + 2 * f + u, 2 * COLS)
        return whole(bcol_out.at[f, u], bcol_in.at[f, u], 10 + 2 * f + u, 2 * COLS)

    def arrived(kind, f, u=None):
        all_of(kind, f, u).wait_recv()

    def load(ref, rows):
        return [ref[z, rows, :] for z in range(NZ)]

    def store(ref, rows, planes):
        for z in range(NZ):
            ref[z, rows, :] = planes[z]

    def chunks(body):
        def step(i, carry):
            body(pl.ds(pl.multiple_of(i * 8, 8), 8))
            return carry

        lax.fori_loop(0, YB // 8, step, 0)

    def pressure_planes(rows):
        store(row_out.at[0], rows, depth_forward(load(p_ref, rows)))

    loaded(0)
    chunks(pressure_planes)
    pl.semaphore_wait(barrier, ROWS - 1 + 2 * COLS - 1)
    send_row(0)

    loaded(1)
    for z in range(NZ):
        lab[z, HALO : HALO + YB, :] = lab_ref[z].astype(f32)

    def y_edges():
        before, after = (r + ROWS - 1) % ROWS, (r + 1) % ROWS
        return [
            pltpu.make_async_remote_copy(
                src_ref=lab.at[:, pl.ds(HALO, HALO), :],
                dst_ref=lab.at[:, pl.ds(HALO + YB, HALO), :],
                send_sem=send_sem.at[20], recv_sem=recv_sem.at[20],
                device_id=(before, c), device_id_type=MESH,
            ),
            pltpu.make_async_remote_copy(
                src_ref=lab.at[:, pl.ds(YB, HALO), :],
                dst_ref=lab.at[:, pl.ds(0, HALO), :],
                send_sem=send_sem.at[21], recv_sem=recv_sem.at[21],
                device_id=(after, c), device_id_type=MESH,
            ),
        ]

    def x_edges():
        before, after = (c + COLS - 1) % COLS, (c + 1) % COLS
        return [
            pltpu.make_async_remote_copy(
                src_ref=edge_out.at[0], dst_ref=edge_in.at[1],
                send_sem=send_sem.at[22], recv_sem=recv_sem.at[22],
                device_id=(r, before), device_id_type=MESH,
            ),
            pltpu.make_async_remote_copy(
                src_ref=edge_out.at[1], dst_ref=edge_in.at[0],
                send_sem=send_sem.at[23], recv_sem=recv_sem.at[23],
                device_id=(r, after), device_id_type=MESH,
            ),
        ]

    def ids(shape, dim):
        return lax.broadcasted_iota(jnp.int32, shape, dim)

    def banded(offset):
        def tap(t, total):
            return jnp.where(offset == t, taps_ref[t], total)

        return lax.fori_loop(0, TAPS, tap, jnp.zeros(offset.shape, f32), unroll=3)

    def fill_bands():
        wide = (XB, XB)
        band = banded(ids(wide, 0) - ids(wide, 1) + HALO)
        none = jnp.zeros(wide, bf16)
        for part, value in enumerate(halves(band)):
            top_rows = jnp.concatenate([value, none], axis=1)
            low_rows = jnp.concatenate([none, value], axis=1)
            across[part] = jnp.concatenate([top_rows, low_rows], axis=0)
        edge_band[0] = banded(ids(wide, 0) % HALO - ids(wide, 1))
        edge_band[1] = banded(ids(wide, 0) % HALO - ids(wide, 1) + XB + HALO)
        tall = (4 * YB, 8 * YB)
        row, line = ids(tall, 0), ids(tall, 1)
        offset = jnp.where(row // YB == line // (2 * YB), line % (2 * YB) - row % YB, -1)
        for part, value in enumerate(halves(banded(offset))):
            down[part] = value

    def fill_damping():
        def absorb(position, length, low_width, high_width):
            size = position.shape
            low_side = jnp.maximum(low_width - position, 0).astype(f32)
            high_side = jnp.maximum(position - (length - 1 - high_width), 0).astype(f32)
            low_side = low_side / jnp.full(size, low_width, jnp.int32).astype(f32)
            high_side = high_side / jnp.full(size, high_width, jnp.int32).astype(f32)
            low_side, high_side = low_side * low_side, high_side * high_side
            total = low_side * low_side + high_side * high_side
            return jnp.exp((-0.5 * time_step * absorption * reference_speed) * total)

        damp[0:8] = absorb(c * XB + ids((8, XB), 1), NX, width_ref[0], width_ref[1])
        damp[8:] = absorb(r * YB + ids((YB, XB), 0), NY, width_ref[2], width_ref[3])

    def pack_edges():
        wide = (XB, XB)
        source, target = ids(wide, 0), ids(wide, 1)
        total = None
        for g in range(8):
            here = target // HALO == g
            first_lanes = here & (source == target % HALO)
            last_lanes = here & (source == target % HALO + XB - HALO)
            select = jnp.concatenate(
                [jnp.where(first_lanes, 1.0, 0.0), jnp.where(last_lanes, 1.0, 0.0)], axis=1
            ).astype(bf16)
            part = mm(lab[2 * g : 2 * g + 2].reshape(XB, XB).astype(bf16), select)
            total = part if total is None else total + part
        edge_out[0] = total[:, :XB]
        edge_out[1] = total[:, XB:]

    def tables():
        density = [jnp.full((8, XB), density_ref[n], f32) for n in range(LABELS)]
        speed = [jnp.full((8, XB), speed_ref[n], f32) for n in range(LABELS)]
        return [1.0 / d for d in density], [d * s * s for d, s in zip(density, speed)]

    def look_up(label, table):
        value = jnp.broadcast_to(table[0][None], label.shape)
        for n in range(1, LABELS):
            value = jnp.where(label == float(n), table[n][None], value)
        return value

    def fill_raw():
        buoyancy_of, modulus_of = tables()

        def plane(z, carry):
            label = lab[z].reshape(8, 8, XB)
            rows = pl.ds(pl.multiple_of(z * 2 * YB, 2 * YB), 2 * YB)
            raw[rows, :XB] = look_up(label, buoyancy_of).reshape(2 * YB, XB)
            raw[rows, XB:] = look_up(label, modulus_of).reshape(2 * YB, XB)
            return carry

        lax.fori_loop(0, NZ, plane, 0)

    def smooth():
        buoyancy_of, modulus_of = tables()
        edges = [edge_in[0].reshape(16, 8, XB), edge_in[1].reshape(16, 8, XB)]
        sides = [
            halves(jnp.concatenate([look_up(e, t).reshape(XB, XB) for e in edges], axis=1))
            for t in (buoyancy_of, modulus_of)
        ]
        group_of = ids((XB, XB), 0) // HALO

        def quarter(i, carry):
            rows = pl.ds(pl.multiple_of(i * 8 * YB, 8 * YB), 8 * YB)
            high, low_part = halves(raw[rows, :])
            main = mm(high, across[0]) + mm(low_part, across[0]) + mm(high, across[1])
            parts = []
            for g in range(2):
                inside = group_of == 2 * i + g
                parts.append(
                    jnp.concatenate(
                        [jnp.where(inside, edge_band[s], 0.0) for s in range(2)], axis=0
                    )
                )
            high, low_part = halves(jnp.concatenate(parts, axis=1))
            columns = []
            for side_high, side_low in sides:
                out = mm(side_high, high) + mm(side_low, high) + mm(side_high, low_part)
                columns.append(jnp.concatenate([out[:, :XB], out[:, XB:]], axis=0))
            high, low_part = halves(main + jnp.concatenate(columns, axis=1))
            out = mm(down[0], high) + mm(down[0], low_part) + mm(down[1], high)
            planes = pl.ds(i * 4, 4)
            coef[0, planes] = out[:, :XB].reshape(4, YB, XB)
            coef[1, planes] = out[:, XB:].reshape(4, YB, XB)
            return carry

        lax.fori_loop(0, 4, quarter, 0)

    tile_rows = lax.broadcasted_iota(jnp.int32, (8, XB), 0)
    one, zero = jnp.ones((8, XB), f32), jnp.zeros((8, XB), f32)
    top = jnp.where(tile_rows < SLOTS, one, zero)
    bottom = 1.0 - top
    flat = jnp.where(jnp.full((8, XB), j, jnp.int32) == 0, one, zero)
    deep = 1.0 - flat

    def slot_of(u):
        return u * CHUNK + q * SLOTS + tile_rows % SLOTS

    def first_of(u):
        return jnp.where(slot_of(u) == 0, one, zero)

    def turned(value):
        return pltpu.roll(value, SLOTS, 0)

    pi2 = np.float32(math.pi * math.pi)
    kz = jnp.full((8, XB), j, jnp.int32).astype(f32) * np.float32(2.0 * math.pi / NZ)

    def square_of(u):
        ky = slot_of(u).astype(f32) * np.float32(2.0 * math.pi / NY)
        return ky * ky + kz * kz + pi2 * bottom * (first_of(u) * deep + flat)

    squares = (square_of(0), pi2 + pi2 * bottom, square_of(1))
    scale = np.float32((0.5 * reference_speed * time_step) ** 2)

    def fill_kappa(kc, carry):
        kx2 = xt_ref[2, pl.ds(kc, 1), :]
        for g, part in enumerate(squares):
            v2 = scale * (kx2 + part)
            series = 1.0 + v2 * np.float32(-1.0 / 110.0)
            series = 1.0 + v2 * np.float32(-1.0 / 72.0) * series
            series = 1.0 + v2 * np.float32(-1.0 / 42.0) * series
            series = 1.0 + v2 * np.float32(-1.0 / 20.0) * series
            kappa[g, kc] = 1.0 + v2 * np.float32(-1.0 / 6.0) * series
        return carry

    loaded(2)
    lax.fori_loop(0, COLS, fill_kappa, 0)

    for edge in y_edges():
        edge.start()
    loaded(3, 4)
    fill_bands()
    fill_damping()

    def lines(ref, f):
        return ref[f].reshape(NY, XB)

    def put_col(f, value):
        col_out[f] = value.reshape(2, 2 * COLS, 2 * SLOTS, XB)
        send_col(f, 0)
        send_col(f, 1)

    def row_product(table, values):
        parts = [halves(v) for v in values]
        high = [part[0] for part in parts]
        low_part = [part[1] for part in parts]
        if len(values) == 1:
            both = mm(table[0], jnp.concatenate([high[0], low_part[0]], axis=1))
            return [both[:, :XB] + both[:, XB:] + mm(table[1], high[0])]
        high = jnp.concatenate(high, axis=1)
        low_part = jnp.concatenate(low_part, axis=1)
        result = mm(table[0], high) + mm(table[0], low_part) + mm(table[1], high)
        return [result[:, :XB], result[:, XB:]]

    def y_derivative(value, sign):
        tiles = value.reshape(NY // 8, 8, XB)
        same = tiles * yd_ref[0]
        cross = pltpu.roll(tiles, SLOTS, 1) * yd_ref[1]
        return (cross + same if sign > 0 else cross - same).reshape(NY, XB)

    def x_forward(f, u):
        first, groups = first_of(u), 2 - u
        general = (1.0 - first) * deep
        rest = (1.0 - first) * flat
        lone = first * deep
        re_r, re_turned_r = top + bottom * lone, bottom * general
        re_i, re_turned_i = bottom * general, bottom * flat - top * general
        im_r, im_turned_r = -bottom * general, top * (general + rest)
        im_i, im_turned_i = top * general + lone + bottom * rest, bottom * general
        for n in range(COLS):
            tr, ti = col_in[f, u, n], col_in[f, u, COLS + n]
            rr, ri = turned(tr), turned(ti)
            xb[0, 0, n] = re_r * tr + re_turned_r * rr + re_i * ti + re_turned_i * ri
            xb[0, 1, n] = im_r * tr + im_turned_r * rr + im_i * ti + im_turned_i * ri
            if u == 0:
                xb[1, 0, n] = first * flat * (top * rr + bottom * ti)
                xb[1, 1, n] = zero

        def group(g, carry):
            values = [(xb[g, 0, n], xb[g, 1, n]) for n in range(COLS)]
            values = short_transform(values, -1.0)
            for kc in range(COLS):
                re, im = values[kc]
                cs, sn = xt_ref[0, kc : kc + 1, :], xt_ref[1, kc : kc + 1, :]
                xs[g, kc, :, :XB] = re * cs + im * sn
                xs[g, kc, :, XB:] = im * cs - re * sn
            return carry

        lax.fori_loop(0, groups, group, 0)
        high, low_part = halves(xs[:groups].reshape(groups * COLS * 8, 2 * XB))
        out = mm(high, wx_ref[0]) + mm(low_part, wx_ref[0]) + mm(high, wx_ref[1])
        return out.reshape(groups, COLS, 8, 2 * XB)

    def kappa_of(u):
        return kappa[0:2] if u == 0 else kappa[2:3]

    def x_derivative(re, im, sign):
        same = xt_ref[3][None, :, None, :]
        cross = xt_ref[4][None, :, None, :]
        if sign > 0:
            return -(re * same + im * cross), re * cross - im * same
        return re * same - im * cross, im * same + re * cross

    def x_inverse(value, f, u):
        first, groups = first_of(u), 2 - u
        high, low_part = halves(value.reshape(groups * COLS * 8, 2 * XB))
        out = mm(high, ux_ref[0]) + mm(low_part, ux_ref[0]) + mm(high, ux_ref[1])
        xs[:groups] = out.reshape(groups, COLS, 8, 2 * XB)

        def group(g, carry):
            values = []
            for kc in range(COLS):
                re, im = xs[g, kc, :, :XB], xs[g, kc, :, XB:]
                cs, sn = xt_ref[0, kc : kc + 1, :], xt_ref[1, kc : kc + 1, :]
                values.append((re * cs - im * sn, im * cs + re * sn))
            values = short_transform(values, 1.0)
            for n in range(COLS):
                xb[g, 0, n] = values[n][0]
                xb[g, 1, n] = values[n][1]
            return carry

        lax.fori_loop(0, groups, group, 0)
        half = 0.5 * (1.0 - first) * deep
        rest = (1.0 - first) * flat
        lone = first * deep
        r_re = top * half + top * flat + lone
        r_re_turned = top * half
        r_im, r_im_turned = -bottom * half, bottom * (half + rest)
        i_re, i_re_turned = bottom * half, top * flat - bottom * half
        i_im, i_im_turned = top * half + lone + bottom * rest, top * half
        for n in range(COLS):
            vr, vi = xb[0, 0, n], xb[0, 1, n]
            wr, wi = turned(vr), turned(vi)
            out_r = r_re * vr + r_re_turned * wr + r_im * vi + r_im_turned * wi
            out_i = i_re * vr + i_re_turned * wr + i_im * vi + i_im_turned * wi
            if u == 0:
                extra = first * flat * bottom
                out_r = out_r + extra * turned(xb[1, 0, n])
                out_i = out_i + extra * xb[1, 0, n]
            bcol_out[f, u, n] = out_r
            bcol_out[f, u, COLS + n] = out_i

    loaded(5)
    arrived("row", 0)
    put_col(0, row_product(fy_ref, [lines(row_in, 0)])[0])

    for edge in y_edges():
        edge.wait_recv()
    pack_edges()
    for edge in x_edges():
        edge.start()
    loaded(7, 8)
    fill_raw()

    loaded(6, 9)
    for u in range(2):
        arrived("col", 0, u)
        spectrum = x_forward(0, u)
        re, im = spectrum[..., :XB] * kappa_of(u), spectrum[..., XB:] * kappa_of(u)
        dre, dim = x_derivative(re, im, 1)
        x_inverse(jnp.concatenate([dre, dim], axis=-1), 0, u)
        send_bcol(0, u)
        if u == 1:
            send_bcol(1, 0)
        x_inverse(jnp.concatenate([re, im], axis=-1), 1, u)
    send_bcol(1, 1)

    for edge in x_edges():
        edge.wait_recv()
    smooth()
    loaded(10, 11, 12, 13, 14)

    arrived("bcol", 0, 0)
    arrived("bcol", 0, 1)
    brow_out[0] = row_product(gy_ref, [lines(bcol_in, 0)])[0].reshape(ROWS, YB, XB)
    send_brow(0)

    dx = damp[0:8]

    arrived("brow", 0)

    def update_x(rows):
        grad = depth_inverse(load(brow_in.at[0], rows))
        fresh = []
        for z in range(NZ):
            change = time_step * coef[0, z, rows, :] * grad[z]
            fresh.append(dx * (dx * vx_ref[z, rows, :] - change))
        store(vxo_ref, rows, fresh)
        store(row_out.at[1], rows, depth_forward(fresh))

    chunks(update_x)
    send_row(1)
    writes[0].start()

    arrived("bcol", 1, 0)
    arrived("bcol", 1, 1)
    flow = lines(bcol_in, 1)
    plain, slope = row_product(gy_ref, [flow, y_derivative(flow, 1)])
    brow_out[1] = slope.reshape(ROWS, YB, XB)
    send_brow(1)
    brow_out[2] = plain.reshape(ROWS, YB, XB)
    send_brow(2)

    arrived("row", 1)
    put_col(1, row_product(fy_ref, [lines(row_in, 1)])[0])

    arrived("brow", 1)

    def update_y(rows):
        grad = depth_inverse(load(brow_in.at[1], rows))
        dy = damp[pl.ds(pl.multiple_of(rows.start + 8, 8), 8), :]
        fresh = []
        for z in range(NZ):
            change = time_step * coef[0, z, rows, :] * grad[z]
            fresh.append(dy * (dy * vy_ref[z, rows, :] - change))
        store(vyo_ref, rows, fresh)
        store(row_out.at[2], rows, depth_forward(fresh))

    chunks(update_y)
    send_row(2)
    writes[1].start()

    arrived("brow", 2)

    def update_z(rows):
        grad = depth_inverse(depth_derivative(load(brow_in.at[2], rows), 1))
        fresh = []
        for z in range(NZ):
            fresh.append(vz_ref[z, rows, :] - time_step * coef[0, z, rows, :] * grad[z])
        store(vzo_ref, rows, fresh)
        store(row_out.at[3], rows, depth_derivative(depth_forward(fresh), -1))

    chunks(update_z)
    send_row(3)
    writes[2].start()

    arrived("row", 2)
    arrived("row", 3)
    aside, below = row_product(fy_ref, [lines(row_in, 2), lines(row_in, 3)])
    put_col(2, below + y_derivative(aside, -1))

    flows = []
    for u in range(2):
        arrived("col", 1, u)
        flow_x = x_forward(1, u)
        flows.append(x_derivative(flow_x[..., :XB], flow_x[..., XB:], -1))
    for u in range(2):
        arrived("col", 2, u)
        remains = x_forward(2, u)
        tre = (flows[u][0] + remains[..., :XB]) * kappa_of(u)
        tim = (flows[u][1] + remains[..., XB:]) * kappa_of(u)
        x_inverse(jnp.concatenate([tre, tim], axis=-1), 2, u)
        send_bcol(2, u)

    arrived("bcol", 2, 0)
    arrived("bcol", 2, 1)
    brow_out[3] = row_product(gy_ref, [lines(bcol_in, 2)])[0].reshape(ROWS, YB, XB)
    send_brow(3)

    arrived("brow", 3)

    def update_p(rows):
        divergence = depth_inverse(load(brow_in.at[3], rows))
        both = dx * damp[pl.ds(pl.multiple_of(rows.start + 8, 8), 8), :]
        for z in range(NZ):
            change = time_step * coef[1, z, rows, :] * divergence[z]
            po_ref[z, rows, :] = both * (both * p_ref[z, rows, :] - change)

    chunks(update_p)
    writes[3].start()

    for f in range(4):
        all_of("row", f).wait_send()
        all_of("brow", f).wait_send()
    for f in range(3):
        for u in range(2):
            all_of("col", f, u).wait_send()
            all_of("bcol", f, u).wait_send()
    for edge in y_edges() + x_edges():
        edge.wait_send()
    for write in writes:
        write.wait()


def write_kernel(a, b, c, d, a_out, b_out, c_out, d_out, held, in_sem, out_sem):
    arrays = ((a, a_out), (b, b_out), (c, c_out), (d, d_out))
    loads = [pltpu.make_async_copy(x, held.at[n], in_sem.at[n]) for n, (x, _) in enumerate(arrays)]
    stores = [pltpu.make_async_copy(held.at[n], y, out_sem.at[n]) for n, (_, y) in enumerate(arrays)]
    for load in loads:
        load.start()
    for load, store in zip(loads, stores):
        load.wait()
        store.start()
    for store in stores:
        store.wait()


def on_device(
    labels, pressure, velocity_x, velocity_y, velocity_z,
    speed_table, density_table, filter_taps, layer_width,
):
    fy, gy, yd = row_tables()
    wx, ux, xt = column_tables()
    brick = jax.ShapeDtypeStruct(pressure.shape, f32)
    row_buffer = lambda n: pltpu.VMEM((n, ROWS, YB, XB), f32)
    col_buffer = lambda n: pltpu.VMEM((n, 2, 2 * COLS, 2 * SLOTS, XB), f32)
    results = pl.pallas_call(
        step_kernel,
        out_shape=(brick,) * 4,
        in_specs=[pl.BlockSpec(memory_space=pl.ANY)] * 15,
        out_specs=(pl.BlockSpec(memory_space=pl.ANY),) * 4,
        scratch_shapes=[
            row_buffer(4), row_buffer(4), col_buffer(3), col_buffer(3),
            col_buffer(3), col_buffer(3), row_buffer(4), row_buffer(4),
            pltpu.VMEM((3, COLS, 8, XB), f32),
            pltpu.VMEM((2, 2, COLS, 8, XB), f32),
            pltpu.VMEM((2, COLS, 8, 2 * XB), f32),
            pltpu.VMEM((2, NZ, YB, XB), f32),
            pltpu.VMEM((NZ, 2 * YB, XB), f32),
            pltpu.VMEM((2, XB, XB), f32),
            pltpu.VMEM((2, XB, XB), f32),
            pltpu.VMEM((NZ * 2 * YB, 2 * XB), f32),
            pltpu.VMEM((2, 2 * XB, 2 * XB), bf16),
            pltpu.VMEM((2, XB, XB), f32),
            pltpu.VMEM((2, 4 * YB, 8 * YB), bf16),
            pltpu.VMEM((8 + YB, XB), f32),
            pltpu.VMEM(labels.shape, jnp.int32),
            *[pltpu.VMEM(pressure.shape, f32)] * 4,
            pltpu.SMEM((LABELS,), f32), pltpu.SMEM((LABELS,), f32),
            pltpu.SMEM((TAPS,), f32), pltpu.SMEM((4,), jnp.int32),
            *[pltpu.VMEM(t.shape, t.dtype) for t in (fy, gy, yd, wx, ux, xt)],
            *[pltpu.VMEM(pressure.shape, f32)] * 4,
            pltpu.SemaphoreType.DMA((24,)),
            pltpu.SemaphoreType.DMA((24,)),
            pltpu.SemaphoreType.DMA((15,)),
            pltpu.SemaphoreType.DMA((4,)),
        ],
        compiler_params=pltpu.CompilerParams(
            collective_id=0, has_side_effects=True, vmem_limit_bytes=VMEM_BYTES
        ),
    )(
        labels, pressure, velocity_x, velocity_y, velocity_z,
        speed_table, density_table, filter_taps, layer_width,
        jnp.asarray(fy), jnp.asarray(gy), jnp.asarray(yd),
        jnp.asarray(wx), jnp.asarray(ux), jnp.asarray(xt),
    )
    return pl.pallas_call(
        write_kernel,
        out_shape=(brick,) * 4,
        in_specs=[pl.BlockSpec(memory_space=pl.ANY)] * 4,
        out_specs=(pl.BlockSpec(memory_space=pl.ANY),) * 4,
        scratch_shapes=[
            pltpu.VMEM((4,) + pressure.shape, f32),
            pltpu.SemaphoreType.DMA((4,)), pltpu.SemaphoreType.DMA((4,)),
        ],
        compiler_params=pltpu.CompilerParams(vmem_limit_bytes=VMEM_BYTES),
    )(*results)


def solution(mesh):
    brick = P(None, "row", "col")
    return jax.shard_map(
        on_device,
        mesh=mesh,
        in_specs=(brick,) * 5 + (P(),) * 4,
        out_specs=(brick,) * 4,
        check_vma=False,
    )
```

```python
import functools
import math

import jax
import jax.numpy as jnp
import numpy as np
from jax import lax
from jax.experimental import pallas as pl
from jax.experimental.pallas import tpu as pltpu
from jax.sharding import PartitionSpec as P

time_step = 0.15
reference_speed = 2.0
absorption = 6.0
MESH = pl.DeviceIdType.MESH

NZ, NY, NX = 16, 512, 2048
ROWS, COLS = 16, 16
YB, XB = NY // ROWS, NX // COLS
SLOTS, HALO = 4, 16
CHUNK = 2 * COLS * SLOTS
STEP_BYTES, WRITE_BYTES = 40 << 20, 4 << 20
TAPS, LABELS = 33, 12
f32, bf16 = jnp.float32, jnp.bfloat16


def split_table(table):
    high = table.astype(np.float32).astype(bf16)
    low = (table - high.astype(np.float64)).astype(np.float32).astype(bf16)
    return np.stack([high, low])


def row_tables():
    slot = np.arange(NY // 2)
    y = np.arange(NY)
    angle = 2.0 * np.pi * ((slot[:, None] * y[None, :]) % NY) / NY
    real, imag = np.cos(angle), -np.sin(angle)
    imag[0] = np.where(y % 2 == 0, 1.0, -1.0)

    def order(a, b):
        pair = [t.reshape((2 * 2 * COLS, SLOTS) + t.shape[1:]) for t in (a, b)]
        return np.stack(pair, axis=1)

    forward = order(real, imag).reshape(NY, NY)
    weight = np.where(slot == 0, 1.0, 2.0)[:, None] / NY
    inverse = order(real * weight, imag * weight).reshape(NY, NY).T
    wave = 2.0 * np.pi * slot / NY
    same = -wave * np.sin(0.5 * wave)
    cross = wave * np.cos(0.5 * wave)
    same_imag = same.copy()
    same_imag[0] = -np.pi
    tables = [order(same, same_imag), order(-cross, cross)]
    wide = [np.broadcast_to(t.reshape(-1, 2 * SLOTS, 1), (NY // 8, 8, XB)) for t in tables]
    return split_table(forward), split_table(inverse), np.stack(wide).astype(np.float32)


def column_tables():
    x = np.arange(XB)
    angle = 2.0 * np.pi * ((x[:, None] * x[None, :]) % XB) / XB
    c, s = np.cos(angle), np.sin(angle)
    forward = np.block([[c, -s], [s, c]])
    inverse = np.block([[c, s], [-s, c]]) / NX
    kc = np.arange(COLS)
    twist = 2.0 * np.pi * (kc[:, None] * x[None, :]) / NX
    index = kc[:, None] + COLS * x[None, :]
    wave = 2.0 * np.pi * np.where(index < NX // 2, index, index - NX) / NX
    same = wave * np.sin(0.5 * wave)
    cross = wave * np.cos(0.5 * wave)
    small = np.stack([np.cos(twist), np.sin(twist), wave * wave, same, cross]).astype(np.float32)
    return split_table(forward), split_table(inverse), small


def scaled(value, factor):
    if abs(factor - 1.0) < 1e-12:
        return value
    if abs(factor + 1.0) < 1e-12:
        return -value
    return value * np.float32(factor)


def weighted(terms):
    total = None
    for value, factor in terms:
        if abs(factor) < 1e-12:
            continue
        if total is None:
            total = scaled(value, factor)
        elif abs(factor + 1.0) < 1e-12:
            total = total - value
        else:
            total = total + scaled(value, factor)
    return total


def cos16(n):
    return math.cos(2.0 * math.pi * (n % 16) / 16)


def sin16(n):
    return math.sin(2.0 * math.pi * (n % 16) / 16)


def depth_forward(p):
    even = [p[0]] + [p[n] + p[16 - n] for n in range(1, 8)] + [p[8]]
    odd = [None] + [p[n] - p[16 - n] for n in range(1, 8)]
    plus = [even[n] + even[8 - n] for n in range(4)] + [even[4]]
    minus = [even[n] - even[8 - n] for n in range(4)]
    odd_plus = [None] + [odd[n] + odd[8 - n] for n in range(1, 4)] + [odd[4]]
    odd_minus = [None] + [odd[n] - odd[8 - n] for n in range(1, 4)]

    def real_of(k):
        side = plus if k % 2 == 0 else minus
        return weighted([(side[n], cos16(k * n)) for n in range(len(side))])

    def imag_of(k):
        if k % 2 == 0:
            return weighted([(odd_minus[n], -sin16(k * n)) for n in range(1, 4)])
        return weighted([(odd_plus[n], -sin16(k * n)) for n in range(1, 5)])

    out = [real_of(0), real_of(8)]
    for k in range(1, 8):
        out += [real_of(k), imag_of(k)]
    return out


def depth_inverse(m):
    real = [m[0]] + [m[2 * k] for k in range(1, 8)] + [m[1]]
    imag = [None] + [m[2 * k + 1] for k in range(1, 8)]
    weight = [1.0 / 16] + [2.0 / 16] * 7 + [1.0 / 16]

    def terms(values, ids, n, wave):
        return weighted([(values[k], weight[k] * wave(k * n)) for k in ids])

    out = [None] * 16
    for n in range(0, 5):
        ce = terms(real, range(0, 9, 2), n, cos16)
        co = terms(real, range(1, 9, 2), n, cos16)
        so = terms(imag, range(1, 8, 2), n, lambda v: -sin16(v))
        se = terms(imag, range(2, 8, 2), n, lambda v: -sin16(v))
        near = ce if co is None else ce + co
        far = ce if co is None else ce - co
        if n == 0:
            out[0], out[8] = near, far
            continue
        if se is None:
            d_near, d_far = so, so
        else:
            d_near, d_far = so + se, so - se
        out[n], out[16 - n] = near + d_near, near - d_near
        if n < 4:
            out[8 - n], out[8 + n] = far + d_far, far - d_far
    return out


def depth_derivative(m, sign):
    out = [jnp.zeros_like(m[0]), m[1] * np.float32(-sign * math.pi)]
    for k in range(1, 8):
        wave = 2.0 * math.pi * k / 16
        a = np.float32(-sign * wave * math.sin(0.5 * wave))
        b = np.float32(wave * math.cos(0.5 * wave))
        out += [m[2 * k] * a - m[2 * k + 1] * b, m[2 * k + 1] * a + m[2 * k] * b]
    return out


def short_transform(values, sign):
    count = len(values)
    if count == 1:
        return values
    even = short_transform(values[0::2], sign)
    odd = short_transform(values[1::2], sign)
    out = [None] * count
    for k in range(count // 2):
        angle = sign * 2.0 * math.pi * k / count
        c, s = math.cos(angle), math.sin(angle)
        re, im = odd[k]
        if k == 0:
            tr, ti = re, im
        elif abs(c) < 1e-9:
            tr, ti = (-im, re) if s > 0 else (im, -re)
        elif abs(abs(c) - abs(s)) < 1e-9:
            h = np.float32(abs(c))
            cs, ss = (1 if c > 0 else -1), (1 if s > 0 else -1)
            first = re if cs > 0 else -re
            tr = (first - im if ss > 0 else first + im) * h
            second = im if cs > 0 else -im
            ti = (second + re if ss > 0 else second - re) * h
        else:
            tr = re * np.float32(c) - im * np.float32(s)
            ti = re * np.float32(s) + im * np.float32(c)
        er, ei = even[k]
        out[k] = (er + tr, ei + ti)
        out[k + count // 2] = (er - tr, ei - ti)
    return out


def halves(value):
    high = value.astype(bf16)
    low = (value - high.astype(f32)).astype(bf16)
    return high, low


def mm(a, b):
    return jnp.dot(a, b, preferred_element_type=f32)


def step_kernel(
    lab_hbm, p_hbm, vx_hbm, vy_hbm, vz_hbm, speed_hbm, density_hbm, taps_hbm, width_hbm,
    fy_hbm, gy_hbm, yd_hbm, wx_hbm, ux_hbm, xt_hbm,
    po_ref, vxo_ref, vyo_ref, vzo_ref,
    row_out, row_in, col_out, col_in, bcol_out, bcol_in, brow_out, brow_in,
    kappa, xb, xs, coef, lab, edge_out, edge_in, raw, across, edge_band, down, damp,
    lab_ref, p_ref, vx_ref, vy_ref, vz_ref, speed_ref, density_ref, taps_ref, width_ref,
    fy_ref, gy_ref, yd_ref, wx_ref, ux_ref, xt_ref,
    send_sem, recv_sem, load_sem,
):
    def loaded(*numbers):
        for n in numbers:
            fetches[n].wait()

    r, c = lax.axis_index("row"), lax.axis_index("col")
    j, h = r // 2, r % 2
    q = h * COLS + c

    barrier = pltpu.get_barrier_semaphore()

    x_low, y_chip, core = r // 8, (r // 2) % 4, r % 2
    z_chip, x_high = c // 2, c % 2

    def pick(i, values):
        value = jnp.int32(values[0])
        for n in range(1, len(values)):
            value = jnp.where(i == n, jnp.int32(values[n]), value)
        return value

    def row_partner(i, other):
        x = (x_low + pick(i, (1, 0, 1, 1, 0, 0, 1, 0))) % 2
        y = (y_chip + pick(i, (2, 2, 1, 3, 1, 3, 0, 0))) % 4
        return (x * 4 + y) * 2 + (core + other) % 2

    def plane_partner(i, other):
        z = (z_chip + pick(i, (4, 3, 5, 4, 2, 6, 3, 5, 1, 7, 2, 6, 0, 1, 7, 0))) % 8
        x = (x_high + pick(i, (1, 1, 1, 0, 1, 1, 0, 0, 1, 1, 0, 0, 1, 0, 0, 0))) % 2
        return (core + other) % 2 * COLS + z * 2 + x

    def each_partner(partner, classes, body):
        def step(i, carry):
            body(partner(i, 0))
            body(partner(i, 1))
            return carry

        lax.fori_loop(0, classes - 1, step, 0)
        body(partner(classes - 1, 1))

    def row_device(t):
        return (t, c)

    def plane_device(t):
        return (2 * j + t // COLS, t % COLS)

    def greet(device):
        pl.semaphore_signal(barrier, inc=1, device_id=device, device_id_type=MESH)

    each_partner(plane_partner, COLS, lambda t: greet(plane_device(t)))
    each_partner(row_partner, ROWS // 2, lambda t: greet(row_device(t)))

    fetches = [
        pltpu.make_async_copy(source, target, load_sem.at[n])
        for n, (source, target) in enumerate(
            [
                (p_hbm, p_ref), (lab_hbm, lab_ref), (xt_hbm, xt_ref), (taps_hbm, taps_ref),
                (width_hbm, width_ref), (fy_hbm, fy_ref), (wx_hbm, wx_ref),
                (speed_hbm, speed_ref), (density_hbm, density_ref), (ux_hbm, ux_ref),
                (gy_hbm, gy_ref), (vx_hbm, vx_ref), (yd_hbm, yd_ref), (vy_hbm, vy_ref),
                (vz_hbm, vz_ref),
            ]
        )
    ]
    for fetch in fetches:
        fetch.start()
    def start_all(src, dst, sem, partner, classes, device_of, own):
        def start(t):
            pltpu.make_async_remote_copy(
                src_ref=src.at[t], dst_ref=dst.at[own], send_sem=send_sem.at[sem],
                recv_sem=recv_sem.at[sem], device_id=device_of(t), device_id_type=MESH,
            ).start()

        each_partner(partner, classes, start)
        dst[own] = src[own]

    def row_all(src, dst, sem):
        start_all(src, dst, sem, row_partner, ROWS // 2, row_device, r)

    def plane_all(src, dst, sem):
        start_all(src, dst, sem, plane_partner, COLS, plane_device, q)

    def whole(src, dst, sem, count):
        span = pl.ds(0, count - 1)
        return pltpu.make_async_remote_copy(
            src_ref=src.at[span], dst_ref=dst.at[span], send_sem=send_sem.at[sem],
            recv_sem=recv_sem.at[sem], device_id=((r + 1) % ROWS, c), device_id_type=MESH,
        )

    def send_row(f):
        row_all(row_out.at[f], row_in.at[f], f)

    def send_col(f, u):
        plane_all(col_out.at[f, u], col_in.at[f, u], 4 + 2 * f + u)

    def send_bcol(f, u):
        plane_all(bcol_out.at[f, u], bcol_in.at[f, u], 10 + 2 * f + u)

    def send_brow(f):
        row_all(brow_out.at[f], brow_in.at[f], 16 + f)

    def all_of(kind, f, u=None):
        if kind == "row":
            return whole(row_out.at[f], row_in.at[f], f, ROWS)
        if kind == "brow":
            return whole(brow_out.at[f], brow_in.at[f], 16 + f, ROWS)
        if kind == "col":
            return whole(col_out.at[f, u], col_in.at[f, u], 4 + 2 * f + u, 2 * COLS)
        return whole(bcol_out.at[f, u], bcol_in.at[f, u], 10 + 2 * f + u, 2 * COLS)

    def arrived(kind, f, u=None):
        all_of(kind, f, u).wait_recv()

    def load(ref, rows):
        return [ref[z, rows, :] for z in range(NZ)]

    def store(ref, rows, planes):
        for z in range(NZ):
            ref[z, rows, :] = planes[z]

    def chunks(body):
        def step(i, carry):
            body(pl.ds(pl.multiple_of(i * 8, 8), 8))
            return carry

        lax.fori_loop(0, YB // 8, step, 0)

    def pressure_planes(rows):
        store(row_out.at[0], rows, depth_forward(load(p_ref, rows)))

    loaded(0)
    chunks(pressure_planes)
    pl.semaphore_wait(barrier, ROWS - 1 + 2 * COLS - 1)
    send_row(0)

    loaded(1)
    for z in range(NZ):
        lab[z, HALO : HALO + YB, :] = lab_ref[z].astype(f32)

    def y_edges():
        before, after = (r + ROWS - 1) % ROWS, (r + 1) % ROWS
        return [
            pltpu.make_async_remote_copy(
                src_ref=lab.at[:, pl.ds(HALO, HALO), :],
                dst_ref=lab.at[:, pl.ds(HALO + YB, HALO), :],
                send_sem=send_sem.at[20], recv_sem=recv_sem.at[20],
                device_id=(before, c), device_id_type=MESH,
            ),
            pltpu.make_async_remote_copy(
                src_ref=lab.at[:, pl.ds(YB, HALO), :],
                dst_ref=lab.at[:, pl.ds(0, HALO), :],
                send_sem=send_sem.at[21], recv_sem=recv_sem.at[21],
                device_id=(after, c), device_id_type=MESH,
            ),
        ]

    def x_edges():
        before, after = (c + COLS - 1) % COLS, (c + 1) % COLS
        return [
            pltpu.make_async_remote_copy(
                src_ref=edge_out.at[0], dst_ref=edge_in.at[1],
                send_sem=send_sem.at[22], recv_sem=recv_sem.at[22],
                device_id=(r, before), device_id_type=MESH,
            ),
            pltpu.make_async_remote_copy(
                src_ref=edge_out.at[1], dst_ref=edge_in.at[0],
                send_sem=send_sem.at[23], recv_sem=recv_sem.at[23],
                device_id=(r, after), device_id_type=MESH,
            ),
        ]

    def ids(shape, dim):
        return lax.broadcasted_iota(jnp.int32, shape, dim)

    def banded(offset):
        def tap(t, total):
            return jnp.where(offset == t, taps_ref[t], total)

        return lax.fori_loop(0, TAPS, tap, jnp.zeros(offset.shape, f32), unroll=3)

    def fill_bands():
        wide = (XB, XB)
        band = banded(ids(wide, 0) - ids(wide, 1) + HALO)
        none = jnp.zeros(wide, bf16)
        for part, value in enumerate(halves(band)):
            top_rows = jnp.concatenate([value, none], axis=1)
            low_rows = jnp.concatenate([none, value], axis=1)
            across[part] = jnp.concatenate([top_rows, low_rows], axis=0)
        edge_band[0] = banded(ids(wide, 0) % HALO - ids(wide, 1))
        edge_band[1] = banded(ids(wide, 0) % HALO - ids(wide, 1) + XB + HALO)
        tall = (4 * YB, 8 * YB)
        row, line = ids(tall, 0), ids(tall, 1)
        offset = jnp.where(row // YB == line // (2 * YB), line % (2 * YB) - row % YB, -1)
        for part, value in enumerate(halves(banded(offset))):
            down[part] = value

    def fill_damping():
        def absorb(position, length, low_width, high_width):
            size = position.shape
            low_side = jnp.maximum(low_width - position, 0).astype(f32)
            high_side = jnp.maximum(position - (length - 1 - high_width), 0).astype(f32)
            low_side = low_side / jnp.full(size, low_width, jnp.int32).astype(f32)
            high_side = high_side / jnp.full(size, high_width, jnp.int32).astype(f32)
            low_side, high_side = low_side * low_side, high_side * high_side
            total = low_side * low_side + high_side * high_side
            return jnp.exp((-0.5 * time_step * absorption * reference_speed) * total)

        damp[0:8] = absorb(c * XB + ids((8, XB), 1), NX, width_ref[0], width_ref[1])
        damp[8:] = absorb(r * YB + ids((YB, XB), 0), NY, width_ref[2], width_ref[3])

    def pack_edges():
        wide = (XB, XB)
        source, target = ids(wide, 0), ids(wide, 1)
        total = None
        for g in range(8):
            here = target // HALO == g
            first_lanes = here & (source == target % HALO)
            last_lanes = here & (source == target % HALO + XB - HALO)
            select = jnp.concatenate(
                [jnp.where(first_lanes, 1.0, 0.0), jnp.where(last_lanes, 1.0, 0.0)], axis=1
            ).astype(bf16)
            part = mm(lab[2 * g : 2 * g + 2].reshape(XB, XB).astype(bf16), select)
            total = part if total is None else total + part
        edge_out[0] = total[:, :XB]
        edge_out[1] = total[:, XB:]

    def tables():
        density = [jnp.full((8, XB), density_ref[n], f32) for n in range(LABELS)]
        speed = [jnp.full((8, XB), speed_ref[n], f32) for n in range(LABELS)]
        return [1.0 / d for d in density], [d * s * s for d, s in zip(density, speed)]

    def look_up(label, table):
        value = jnp.broadcast_to(table[0][None], label.shape)
        for n in range(1, LABELS):
            value = jnp.where(label == float(n), table[n][None], value)
        return value

    def fill_raw():
        buoyancy_of, modulus_of = tables()

        def plane(z, carry):
            label = lab[z].reshape(8, 8, XB)
            rows = pl.ds(pl.multiple_of(z * 2 * YB, 2 * YB), 2 * YB)
            raw[rows, :XB] = look_up(label, buoyancy_of).reshape(2 * YB, XB)
            raw[rows, XB:] = look_up(label, modulus_of).reshape(2 * YB, XB)
            return carry

        lax.fori_loop(0, NZ, plane, 0)

    def smooth():
        buoyancy_of, modulus_of = tables()
        edges = [edge_in[0].reshape(16, 8, XB), edge_in[1].reshape(16, 8, XB)]
        sides = [
            halves(jnp.concatenate([look_up(e, t).reshape(XB, XB) for e in edges], axis=1))
            for t in (buoyancy_of, modulus_of)
        ]
        group_of = ids((XB, XB), 0) // HALO

        def quarter(i, carry):
            rows = pl.ds(pl.multiple_of(i * 8 * YB, 8 * YB), 8 * YB)
            high, low_part = halves(raw[rows, :])
            main = mm(high, across[0]) + mm(low_part, across[0]) + mm(high, across[1])
            parts = []
            for g in range(2):
                inside = group_of == 2 * i + g
                parts.append(
                    jnp.concatenate(
                        [jnp.where(inside, edge_band[s], 0.0) for s in range(2)], axis=0
                    )
                )
            high, low_part = halves(jnp.concatenate(parts, axis=1))
            columns = []
            for side_high, side_low in sides:
                out = mm(side_high, high) + mm(side_low, high) + mm(side_high, low_part)
                columns.append(jnp.concatenate([out[:, :XB], out[:, XB:]], axis=0))
            high, low_part = halves(main + jnp.concatenate(columns, axis=1))
            out = mm(down[0], high) + mm(down[0], low_part) + mm(down[1], high)
            planes = pl.ds(i * 4, 4)
            coef[0, planes] = out[:, :XB].reshape(4, YB, XB)
            coef[1, planes] = out[:, XB:].reshape(4, YB, XB)
            return carry

        lax.fori_loop(0, 4, quarter, 0)

    tile_rows = lax.broadcasted_iota(jnp.int32, (8, XB), 0)
    one, zero = jnp.ones((8, XB), f32), jnp.zeros((8, XB), f32)
    top = jnp.where(tile_rows < SLOTS, one, zero)
    bottom = 1.0 - top
    flat = jnp.where(jnp.full((8, XB), j, jnp.int32) == 0, one, zero)
    deep = 1.0 - flat

    def slot_of(u):
        return u * CHUNK + q * SLOTS + tile_rows % SLOTS

    def first_of(u):
        return jnp.where(slot_of(u) == 0, one, zero)

    def turned(value):
        return pltpu.roll(value, SLOTS, 0)

    pi2 = np.float32(math.pi * math.pi)
    kz = jnp.full((8, XB), j, jnp.int32).astype(f32) * np.float32(2.0 * math.pi / NZ)

    def square_of(u):
        ky = slot_of(u).astype(f32) * np.float32(2.0 * math.pi / NY)
        return ky * ky + kz * kz + pi2 * bottom * (first_of(u) * deep + flat)

    squares = (square_of(0), pi2 + pi2 * bottom, square_of(1))
    scale = np.float32((0.5 * reference_speed * time_step) ** 2)

    def fill_kappa(kc, carry):
        kx2 = xt_ref[2, pl.ds(kc, 1), :]
        for g, part in enumerate(squares):
            v2 = scale * (kx2 + part)
            series = 1.0 + v2 * np.float32(-1.0 / 110.0)
            series = 1.0 + v2 * np.float32(-1.0 / 72.0) * series
            series = 1.0 + v2 * np.float32(-1.0 / 42.0) * series
            series = 1.0 + v2 * np.float32(-1.0 / 20.0) * series
            kappa[g, kc] = 1.0 + v2 * np.float32(-1.0 / 6.0) * series
        return carry

    loaded(2)
    lax.fori_loop(0, COLS, fill_kappa, 0)

    for edge in y_edges():
        edge.start()
    loaded(3, 4)
    fill_bands()
    fill_damping()

    def lines(ref, f):
        return ref[f].reshape(NY, XB)

    def put_col(f, value):
        col_out[f] = value.reshape(2, 2 * COLS, 2 * SLOTS, XB)
        send_col(f, 0)
        send_col(f, 1)

    def row_product(table, values):
        parts = [halves(v) for v in values]
        high = [part[0] for part in parts]
        low_part = [part[1] for part in parts]
        if len(values) == 1:
            both = mm(table[0], jnp.concatenate([high[0], low_part[0]], axis=1))
            return [both[:, :XB] + both[:, XB:] + mm(table[1], high[0])]
        high = jnp.concatenate(high, axis=1)
        low_part = jnp.concatenate(low_part, axis=1)
        result = mm(table[0], high) + mm(table[0], low_part) + mm(table[1], high)
        return [result[:, :XB], result[:, XB:]]

    def y_derivative(value, sign):
        tiles = value.reshape(NY // 8, 8, XB)
        same = tiles * yd_ref[0]
        cross = pltpu.roll(tiles, SLOTS, 1) * yd_ref[1]
        return (cross + same if sign > 0 else cross - same).reshape(NY, XB)

    def x_forward(f, u):
        first, groups = first_of(u), 2 - u
        general = (1.0 - first) * deep
        rest = (1.0 - first) * flat
        lone = first * deep
        re_r, re_turned_r = top + bottom * lone, bottom * general
        re_i, re_turned_i = bottom * general, bottom * flat - top * general
        im_r, im_turned_r = -bottom * general, top * (general + rest)
        im_i, im_turned_i = top * general + lone + bottom * rest, bottom * general
        for n in range(COLS):
            tr, ti = col_in[f, u, n], col_in[f, u, COLS + n]
            rr, ri = turned(tr), turned(ti)
            xb[0, 0, n] = re_r * tr + re_turned_r * rr + re_i * ti + re_turned_i * ri
            xb[0, 1, n] = im_r * tr + im_turned_r * rr + im_i * ti + im_turned_i * ri
            if u == 0:
                xb[1, 0, n] = first * flat * (top * rr + bottom * ti)
                xb[1, 1, n] = zero

        def group(g, carry):
            values = [(xb[g, 0, n], xb[g, 1, n]) for n in range(COLS)]
            values = short_transform(values, -1.0)
            for kc in range(COLS):
                re, im = values[kc]
                cs, sn = xt_ref[0, kc : kc + 1, :], xt_ref[1, kc : kc + 1, :]
                xs[g, kc, :, :XB] = re * cs + im * sn
                xs[g, kc, :, XB:] = im * cs - re * sn
            return carry

        lax.fori_loop(0, groups, group, 0)
        high, low_part = halves(xs[:groups].reshape(groups * COLS * 8, 2 * XB))
        out = mm(high, wx_ref[0]) + mm(low_part, wx_ref[0]) + mm(high, wx_ref[1])
        return out.reshape(groups, COLS, 8, 2 * XB)

    def kappa_of(u):
        return kappa[0:2] if u == 0 else kappa[2:3]

    def x_derivative(re, im, sign):
        same = xt_ref[3][None, :, None, :]
        cross = xt_ref[4][None, :, None, :]
        if sign > 0:
            return -(re * same + im * cross), re * cross - im * same
        return re * same - im * cross, im * same + re * cross

    def x_inverse(value, f, u):
        first, groups = first_of(u), 2 - u
        high, low_part = halves(value.reshape(groups * COLS * 8, 2 * XB))
        out = mm(high, ux_ref[0]) + mm(low_part, ux_ref[0]) + mm(high, ux_ref[1])
        xs[:groups] = out.reshape(groups, COLS, 8, 2 * XB)

        def group(g, carry):
            values = []
            for kc in range(COLS):
                re, im = xs[g, kc, :, :XB], xs[g, kc, :, XB:]
                cs, sn = xt_ref[0, kc : kc + 1, :], xt_ref[1, kc : kc + 1, :]
                values.append((re * cs - im * sn, im * cs + re * sn))
            values = short_transform(values, 1.0)
            for n in range(COLS):
                xb[g, 0, n] = values[n][0]
                xb[g, 1, n] = values[n][1]
            return carry

        lax.fori_loop(0, groups, group, 0)
        half = 0.5 * (1.0 - first) * deep
        rest = (1.0 - first) * flat
        lone = first * deep
        r_re = top * half + top * flat + lone
        r_re_turned = top * half
        r_im, r_im_turned = -bottom * half, bottom * (half + rest)
        i_re, i_re_turned = bottom * half, top * flat - bottom * half
        i_im, i_im_turned = top * half + lone + bottom * rest, top * half
        for n in range(COLS):
            vr, vi = xb[0, 0, n], xb[0, 1, n]
            wr, wi = turned(vr), turned(vi)
            out_r = r_re * vr + r_re_turned * wr + r_im * vi + r_im_turned * wi
            out_i = i_re * vr + i_re_turned * wr + i_im * vi + i_im_turned * wi
            if u == 0:
                extra = first * flat * bottom
                out_r = out_r + extra * turned(xb[1, 0, n])
                out_i = out_i + extra * xb[1, 0, n]
            bcol_out[f, u, n] = out_r
            bcol_out[f, u, COLS + n] = out_i

    loaded(5)
    arrived("row", 0)
    put_col(0, row_product(fy_ref, [lines(row_in, 0)])[0])

    for edge in y_edges():
        edge.wait_recv()
    pack_edges()
    for edge in x_edges():
        edge.start()
    loaded(7, 8)
    fill_raw()

    loaded(6, 9)
    for u in range(2):
        arrived("col", 0, u)
        spectrum = x_forward(0, u)
        re, im = spectrum[..., :XB] * kappa_of(u), spectrum[..., XB:] * kappa_of(u)
        dre, dim = x_derivative(re, im, 1)
        x_inverse(jnp.concatenate([dre, dim], axis=-1), 0, u)
        send_bcol(0, u)
        if u == 1:
            send_bcol(1, 0)
        x_inverse(jnp.concatenate([re, im], axis=-1), 1, u)
    send_bcol(1, 1)

    for edge in x_edges():
        edge.wait_recv()
    smooth()
    loaded(10, 11, 12, 13, 14)

    arrived("bcol", 0, 0)
    arrived("bcol", 0, 1)
    brow_out[0] = row_product(gy_ref, [lines(bcol_in, 0)])[0].reshape(ROWS, YB, XB)
    send_brow(0)

    dx = damp[0:8]

    arrived("brow", 0)

    def update_x(rows):
        grad = depth_inverse(load(brow_in.at[0], rows))
        fresh = []
        for z in range(NZ):
            change = time_step * coef[0, z, rows, :] * grad[z]
            fresh.append(dx * (dx * vx_ref[z, rows, :] - change))
        store(vxo_ref, rows, fresh)
        store(row_out.at[1], rows, depth_forward(fresh))

    chunks(update_x)
    send_row(1)

    arrived("bcol", 1, 0)
    arrived("bcol", 1, 1)
    flow = lines(bcol_in, 1)
    plain, slope = row_product(gy_ref, [flow, y_derivative(flow, 1)])
    brow_out[1] = slope.reshape(ROWS, YB, XB)
    send_brow(1)
    brow_out[2] = plain.reshape(ROWS, YB, XB)
    send_brow(2)

    arrived("row", 1)
    put_col(1, row_product(fy_ref, [lines(row_in, 1)])[0])

    arrived("brow", 1)

    def update_y(rows):
        grad = depth_inverse(load(brow_in.at[1], rows))
        dy = damp[pl.ds(pl.multiple_of(rows.start + 8, 8), 8), :]
        fresh = []
        for z in range(NZ):
            change = time_step * coef[0, z, rows, :] * grad[z]
            fresh.append(dy * (dy * vy_ref[z, rows, :] - change))
        store(vyo_ref, rows, fresh)
        store(row_out.at[2], rows, depth_forward(fresh))

    chunks(update_y)
    send_row(2)

    arrived("brow", 2)

    def update_z(rows):
        grad = depth_inverse(depth_derivative(load(brow_in.at[2], rows), 1))
        fresh = []
        for z in range(NZ):
            fresh.append(vz_ref[z, rows, :] - time_step * coef[0, z, rows, :] * grad[z])
        store(vzo_ref, rows, fresh)
        store(row_out.at[3], rows, depth_derivative(depth_forward(fresh), -1))

    chunks(update_z)
    send_row(3)

    arrived("row", 2)
    arrived("row", 3)
    aside, below = row_product(fy_ref, [lines(row_in, 2), lines(row_in, 3)])
    put_col(2, below + y_derivative(aside, -1))

    flows = []
    for u in range(2):
        arrived("col", 1, u)
        flow_x = x_forward(1, u)
        flows.append(x_derivative(flow_x[..., :XB], flow_x[..., XB:], -1))
    for u in range(2):
        arrived("col", 2, u)
        remains = x_forward(2, u)
        tre = (flows[u][0] + remains[..., :XB]) * kappa_of(u)
        tim = (flows[u][1] + remains[..., XB:]) * kappa_of(u)
        x_inverse(jnp.concatenate([tre, tim], axis=-1), 2, u)
        send_bcol(2, u)

    arrived("bcol", 2, 0)
    arrived("bcol", 2, 1)
    brow_out[3] = row_product(gy_ref, [lines(bcol_in, 2)])[0].reshape(ROWS, YB, XB)
    send_brow(3)

    arrived("brow", 3)

    def update_p(rows):
        divergence = depth_inverse(load(brow_in.at[3], rows))
        both = dx * damp[pl.ds(pl.multiple_of(rows.start + 8, 8), 8), :]
        for z in range(NZ):
            change = time_step * coef[1, z, rows, :] * divergence[z]
            po_ref[z, rows, :] = both * (both * p_ref[z, rows, :] - change)

    chunks(update_p)

    for f in range(4):
        all_of("row", f).wait_send()
        all_of("brow", f).wait_send()
    for f in range(3):
        for u in range(2):
            all_of("col", f, u).wait_send()
            all_of("bcol", f, u).wait_send()
    for edge in y_edges() + x_edges():
        edge.wait_send()


def write_kernel(a, b, c, d, a_out, b_out, c_out, d_out, sem):
    pairs = ((a, a_out), (b, b_out), (c, c_out), (d, d_out))
    copies = [pltpu.make_async_copy(x, y, sem.at[n]) for n, (x, y) in enumerate(pairs)]
    for copy in copies:
        copy.start()
    for copy in copies:
        copy.wait()


def on_device(
    labels, pressure, velocity_x, velocity_y, velocity_z,
    speed_table, density_table, filter_taps, layer_width,
):
    fy, gy, yd = row_tables()
    wx, ux, xt = column_tables()
    brick = jax.ShapeDtypeStruct(pressure.shape, f32)
    row_buffer = lambda n: pltpu.VMEM((n, ROWS, YB, XB), f32)
    col_buffer = lambda n: pltpu.VMEM((n, 2, 2 * COLS, 2 * SLOTS, XB), f32)
    hold = lambda t: pltpu.with_memory_space_constraint(t, pltpu.HBM)
    results = pl.pallas_call(
        step_kernel,
        out_shape=(brick,) * 4,
        in_specs=[pl.BlockSpec(memory_space=pl.ANY)] * 15,
        out_specs=(pl.BlockSpec(memory_space=pltpu.VMEM),) * 4,
        scratch_shapes=[
            row_buffer(4), row_buffer(4), col_buffer(3), col_buffer(3),
            col_buffer(3), col_buffer(3), row_buffer(4), row_buffer(4),
            pltpu.VMEM((3, COLS, 8, XB), f32),
            pltpu.VMEM((2, 2, COLS, 8, XB), f32),
            pltpu.VMEM((2, COLS, 8, 2 * XB), f32),
            pltpu.VMEM((2, NZ, YB, XB), f32),
            pltpu.VMEM((NZ, 2 * YB, XB), f32),
            pltpu.VMEM((2, XB, XB), f32),
            pltpu.VMEM((2, XB, XB), f32),
            pltpu.VMEM((NZ * 2 * YB, 2 * XB), f32),
            pltpu.VMEM((2, 2 * XB, 2 * XB), bf16),
            pltpu.VMEM((2, XB, XB), f32),
            pltpu.VMEM((2, 4 * YB, 8 * YB), bf16),
            pltpu.VMEM((8 + YB, XB), f32),
            pltpu.VMEM(labels.shape, jnp.int32),
            *[pltpu.VMEM(pressure.shape, f32)] * 4,
            pltpu.SMEM((LABELS,), f32), pltpu.SMEM((LABELS,), f32),
            pltpu.SMEM((TAPS,), f32), pltpu.SMEM((4,), jnp.int32),
            *[pltpu.VMEM(t.shape, t.dtype) for t in (fy, gy, yd, wx, ux, xt)],
            pltpu.SemaphoreType.DMA((24,)),
            pltpu.SemaphoreType.DMA((24,)),
            pltpu.SemaphoreType.DMA((15,)),
        ],
        compiler_params=pltpu.CompilerParams(
            collective_id=0, has_side_effects=True, vmem_limit_bytes=STEP_BYTES
        ),
    )(
        *[
            hold(t)
            for t in (
                labels, pressure, velocity_x, velocity_y, velocity_z,
                speed_table, density_table, filter_taps, layer_width,
                jnp.asarray(fy), jnp.asarray(gy), jnp.asarray(yd),
                jnp.asarray(wx), jnp.asarray(ux), jnp.asarray(xt),
            )
        ]
    )
    return pl.pallas_call(
        write_kernel,
        out_shape=(brick,) * 4,
        in_specs=[pl.BlockSpec(memory_space=pltpu.VMEM)] * 4,
        out_specs=(pl.BlockSpec(memory_space=pl.ANY),) * 4,
        scratch_shapes=[pltpu.SemaphoreType.DMA((4,))],
        compiler_params=pltpu.CompilerParams(vmem_limit_bytes=WRITE_BYTES),
    )(*results)


def solution(mesh):
    brick = P(None, "row", "col")
    return jax.shard_map(
        on_device,
        mesh=mesh,
        in_specs=(brick,) * 5 + (P(),) * 4,
        out_specs=(brick,) * 4,
        check_vma=False,
    )
```

```python
import functools
import math

import jax
import jax.numpy as jnp
import numpy as np
from jax import lax
from jax.experimental import pallas as pl
from jax.experimental.pallas import tpu as pltpu
from jax.sharding import PartitionSpec as P

time_step = 0.15
reference_speed = 2.0
absorption = 6.0
MESH = pl.DeviceIdType.MESH

NZ, NY, NX = 16, 512, 2048
ROWS, COLS = 16, 16
YB, XB = NY // ROWS, NX // COLS
SLOTS, HALO = 4, 16
CHUNK = 2 * COLS * SLOTS
STEP_BYTES, WRITE_BYTES = 40 << 20, 4 << 20
TAPS, LABELS = 33, 12
f32, bf16 = jnp.float32, jnp.bfloat16


def split_table(table):
    high = table.astype(np.float32).astype(bf16)
    low = (table - high.astype(np.float64)).astype(np.float32).astype(bf16)
    return np.stack([high, low])


def row_tables():
    slot = np.arange(NY // 2)
    y = np.arange(NY)
    angle = 2.0 * np.pi * ((slot[:, None] * y[None, :]) % NY) / NY
    real, imag = np.cos(angle), -np.sin(angle)
    imag[0] = np.where(y % 2 == 0, 1.0, -1.0)

    def order(a, b):
        pair = [t.reshape((2 * 2 * COLS, SLOTS) + t.shape[1:]) for t in (a, b)]
        return np.stack(pair, axis=1)

    forward = order(real, imag).reshape(NY, NY)
    weight = np.where(slot == 0, 1.0, 2.0)[:, None] / NY
    inverse = order(real * weight, imag * weight).reshape(NY, NY).T
    return split_table(forward), split_table(inverse)


def column_tables():
    x = np.arange(XB)
    angle = 2.0 * np.pi * ((x[:, None] * x[None, :]) % XB) / XB
    c, s = np.cos(angle), np.sin(angle)
    forward = np.block([[c, -s], [s, c]])
    inverse = np.block([[c, s], [-s, c]]) / NX
    kc = np.arange(COLS)
    twist = 2.0 * np.pi * (kc[:, None] * x[None, :]) / NX
    index = kc[:, None] + COLS * x[None, :]
    wave = 2.0 * np.pi * np.where(index < NX // 2, index, index - NX) / NX
    same = wave * np.sin(0.5 * wave)
    cross = wave * np.cos(0.5 * wave)
    small = np.stack([np.cos(twist), np.sin(twist), wave * wave, same, cross]).astype(np.float32)
    return split_table(forward), split_table(inverse), small


def scaled(value, factor):
    if abs(factor - 1.0) < 1e-12:
        return value
    if abs(factor + 1.0) < 1e-12:
        return -value
    return value * np.float32(factor)


def weighted(terms):
    total = None
    for value, factor in terms:
        if abs(factor) < 1e-12:
            continue
        if total is None:
            total = scaled(value, factor)
        elif abs(factor + 1.0) < 1e-12:
            total = total - value
        else:
            total = total + scaled(value, factor)
    return total


def cos16(n):
    return math.cos(2.0 * math.pi * (n % 16) / 16)


def sin16(n):
    return math.sin(2.0 * math.pi * (n % 16) / 16)


def depth_forward(p):
    even = [p[0]] + [p[n] + p[16 - n] for n in range(1, 8)] + [p[8]]
    odd = [None] + [p[n] - p[16 - n] for n in range(1, 8)]
    plus = [even[n] + even[8 - n] for n in range(4)] + [even[4]]
    minus = [even[n] - even[8 - n] for n in range(4)]
    odd_plus = [None] + [odd[n] + odd[8 - n] for n in range(1, 4)] + [odd[4]]
    odd_minus = [None] + [odd[n] - odd[8 - n] for n in range(1, 4)]

    def real_of(k):
        side = plus if k % 2 == 0 else minus
        return weighted([(side[n], cos16(k * n)) for n in range(len(side))])

    def imag_of(k):
        if k % 2 == 0:
            return weighted([(odd_minus[n], -sin16(k * n)) for n in range(1, 4)])
        return weighted([(odd_plus[n], -sin16(k * n)) for n in range(1, 5)])

    out = [real_of(0), real_of(8)]
    for k in range(1, 8):
        out += [real_of(k), imag_of(k)]
    return out


def depth_inverse(m):
    real = [m[0]] + [m[2 * k] for k in range(1, 8)] + [m[1]]
    imag = [None] + [m[2 * k + 1] for k in range(1, 8)]
    weight = [1.0 / 16] + [2.0 / 16] * 7 + [1.0 / 16]

    def terms(values, ids, n, wave):
        return weighted([(values[k], weight[k] * wave(k * n)) for k in ids])

    out = [None] * 16
    for n in range(0, 5):
        ce = terms(real, range(0, 9, 2), n, cos16)
        co = terms(real, range(1, 9, 2), n, cos16)
        so = terms(imag, range(1, 8, 2), n, lambda v: -sin16(v))
        se = terms(imag, range(2, 8, 2), n, lambda v: -sin16(v))
        near = ce if co is None else ce + co
        far = ce if co is None else ce - co
        if n == 0:
            out[0], out[8] = near, far
            continue
        if se is None:
            d_near, d_far = so, so
        else:
            d_near, d_far = so + se, so - se
        out[n], out[16 - n] = near + d_near, near - d_near
        if n < 4:
            out[8 - n], out[8 + n] = far + d_far, far - d_far
    return out


def depth_derivative(m, sign):
    out = [jnp.zeros_like(m[0]), m[1] * np.float32(-sign * math.pi)]
    for k in range(1, 8):
        wave = 2.0 * math.pi * k / 16
        a = np.float32(-sign * wave * math.sin(0.5 * wave))
        b = np.float32(wave * math.cos(0.5 * wave))
        out += [m[2 * k] * a - m[2 * k + 1] * b, m[2 * k + 1] * a + m[2 * k] * b]
    return out


def short_transform(values, sign):
    count = len(values)
    if count == 1:
        return values
    even = short_transform(values[0::2], sign)
    odd = short_transform(values[1::2], sign)
    out = [None] * count
    for k in range(count // 2):
        angle = sign * 2.0 * math.pi * k / count
        c, s = math.cos(angle), math.sin(angle)
        re, im = odd[k]
        if k == 0:
            tr, ti = re, im
        elif abs(c) < 1e-9:
            tr, ti = (-im, re) if s > 0 else (im, -re)
        elif abs(abs(c) - abs(s)) < 1e-9:
            h = np.float32(abs(c))
            cs, ss = (1 if c > 0 else -1), (1 if s > 0 else -1)
            first = re if cs > 0 else -re
            tr = (first - im if ss > 0 else first + im) * h
            second = im if cs > 0 else -im
            ti = (second + re if ss > 0 else second - re) * h
        else:
            tr = re * np.float32(c) - im * np.float32(s)
            ti = re * np.float32(s) + im * np.float32(c)
        er, ei = even[k]
        out[k] = (er + tr, ei + ti)
        out[k + count // 2] = (er - tr, ei - ti)
    return out


def halves(value):
    high = value.astype(bf16)
    low = (value - high.astype(f32)).astype(bf16)
    return high, low


def mm(a, b):
    return jnp.dot(a, b, preferred_element_type=f32)


def step_kernel(
    lab_hbm, p_hbm, vx_hbm, vy_hbm, vz_hbm, speed_hbm, density_hbm, taps_hbm, width_hbm,
    fy_hbm, gy_hbm, wx_hbm, ux_hbm, xt_hbm,
    po_ref, vxo_ref, vyo_ref, vzo_ref,
    row_out, row_in, col_out, col_in, bcol_out, bcol_in, brow_out, brow_in,
    kappa, xb, xs, coef, lab, edge_out, edge_in, raw, across, edge_band, down, damp,
    lab_ref, p_ref, vx_ref, vy_ref, vz_ref, speed_ref, density_ref, taps_ref, width_ref,
    fy_ref, gy_ref, wx_ref, ux_ref, xt_ref, yd_ref,
    send_sem, recv_sem, load_sem,
):
    def loaded(*numbers):
        for n in numbers:
            fetches[n].wait()

    r, c = lax.axis_index("row"), lax.axis_index("col")
    j, h = r // 2, r % 2
    q = h * COLS + c

    barrier = pltpu.get_barrier_semaphore()

    x_low, y_chip, core = r // 8, (r // 2) % 4, r % 2
    z_chip, x_high = c // 2, c % 2

    def pick(i, values):
        value = jnp.int32(values[0])
        for n in range(1, len(values)):
            value = jnp.where(i == n, jnp.int32(values[n]), value)
        return value

    def row_partner(i, other):
        x = (x_low + pick(i, (1, 0, 1, 1, 0, 0, 1, 0))) % 2
        y = (y_chip + pick(i, (2, 2, 1, 3, 1, 3, 0, 0))) % 4
        return (x * 4 + y) * 2 + (core + other) % 2

    def plane_partner(i, other):
        z = (z_chip + pick(i, (4, 3, 5, 4, 2, 6, 3, 5, 1, 7, 2, 6, 0, 1, 7, 0))) % 8
        x = (x_high + pick(i, (1, 1, 1, 0, 1, 1, 0, 0, 1, 1, 0, 0, 1, 0, 0, 0))) % 2
        return (core + other) % 2 * COLS + z * 2 + x

    def each_partner(partner, classes, body):
        def step(i, carry):
            body(partner(i, 0))
            body(partner(i, 1))
            return carry

        lax.fori_loop(0, classes - 1, step, 0)
        body(partner(classes - 1, 1))

    def row_device(t):
        return (t, c)

    def plane_device(t):
        return (2 * j + t // COLS, t % COLS)

    def greet(device):
        pl.semaphore_signal(barrier, inc=1, device_id=device, device_id_type=MESH)

    each_partner(plane_partner, COLS, lambda t: greet(plane_device(t)))
    each_partner(row_partner, ROWS // 2, lambda t: greet(row_device(t)))

    fetches = [
        pltpu.make_async_copy(source, target, load_sem.at[n])
        for n, (source, target) in enumerate(
            [
                (p_hbm, p_ref), (lab_hbm, lab_ref), (xt_hbm, xt_ref), (taps_hbm, taps_ref),
                (width_hbm, width_ref), (fy_hbm, fy_ref), (wx_hbm, wx_ref),
                (speed_hbm, speed_ref), (density_hbm, density_ref), (ux_hbm, ux_ref),
                (gy_hbm, gy_ref), (vx_hbm, vx_ref), (vy_hbm, vy_ref),
                (vz_hbm, vz_ref),
            ]
        )
    ]
    for fetch in fetches:
        fetch.start()
    def start_all(src, dst, sem, partner, classes, device_of, own):
        def start(t):
            pltpu.make_async_remote_copy(
                src_ref=src.at[t], dst_ref=dst.at[own], send_sem=send_sem.at[sem],
                recv_sem=recv_sem.at[sem], device_id=device_of(t), device_id_type=MESH,
            ).start()

        each_partner(partner, classes, start)
        dst[own] = src[own]

    def row_all(src, dst, sem):
        start_all(src, dst, sem, row_partner, ROWS // 2, row_device, r)

    def plane_all(src, dst, sem):
        start_all(src, dst, sem, plane_partner, COLS, plane_device, q)

    def whole(src, dst, sem, count):
        span = pl.ds(0, count - 1)
        return pltpu.make_async_remote_copy(
            src_ref=src.at[span], dst_ref=dst.at[span], send_sem=send_sem.at[sem],
            recv_sem=recv_sem.at[sem], device_id=((r + 1) % ROWS, c), device_id_type=MESH,
        )

    def send_row(f):
        row_all(row_out.at[f], row_in.at[f], f)

    def send_col(f, u):
        plane_all(col_out.at[f, u], col_in.at[f, u], 4 + 2 * f + u)

    def send_bcol(f, u):
        plane_all(bcol_out.at[f, u], bcol_in.at[f, u], 10 + 2 * f + u)

    def send_brow(f):
        row_all(brow_out.at[f], brow_in.at[f], 16 + f)

    def all_of(kind, f, u=None):
        if kind == "row":
            return whole(row_out.at[f], row_in.at[f], f, ROWS)
        if kind == "brow":
            return whole(brow_out.at[f], brow_in.at[f], 16 + f, ROWS)
        if kind == "col":
            return whole(col_out.at[f, u], col_in.at[f, u], 4 + 2 * f + u, 2 * COLS)
        return whole(bcol_out.at[f, u], bcol_in.at[f, u], 10 + 2 * f + u, 2 * COLS)

    def arrived(kind, f, u=None):
        all_of(kind, f, u).wait_recv()

    def load(ref, rows):
        return [ref[z, rows, :] for z in range(NZ)]

    def store(ref, rows, planes):
        for z in range(NZ):
            ref[z, rows, :] = planes[z]

    def chunks(body):
        def step(i, carry):
            body(pl.ds(pl.multiple_of(i * 8, 8), 8))
            return carry

        lax.fori_loop(0, YB // 8, step, 0)

    def pressure_planes(rows):
        store(row_out.at[0], rows, depth_forward(load(p_ref, rows)))

    loaded(0)
    chunks(pressure_planes)
    pl.semaphore_wait(barrier, ROWS - 1 + 2 * COLS - 1)
    send_row(0)

    loaded(1)
    for z in range(NZ):
        lab[z, HALO : HALO + YB, :] = lab_ref[z].astype(f32)

    def y_edges():
        before, after = (r + ROWS - 1) % ROWS, (r + 1) % ROWS
        return [
            pltpu.make_async_remote_copy(
                src_ref=lab.at[:, pl.ds(HALO, HALO), :],
                dst_ref=lab.at[:, pl.ds(HALO + YB, HALO), :],
                send_sem=send_sem.at[20], recv_sem=recv_sem.at[20],
                device_id=(before, c), device_id_type=MESH,
            ),
            pltpu.make_async_remote_copy(
                src_ref=lab.at[:, pl.ds(YB, HALO), :],
                dst_ref=lab.at[:, pl.ds(0, HALO), :],
                send_sem=send_sem.at[21], recv_sem=recv_sem.at[21],
                device_id=(after, c), device_id_type=MESH,
            ),
        ]

    def x_edges():
        before, after = (c + COLS - 1) % COLS, (c + 1) % COLS
        return [
            pltpu.make_async_remote_copy(
                src_ref=edge_out.at[0], dst_ref=edge_in.at[1],
                send_sem=send_sem.at[22], recv_sem=recv_sem.at[22],
                device_id=(r, before), device_id_type=MESH,
            ),
            pltpu.make_async_remote_copy(
                src_ref=edge_out.at[1], dst_ref=edge_in.at[0],
                send_sem=send_sem.at[23], recv_sem=recv_sem.at[23],
                device_id=(r, after), device_id_type=MESH,
            ),
        ]

    def ids(shape, dim):
        return lax.broadcasted_iota(jnp.int32, shape, dim)

    def banded(offset):
        def tap(t, total):
            return jnp.where(offset == t, taps_ref[t], total)

        return lax.fori_loop(0, TAPS, tap, jnp.zeros(offset.shape, f32), unroll=3)

    def fill_bands():
        wide = (XB, XB)
        band = banded(ids(wide, 0) - ids(wide, 1) + HALO)
        none = jnp.zeros(wide, bf16)
        for part, value in enumerate(halves(band)):
            top_rows = jnp.concatenate([value, none], axis=1)
            low_rows = jnp.concatenate([none, value], axis=1)
            across[part] = jnp.concatenate([top_rows, low_rows], axis=0)
        edge_band[0] = banded(ids(wide, 0) % HALO - ids(wide, 1))
        edge_band[1] = banded(ids(wide, 0) % HALO - ids(wide, 1) + XB + HALO)
        tall = (4 * YB, 8 * YB)
        row, line = ids(tall, 0), ids(tall, 1)
        offset = jnp.where(row // YB == line // (2 * YB), line % (2 * YB) - row % YB, -1)
        for part, value in enumerate(halves(banded(offset))):
            down[part] = value

    def fill_damping():
        def absorb(position, length, low_width, high_width):
            size = position.shape
            low_side = jnp.maximum(low_width - position, 0).astype(f32)
            high_side = jnp.maximum(position - (length - 1 - high_width), 0).astype(f32)
            low_side = low_side / jnp.full(size, low_width, jnp.int32).astype(f32)
            high_side = high_side / jnp.full(size, high_width, jnp.int32).astype(f32)
            low_side, high_side = low_side * low_side, high_side * high_side
            total = low_side * low_side + high_side * high_side
            return jnp.exp((-0.5 * time_step * absorption * reference_speed) * total)

        damp[0:8] = absorb(c * XB + ids((8, XB), 1), NX, width_ref[0], width_ref[1])
        damp[8:] = absorb(r * YB + ids((YB, XB), 0), NY, width_ref[2], width_ref[3])

    def pack_edges():
        wide = (XB, XB)
        source, target = ids(wide, 0), ids(wide, 1)
        total = None
        for g in range(8):
            here = target // HALO == g
            first_lanes = here & (source == target % HALO)
            last_lanes = here & (source == target % HALO + XB - HALO)
            select = jnp.concatenate(
                [jnp.where(first_lanes, 1.0, 0.0), jnp.where(last_lanes, 1.0, 0.0)], axis=1
            ).astype(bf16)
            part = mm(lab[2 * g : 2 * g + 2].reshape(XB, XB).astype(bf16), select)
            total = part if total is None else total + part
        edge_out[0] = total[:, :XB]
        edge_out[1] = total[:, XB:]

    def tables():
        density = [jnp.full((8, XB), density_ref[n], f32) for n in range(LABELS)]
        speed = [jnp.full((8, XB), speed_ref[n], f32) for n in range(LABELS)]
        return [1.0 / d for d in density], [d * s * s for d, s in zip(density, speed)]

    def look_up(label, table):
        value = jnp.broadcast_to(table[0][None], label.shape)
        for n in range(1, LABELS):
            value = jnp.where(label == float(n), table[n][None], value)
        return value

    def fill_raw():
        buoyancy_of, modulus_of = tables()

        def plane(z, carry):
            label = lab[z].reshape(8, 8, XB)
            rows = pl.ds(pl.multiple_of(z * 2 * YB, 2 * YB), 2 * YB)
            raw[rows, :XB] = look_up(label, buoyancy_of).reshape(2 * YB, XB)
            raw[rows, XB:] = look_up(label, modulus_of).reshape(2 * YB, XB)
            return carry

        lax.fori_loop(0, NZ, plane, 0)

    def smooth():
        buoyancy_of, modulus_of = tables()
        edges = [edge_in[0].reshape(16, 8, XB), edge_in[1].reshape(16, 8, XB)]
        sides = [
            halves(jnp.concatenate([look_up(e, t).reshape(XB, XB) for e in edges], axis=1))
            for t in (buoyancy_of, modulus_of)
        ]
        group_of = ids((XB, XB), 0) // HALO

        def quarter(i, carry):
            rows = pl.ds(pl.multiple_of(i * 8 * YB, 8 * YB), 8 * YB)
            high, low_part = halves(raw[rows, :])
            main = mm(high, across[0]) + mm(low_part, across[0]) + mm(high, across[1])
            parts = []
            for g in range(2):
                inside = group_of == 2 * i + g
                parts.append(
                    jnp.concatenate(
                        [jnp.where(inside, edge_band[s], 0.0) for s in range(2)], axis=0
                    )
                )
            high, low_part = halves(jnp.concatenate(parts, axis=1))
            columns = []
            for side_high, side_low in sides:
                out = mm(side_high, high) + mm(side_low, high) + mm(side_high, low_part)
                columns.append(jnp.concatenate([out[:, :XB], out[:, XB:]], axis=0))
            high, low_part = halves(main + jnp.concatenate(columns, axis=1))
            out = mm(down[0], high) + mm(down[0], low_part) + mm(down[1], high)
            planes = pl.ds(i * 4, 4)
            coef[0, planes] = out[:, :XB].reshape(4, YB, XB)
            coef[1, planes] = out[:, XB:].reshape(4, YB, XB)
            return carry

        lax.fori_loop(0, 4, quarter, 0)

    tile_rows = lax.broadcasted_iota(jnp.int32, (8, XB), 0)
    one, zero = jnp.ones((8, XB), f32), jnp.zeros((8, XB), f32)
    top = jnp.where(tile_rows < SLOTS, one, zero)
    bottom = 1.0 - top
    flat = jnp.where(jnp.full((8, XB), j, jnp.int32) == 0, one, zero)
    deep = 1.0 - flat

    def slot_of(u):
        return u * CHUNK + q * SLOTS + tile_rows % SLOTS

    def first_of(u):
        return jnp.where(slot_of(u) == 0, one, zero)

    def turned(value):
        return pltpu.roll(value, SLOTS, 0)

    pi2 = np.float32(math.pi * math.pi)
    kz = jnp.full((8, XB), j, jnp.int32).astype(f32) * np.float32(2.0 * math.pi / NZ)

    def square_of(u):
        ky = slot_of(u).astype(f32) * np.float32(2.0 * math.pi / NY)
        return ky * ky + kz * kz + pi2 * bottom * (first_of(u) * deep + flat)

    squares = (square_of(0), pi2 + pi2 * bottom, square_of(1))
    scale = np.float32((0.5 * reference_speed * time_step) ** 2)

    def fill_kappa(kc, carry):
        kx2 = xt_ref[2, pl.ds(kc, 1), :]
        for g, part in enumerate(squares):
            v2 = scale * (kx2 + part)
            series = 1.0 + v2 * np.float32(-1.0 / 110.0)
            series = 1.0 + v2 * np.float32(-1.0 / 72.0) * series
            series = 1.0 + v2 * np.float32(-1.0 / 42.0) * series
            series = 1.0 + v2 * np.float32(-1.0 / 20.0) * series
            kappa[g, kc] = 1.0 + v2 * np.float32(-1.0 / 6.0) * series
        return carry

    loaded(2)
    lax.fori_loop(0, COLS, fill_kappa, 0)

    for edge in y_edges():
        edge.start()
    loaded(3, 4)
    fill_bands()
    fill_damping()

    def lines(ref, f):
        return ref[f].reshape(NY, XB)

    def put_col(f, value):
        col_out[f] = value.reshape(2, 2 * COLS, 2 * SLOTS, XB)
        send_col(f, 0)
        send_col(f, 1)

    def row_product(table, values):
        parts = [halves(v) for v in values]
        high = [part[0] for part in parts]
        low_part = [part[1] for part in parts]
        if len(values) == 1:
            both = mm(table[0], jnp.concatenate([high[0], low_part[0]], axis=1))
            return [both[:, :XB] + both[:, XB:] + mm(table[1], high[0])]
        high = jnp.concatenate(high, axis=1)
        low_part = jnp.concatenate(low_part, axis=1)
        result = mm(table[0], high) + mm(table[0], low_part) + mm(table[1], high)
        return [result[:, :XB], result[:, XB:]]

    def fill_slopes(n, carry):
        slots = n * SLOTS + tile_rows % SLOTS
        angle = slots.astype(f32) * np.float32(math.pi / NY)
        square = angle * angle
        sine, cosine = one, one
        for k in range(6, 0, -1):
            sine = 1.0 - square * np.float32(1.0 / (2 * k * (2 * k + 1))) * sine
        for k in range(7, 0, -1):
            cosine = 1.0 - square * np.float32(1.0 / (2 * k * (2 * k - 1))) * cosine
        same = -2.0 * square * sine
        edge = jnp.where(slots == 0, bottom * np.float32(math.pi), zero)
        yd_ref[0, n] = same - edge
        yd_ref[1, n] = 2.0 * angle * cosine * (bottom - top)
        return carry

    def y_derivative(value, sign):
        tiles = value.reshape(NY // 8, 8, XB)
        same = tiles * yd_ref[0]
        cross = pltpu.roll(tiles, SLOTS, 1) * yd_ref[1]
        return (cross + same if sign > 0 else cross - same).reshape(NY, XB)

    def x_forward(f, u):
        first, groups = first_of(u), 2 - u
        general = (1.0 - first) * deep
        rest = (1.0 - first) * flat
        lone = first * deep
        re_r, re_turned_r = top + bottom * lone, bottom * general
        re_i, re_turned_i = bottom * general, bottom * flat - top * general
        im_r, im_turned_r = -bottom * general, top * (general + rest)
        im_i, im_turned_i = top * general + lone + bottom * rest, bottom * general
        for n in range(COLS):
            tr, ti = col_in[f, u, n], col_in[f, u, COLS + n]
            rr, ri = turned(tr), turned(ti)
            xb[0, 0, n] = re_r * tr + re_turned_r * rr + re_i * ti + re_turned_i * ri
            xb[0, 1, n] = im_r * tr + im_turned_r * rr + im_i * ti + im_turned_i * ri
            if u == 0:
                xb[1, 0, n] = first * flat * (top * rr + bottom * ti)
                xb[1, 1, n] = zero

        def group(g, carry):
            values = [(xb[g, 0, n], xb[g, 1, n]) for n in range(COLS)]
            values = short_transform(values, -1.0)
            for kc in range(COLS):
                re, im = values[kc]
                cs, sn = xt_ref[0, kc : kc + 1, :], xt_ref[1, kc : kc + 1, :]
                xs[g, kc, :, :XB] = re * cs + im * sn
                xs[g, kc, :, XB:] = im * cs - re * sn
            return carry

        lax.fori_loop(0, groups, group, 0)
        high, low_part = halves(xs[:groups].reshape(groups * COLS * 8, 2 * XB))
        out = mm(high, wx_ref[0]) + mm(low_part, wx_ref[0]) + mm(high, wx_ref[1])
        return out.reshape(groups, COLS, 8, 2 * XB)

    def kappa_of(u):
        return kappa[0:2] if u == 0 else kappa[2:3]

    def x_derivative(re, im, sign):
        same = xt_ref[3][None, :, None, :]
        cross = xt_ref[4][None, :, None, :]
        if sign > 0:
            return -(re * same + im * cross), re * cross - im * same
        return re * same - im * cross, im * same + re * cross

    def x_inverse(value, f, u):
        first, groups = first_of(u), 2 - u
        high, low_part = halves(value.reshape(groups * COLS * 8, 2 * XB))
        out = mm(high, ux_ref[0]) + mm(low_part, ux_ref[0]) + mm(high, ux_ref[1])
        xs[:groups] = out.reshape(groups, COLS, 8, 2 * XB)

        def group(g, carry):
            values = []
            for kc in range(COLS):
                re, im = xs[g, kc, :, :XB], xs[g, kc, :, XB:]
                cs, sn = xt_ref[0, kc : kc + 1, :], xt_ref[1, kc : kc + 1, :]
                values.append((re * cs - im * sn, im * cs + re * sn))
            values = short_transform(values, 1.0)
            for n in range(COLS):
                xb[g, 0, n] = values[n][0]
                xb[g, 1, n] = values[n][1]
            return carry

        lax.fori_loop(0, groups, group, 0)
        half = 0.5 * (1.0 - first) * deep
        rest = (1.0 - first) * flat
        lone = first * deep
        r_re = top * half + top * flat + lone
        r_re_turned = top * half
        r_im, r_im_turned = -bottom * half, bottom * (half + rest)
        i_re, i_re_turned = bottom * half, top * flat - bottom * half
        i_im, i_im_turned = top * half + lone + bottom * rest, top * half
        for n in range(COLS):
            vr, vi = xb[0, 0, n], xb[0, 1, n]
            wr, wi = turned(vr), turned(vi)
            out_r = r_re * vr + r_re_turned * wr + r_im * vi + r_im_turned * wi
            out_i = i_re * vr + i_re_turned * wr + i_im * vi + i_im_turned * wi
            if u == 0:
                extra = first * flat * bottom
                out_r = out_r + extra * turned(xb[1, 0, n])
                out_i = out_i + extra * xb[1, 0, n]
            bcol_out[f, u, n] = out_r
            bcol_out[f, u, COLS + n] = out_i

    loaded(5)
    arrived("row", 0)
    put_col(0, row_product(fy_ref, [lines(row_in, 0)])[0])

    for edge in y_edges():
        edge.wait_recv()
    pack_edges()
    for edge in x_edges():
        edge.start()
    loaded(7, 8)
    fill_raw()
    lax.fori_loop(0, NY // 8, fill_slopes, 0)

    loaded(6, 9)
    for u in range(2):
        arrived("col", 0, u)
        spectrum = x_forward(0, u)
        re, im = spectrum[..., :XB] * kappa_of(u), spectrum[..., XB:] * kappa_of(u)
        x_inverse(jnp.concatenate([re, im], axis=-1), 1, u)
        send_bcol(1, u)
        if u == 1:
            send_bcol(0, 0)
        dre, dim = x_derivative(re, im, 1)
        x_inverse(jnp.concatenate([dre, dim], axis=-1), 0, u)
    send_bcol(0, 1)

    for edge in x_edges():
        edge.wait_recv()
    smooth()
    loaded(10, 11, 12, 13)

    dx = damp[0:8]

    def rows_of_y(rows):
        return damp[pl.ds(pl.multiple_of(rows.start + 8, 8), 8), :]

    def update_x(rows):
        grad = depth_inverse(load(brow_in.at[0], rows))
        fresh = []
        for z in range(NZ):
            change = time_step * coef[0, z, rows, :] * grad[z]
            fresh.append(dx * (dx * vx_ref[z, rows, :] - change))
        store(vxo_ref, rows, fresh)
        store(row_out.at[1], rows, depth_forward(fresh))

    def update_y(rows):
        grad = depth_inverse(load(brow_in.at[1], rows))
        dy = rows_of_y(rows)
        fresh = []
        for z in range(NZ):
            change = time_step * coef[0, z, rows, :] * grad[z]
            fresh.append(dy * (dy * vy_ref[z, rows, :] - change))
        store(vyo_ref, rows, fresh)
        store(row_out.at[2], rows, depth_forward(fresh))

    def update_z(rows):
        grad = depth_inverse(depth_derivative(load(brow_in.at[2], rows), 1))
        fresh = []
        for z in range(NZ):
            fresh.append(vz_ref[z, rows, :] - time_step * coef[0, z, rows, :] * grad[z])
        store(vzo_ref, rows, fresh)
        store(row_out.at[3], rows, depth_derivative(depth_forward(fresh), -1))

    arrived("bcol", 1, 0)
    arrived("bcol", 1, 1)
    flow = lines(bcol_in, 1)
    plain, slope = row_product(gy_ref, [flow, y_derivative(flow, 1)])
    brow_out[1] = slope.reshape(ROWS, YB, XB)
    send_brow(1)
    brow_out[2] = plain.reshape(ROWS, YB, XB)
    send_brow(2)

    arrived("bcol", 0, 0)
    arrived("bcol", 0, 1)
    brow_out[0] = row_product(gy_ref, [lines(bcol_in, 0)])[0].reshape(ROWS, YB, XB)
    send_brow(0)

    arrived("brow", 1)
    chunks(update_y)
    send_row(2)
    arrived("brow", 2)
    chunks(update_z)
    send_row(3)
    arrived("brow", 0)
    chunks(update_x)
    send_row(1)

    arrived("row", 2)
    aside = y_derivative(row_product(fy_ref, [lines(row_in, 2)])[0], -1)
    arrived("row", 3)
    put_col(2, aside + row_product(fy_ref, [lines(row_in, 3)])[0])
    arrived("row", 1)
    put_col(1, row_product(fy_ref, [lines(row_in, 1)])[0])

    remains = []
    for u in range(2):
        arrived("col", 2, u)
        remains.append(x_forward(2, u))
    for u in range(2):
        arrived("col", 1, u)
        flow_x = x_forward(1, u)
        tre, tim = x_derivative(flow_x[..., :XB], flow_x[..., XB:], -1)
        tre = (tre + remains[u][..., :XB]) * kappa_of(u)
        tim = (tim + remains[u][..., XB:]) * kappa_of(u)
        x_inverse(jnp.concatenate([tre, tim], axis=-1), 2, u)
        send_bcol(2, u)

    arrived("bcol", 2, 0)
    arrived("bcol", 2, 1)
    brow_out[3] = row_product(gy_ref, [lines(bcol_in, 2)])[0].reshape(ROWS, YB, XB)
    send_brow(3)

    arrived("brow", 3)

    def update_p(rows):
        divergence = depth_inverse(load(brow_in.at[3], rows))
        both = dx * damp[pl.ds(pl.multiple_of(rows.start + 8, 8), 8), :]
        for z in range(NZ):
            change = time_step * coef[1, z, rows, :] * divergence[z]
            po_ref[z, rows, :] = both * (both * p_ref[z, rows, :] - change)

    chunks(update_p)

    for f in range(4):
        all_of("row", f).wait_send()
        all_of("brow", f).wait_send()
    for f in range(3):
        for u in range(2):
            all_of("col", f, u).wait_send()
            all_of("bcol", f, u).wait_send()
    for edge in y_edges() + x_edges():
        edge.wait_send()


def write_kernel(a, b, c, d, a_out, b_out, c_out, d_out, sem):
    pairs = ((a, a_out), (b, b_out), (c, c_out), (d, d_out))
    copies = [pltpu.make_async_copy(x, y, sem.at[n]) for n, (x, y) in enumerate(pairs)]
    for copy in copies:
        copy.start()
    for copy in copies:
        copy.wait()


def on_device(
    labels, pressure, velocity_x, velocity_y, velocity_z,
    speed_table, density_table, filter_taps, layer_width,
):
    fy, gy = row_tables()
    wx, ux, xt = column_tables()
    brick = jax.ShapeDtypeStruct(pressure.shape, f32)
    row_buffer = lambda n: pltpu.VMEM((n, ROWS, YB, XB), f32)
    col_buffer = lambda n: pltpu.VMEM((n, 2, 2 * COLS, 2 * SLOTS, XB), f32)
    hold = lambda t: pltpu.with_memory_space_constraint(t, pltpu.HBM)
    results = pl.pallas_call(
        step_kernel,
        out_shape=(brick,) * 4,
        in_specs=[pl.BlockSpec(memory_space=pl.ANY)] * 14,
        out_specs=(pl.BlockSpec(memory_space=pltpu.VMEM),) * 4,
        scratch_shapes=[
            row_buffer(4), row_buffer(4), col_buffer(3), col_buffer(3),
            col_buffer(3), col_buffer(3), row_buffer(4), row_buffer(4),
            pltpu.VMEM((3, COLS, 8, XB), f32),
            pltpu.VMEM((2, 2, COLS, 8, XB), f32),
            pltpu.VMEM((2, COLS, 8, 2 * XB), f32),
            pltpu.VMEM((2, NZ, YB, XB), f32),
            pltpu.VMEM((NZ, 2 * YB, XB), f32),
            pltpu.VMEM((2, XB, XB), f32),
            pltpu.VMEM((2, XB, XB), f32),
            pltpu.VMEM((NZ * 2 * YB, 2 * XB), f32),
            pltpu.VMEM((2, 2 * XB, 2 * XB), bf16),
            pltpu.VMEM((2, XB, XB), f32),
            pltpu.VMEM((2, 4 * YB, 8 * YB), bf16),
            pltpu.VMEM((8 + YB, XB), f32),
            pltpu.VMEM(labels.shape, jnp.int32),
            *[pltpu.VMEM(pressure.shape, f32)] * 4,
            pltpu.SMEM((LABELS,), f32), pltpu.SMEM((LABELS,), f32),
            pltpu.SMEM((TAPS,), f32), pltpu.SMEM((4,), jnp.int32),
            *[pltpu.VMEM(t.shape, t.dtype) for t in (fy, gy, wx, ux, xt)],
            pltpu.VMEM((2, NY // 8, 8, XB), f32),
            pltpu.SemaphoreType.DMA((24,)),
            pltpu.SemaphoreType.DMA((24,)),
            pltpu.SemaphoreType.DMA((14,)),
        ],
        compiler_params=pltpu.CompilerParams(
            collective_id=0, has_side_effects=True, vmem_limit_bytes=STEP_BYTES
        ),
    )(
        *[
            hold(t)
            for t in (
                labels, pressure, velocity_x, velocity_y, velocity_z,
                speed_table, density_table, filter_taps, layer_width,
                jnp.asarray(fy), jnp.asarray(gy),
                jnp.asarray(wx), jnp.asarray(ux), jnp.asarray(xt),
            )
        ]
    )
    return pl.pallas_call(
        write_kernel,
        out_shape=(brick,) * 4,
        in_specs=[pl.BlockSpec(memory_space=pltpu.VMEM)] * 4,
        out_specs=(pl.BlockSpec(memory_space=pl.ANY),) * 4,
        scratch_shapes=[pltpu.SemaphoreType.DMA((4,))],
        compiler_params=pltpu.CompilerParams(vmem_limit_bytes=WRITE_BYTES),
    )(*results)


def solution(mesh):
    brick = P(None, "row", "col")
    return jax.shard_map(
        on_device,
        mesh=mesh,
        in_specs=(brick,) * 5 + (P(),) * 4,
        out_specs=(brick,) * 4,
        check_vma=False,
    )
```

```python
import functools
import math

import jax
import jax.numpy as jnp
import numpy as np
from jax import lax
from jax.experimental import pallas as pl
from jax.experimental.pallas import tpu as pltpu
from jax.sharding import PartitionSpec as P

time_step = 0.15
reference_speed = 2.0
absorption = 6.0
MESH = pl.DeviceIdType.MESH

NZ, NY, NX = 16, 512, 2048
ROWS, COLS = 16, 16
YB, XB = NY // ROWS, NX // COLS
SLOTS, HALO = 4, 16
CHUNK = 2 * COLS * SLOTS
STEP_BYTES, WRITE_BYTES = 40 << 20, 4 << 20
TAPS, LABELS = 33, 12
f32, bf16 = jnp.float32, jnp.bfloat16


def split_table(table):
    high = table.astype(np.float32).astype(bf16)
    low = (table - high.astype(np.float64)).astype(np.float32).astype(bf16)
    return np.stack([high, low])


def row_tables():
    slot = np.arange(NY // 2)
    y = np.arange(NY)
    angle = 2.0 * np.pi * ((slot[:, None] * y[None, :]) % NY) / NY
    real, imag = np.cos(angle), -np.sin(angle)
    imag[0] = np.where(y % 2 == 0, 1.0, -1.0)

    def order(a, b):
        pair = [t.reshape((2 * 2 * COLS, SLOTS) + t.shape[1:]) for t in (a, b)]
        return np.stack(pair, axis=1)

    forward = order(real, imag).reshape(NY, NY)
    weight = np.where(slot == 0, 1.0, 2.0)[:, None] / NY
    inverse = order(real * weight, imag * weight).reshape(NY, NY).T
    return split_table(forward), split_table(inverse)


def column_tables():
    x = np.arange(XB)
    angle = 2.0 * np.pi * ((x[:, None] * x[None, :]) % XB) / XB
    c, s = np.cos(angle), np.sin(angle)
    forward = np.block([[c, -s], [s, c]])
    inverse = np.block([[c, s], [-s, c]]) / NX
    kc = np.arange(COLS)
    twist = 2.0 * np.pi * (kc[:, None] * x[None, :]) / NX
    index = kc[:, None] + COLS * x[None, :]
    wave = 2.0 * np.pi * np.where(index < NX // 2, index, index - NX) / NX
    same = wave * np.sin(0.5 * wave)
    cross = wave * np.cos(0.5 * wave)
    small = np.stack([np.cos(twist), np.sin(twist), wave * wave, same, cross]).astype(np.float32)
    return split_table(forward), split_table(inverse), small


def scaled(value, factor):
    if abs(factor - 1.0) < 1e-12:
        return value
    if abs(factor + 1.0) < 1e-12:
        return -value
    return value * np.float32(factor)


def weighted(terms):
    total = None
    for value, factor in terms:
        if abs(factor) < 1e-12:
            continue
        if total is None:
            total = scaled(value, factor)
        elif abs(factor + 1.0) < 1e-12:
            total = total - value
        else:
            total = total + scaled(value, factor)
    return total


def cos16(n):
    return math.cos(2.0 * math.pi * (n % 16) / 16)


def sin16(n):
    return math.sin(2.0 * math.pi * (n % 16) / 16)


def depth_forward(p):
    even = [p[0]] + [p[n] + p[16 - n] for n in range(1, 8)] + [p[8]]
    odd = [None] + [p[n] - p[16 - n] for n in range(1, 8)]
    plus = [even[n] + even[8 - n] for n in range(4)] + [even[4]]
    minus = [even[n] - even[8 - n] for n in range(4)]
    odd_plus = [None] + [odd[n] + odd[8 - n] for n in range(1, 4)] + [odd[4]]
    odd_minus = [None] + [odd[n] - odd[8 - n] for n in range(1, 4)]

    def real_of(k):
        side = plus if k % 2 == 0 else minus
        return weighted([(side[n], cos16(k * n)) for n in range(len(side))])

    def imag_of(k):
        if k % 2 == 0:
            return weighted([(odd_minus[n], -sin16(k * n)) for n in range(1, 4)])
        return weighted([(odd_plus[n], -sin16(k * n)) for n in range(1, 5)])

    out = [real_of(0), real_of(8)]
    for k in range(1, 8):
        out += [real_of(k), imag_of(k)]
    return out


def depth_inverse(m):
    real = [m[0]] + [m[2 * k] for k in range(1, 8)] + [m[1]]
    imag = [None] + [m[2 * k + 1] for k in range(1, 8)]
    weight = [1.0 / 16] + [2.0 / 16] * 7 + [1.0 / 16]

    def terms(values, ids, n, wave):
        return weighted([(values[k], weight[k] * wave(k * n)) for k in ids])

    out = [None] * 16
    for n in range(0, 5):
        ce = terms(real, range(0, 9, 2), n, cos16)
        co = terms(real, range(1, 9, 2), n, cos16)
        so = terms(imag, range(1, 8, 2), n, lambda v: -sin16(v))
        se = terms(imag, range(2, 8, 2), n, lambda v: -sin16(v))
        near = ce if co is None else ce + co
        far = ce if co is None else ce - co
        if n == 0:
            out[0], out[8] = near, far
            continue
        if se is None:
            d_near, d_far = so, so
        else:
            d_near, d_far = so + se, so - se
        out[n], out[16 - n] = near + d_near, near - d_near
        if n < 4:
            out[8 - n], out[8 + n] = far + d_far, far - d_far
    return out


def depth_derivative(m, sign):
    out = [jnp.zeros_like(m[0]), m[1] * np.float32(-sign * math.pi)]
    for k in range(1, 8):
        wave = 2.0 * math.pi * k / 16
        a = np.float32(-sign * wave * math.sin(0.5 * wave))
        b = np.float32(wave * math.cos(0.5 * wave))
        out += [m[2 * k] * a - m[2 * k + 1] * b, m[2 * k + 1] * a + m[2 * k] * b]
    return out


def short_transform(values, sign):
    count = len(values)
    if count == 1:
        return values
    even = short_transform(values[0::2], sign)
    odd = short_transform(values[1::2], sign)
    out = [None] * count
    for k in range(count // 2):
        angle = sign * 2.0 * math.pi * k / count
        c, s = math.cos(angle), math.sin(angle)
        re, im = odd[k]
        if k == 0:
            tr, ti = re, im
        elif abs(c) < 1e-9:
            tr, ti = (-im, re) if s > 0 else (im, -re)
        elif abs(abs(c) - abs(s)) < 1e-9:
            h = np.float32(abs(c))
            cs, ss = (1 if c > 0 else -1), (1 if s > 0 else -1)
            first = re if cs > 0 else -re
            tr = (first - im if ss > 0 else first + im) * h
            second = im if cs > 0 else -im
            ti = (second + re if ss > 0 else second - re) * h
        else:
            tr = re * np.float32(c) - im * np.float32(s)
            ti = re * np.float32(s) + im * np.float32(c)
        er, ei = even[k]
        out[k] = (er + tr, ei + ti)
        out[k + count // 2] = (er - tr, ei - ti)
    return out


def halves(value):
    high = value.astype(bf16)
    low = (value - high.astype(f32)).astype(bf16)
    return high, low


def mm(a, b):
    return jnp.dot(a, b, preferred_element_type=f32)


def step_kernel(
    lab_hbm, p_hbm, vx_hbm, vy_hbm, vz_hbm, speed_hbm, density_hbm, taps_hbm, width_hbm,
    fy_hbm, gy_hbm, wx_hbm, ux_hbm, xt_hbm,
    po_ref, vxo_ref, vyo_ref, vzo_ref,
    row_out, row_in, col_out, col_in, bcol_out, bcol_in, brow_out, brow_in,
    kappa, xb, xs, coef, lab, edge_out, edge_in, raw, across, edge_band, down, damp,
    lab_ref, p_ref, vx_ref, vy_ref, vz_ref, speed_ref, density_ref, taps_ref, width_ref,
    fy_ref, gy_ref, wx_ref, ux_ref, xt_ref, yd_ref,
    send_sem, recv_sem, load_sem,
):
    def loaded(*numbers):
        for n in numbers:
            fetches[n].wait()

    r, c = lax.axis_index("row"), lax.axis_index("col")
    j, h = r // 2, r % 2
    q = h * COLS + c

    barrier = pltpu.get_barrier_semaphore()

    x_low, y_chip, core = r // 8, (r // 2) % 4, r % 2
    z_chip, x_high = c // 2, c % 2

    def pick(i, values):
        value = jnp.int32(values[0])
        for n in range(1, len(values)):
            value = jnp.where(i == n, jnp.int32(values[n]), value)
        return value

    def row_partner(i, other):
        x = (x_low + pick(i, (1, 0, 1, 1, 0, 0, 1, 0))) % 2
        y = (y_chip + pick(i, (2, 2, 1, 3, 1, 3, 0, 0))) % 4
        return (x * 4 + y) * 2 + (core + other) % 2

    def plane_partner(i, other):
        z = (z_chip + pick(i, (4, 3, 5, 4, 2, 6, 3, 5, 1, 7, 2, 6, 0, 1, 7, 0))) % 8
        x = (x_high + pick(i, (1, 1, 1, 0, 1, 1, 0, 0, 1, 1, 0, 0, 1, 0, 0, 0))) % 2
        return (core + other) % 2 * COLS + z * 2 + x

    def each_partner(partner, classes, body):
        def step(i, carry):
            body(partner(i, 0))
            body(partner(i, 1))
            return carry

        lax.fori_loop(0, classes - 1, step, 0)
        body(partner(classes - 1, 1))

    def row_device(t):
        return (t, c)

    def plane_device(t):
        return (2 * j + t // COLS, t % COLS)

    def greet(device):
        pl.semaphore_signal(barrier, inc=1, device_id=device, device_id_type=MESH)

    each_partner(plane_partner, COLS, lambda t: greet(plane_device(t)))
    each_partner(row_partner, ROWS // 2, lambda t: greet(row_device(t)))

    fetches = [
        pltpu.make_async_copy(source, target, load_sem.at[n])
        for n, (source, target) in enumerate(
            [
                (p_hbm, p_ref), (lab_hbm, lab_ref), (xt_hbm, xt_ref), (taps_hbm, taps_ref),
                (width_hbm, width_ref), (fy_hbm, fy_ref), (wx_hbm, wx_ref),
                (speed_hbm, speed_ref), (density_hbm, density_ref), (ux_hbm, ux_ref),
                (gy_hbm, gy_ref), (vx_hbm, vx_ref), (vy_hbm, vy_ref),
                (vz_hbm, vz_ref),
            ]
        )
    ]
    for fetch in fetches:
        fetch.start()
    def start_all(src, dst, sem, partner, classes, device_of, own):
        def start(t):
            pltpu.make_async_remote_copy(
                src_ref=src.at[t], dst_ref=dst.at[own], send_sem=send_sem.at[sem],
                recv_sem=recv_sem.at[sem], device_id=device_of(t), device_id_type=MESH,
            ).start()

        each_partner(partner, classes, start)
        dst[own] = src[own]

    def row_all(src, dst, sem):
        start_all(src, dst, sem, row_partner, ROWS // 2, row_device, r)

    def plane_all(src, dst, sem):
        start_all(src, dst, sem, plane_partner, COLS, plane_device, q)

    def whole(src, dst, sem, count):
        span = pl.ds(0, count - 1)
        return pltpu.make_async_remote_copy(
            src_ref=src.at[span], dst_ref=dst.at[span], send_sem=send_sem.at[sem],
            recv_sem=recv_sem.at[sem], device_id=((r + 1) % ROWS, c), device_id_type=MESH,
        )

    def send_row(f):
        row_all(row_out.at[f], row_in.at[f], f)

    def send_col(f, u):
        plane_all(col_out.at[f, u], col_in.at[f, u], 4 + 2 * f + u)

    def send_bcol(f, u):
        plane_all(bcol_out.at[f, u], bcol_in.at[f, u], 10 + 2 * f + u)

    def send_brow(f):
        row_all(brow_out.at[f], brow_in.at[f], 16 + f)

    def all_of(kind, f, u=None):
        if kind == "row":
            return whole(row_out.at[f], row_in.at[f], f, ROWS)
        if kind == "brow":
            return whole(brow_out.at[f], brow_in.at[f], 16 + f, ROWS)
        if kind == "col":
            return whole(col_out.at[f, u], col_in.at[f, u], 4 + 2 * f + u, 2 * COLS)
        return whole(bcol_out.at[f, u], bcol_in.at[f, u], 10 + 2 * f + u, 2 * COLS)

    def arrived(kind, f, u=None):
        all_of(kind, f, u).wait_recv()

    def load(ref, rows):
        return [ref[z, rows, :] for z in range(NZ)]

    def store(ref, rows, planes):
        for z in range(NZ):
            ref[z, rows, :] = planes[z]

    def chunks(body):
        def step(i, carry):
            body(pl.ds(pl.multiple_of(i * 8, 8), 8))
            return carry

        lax.fori_loop(0, YB // 8, step, 0)

    def pressure_planes(rows):
        store(row_out.at[0], rows, depth_forward(load(p_ref, rows)))

    loaded(0)
    chunks(pressure_planes)
    pl.semaphore_wait(barrier, ROWS - 1 + 2 * COLS - 1)
    send_row(0)

    loaded(1)
    for z in range(NZ):
        lab[z, HALO : HALO + YB, :] = lab_ref[z].astype(f32)

    def y_edges():
        before, after = (r + ROWS - 1) % ROWS, (r + 1) % ROWS
        return [
            pltpu.make_async_remote_copy(
                src_ref=lab.at[:, pl.ds(HALO, HALO), :],
                dst_ref=lab.at[:, pl.ds(HALO + YB, HALO), :],
                send_sem=send_sem.at[20], recv_sem=recv_sem.at[20],
                device_id=(before, c), device_id_type=MESH,
            ),
            pltpu.make_async_remote_copy(
                src_ref=lab.at[:, pl.ds(YB, HALO), :],
                dst_ref=lab.at[:, pl.ds(0, HALO), :],
                send_sem=send_sem.at[21], recv_sem=recv_sem.at[21],
                device_id=(after, c), device_id_type=MESH,
            ),
        ]

    def x_edges():
        before, after = (c + COLS - 1) % COLS, (c + 1) % COLS
        return [
            pltpu.make_async_remote_copy(
                src_ref=edge_out.at[0], dst_ref=edge_in.at[1],
                send_sem=send_sem.at[22], recv_sem=recv_sem.at[22],
                device_id=(r, before), device_id_type=MESH,
            ),
            pltpu.make_async_remote_copy(
                src_ref=edge_out.at[1], dst_ref=edge_in.at[0],
                send_sem=send_sem.at[23], recv_sem=recv_sem.at[23],
                device_id=(r, after), device_id_type=MESH,
            ),
        ]

    def ids(shape, dim):
        return lax.broadcasted_iota(jnp.int32, shape, dim)

    def banded(offset):
        def tap(t, total):
            return jnp.where(offset == t, taps_ref[t], total)

        return lax.fori_loop(0, TAPS, tap, jnp.zeros(offset.shape, f32), unroll=3)

    def fill_bands():
        wide = (XB, XB)
        band = banded(ids(wide, 0) - ids(wide, 1) + HALO)
        none = jnp.zeros(wide, bf16)
        for part, value in enumerate(halves(band)):
            top_rows = jnp.concatenate([value, none], axis=1)
            low_rows = jnp.concatenate([none, value], axis=1)
            across[part] = jnp.concatenate([top_rows, low_rows], axis=0)
        edge_band[0] = banded(ids(wide, 0) % HALO - ids(wide, 1))
        edge_band[1] = banded(ids(wide, 0) % HALO - ids(wide, 1) + XB + HALO)
        tall = (4 * YB, 8 * YB)
        row, line = ids(tall, 0), ids(tall, 1)
        offset = jnp.where(row // YB == line // (2 * YB), line % (2 * YB) - row % YB, -1)
        for part, value in enumerate(halves(banded(offset))):
            down[part] = value

    def fill_damping():
        def absorb(position, length, low_width, high_width):
            size = position.shape
            low_side = jnp.maximum(low_width - position, 0).astype(f32)
            high_side = jnp.maximum(position - (length - 1 - high_width), 0).astype(f32)
            low_side = low_side / jnp.full(size, low_width, jnp.int32).astype(f32)
            high_side = high_side / jnp.full(size, high_width, jnp.int32).astype(f32)
            low_side, high_side = low_side * low_side, high_side * high_side
            total = low_side * low_side + high_side * high_side
            return jnp.exp((-0.5 * time_step * absorption * reference_speed) * total)

        damp[0:8] = absorb(c * XB + ids((8, XB), 1), NX, width_ref[0], width_ref[1])
        damp[8:] = absorb(r * YB + ids((YB, XB), 0), NY, width_ref[2], width_ref[3])

    def pack_edges():
        wide = (XB, XB)
        source, target = ids(wide, 0), ids(wide, 1)
        total = None
        for g in range(8):
            here = target // HALO == g
            first_lanes = here & (source == target % HALO)
            last_lanes = here & (source == target % HALO + XB - HALO)
            select = jnp.concatenate(
                [jnp.where(first_lanes, 1.0, 0.0), jnp.where(last_lanes, 1.0, 0.0)], axis=1
            ).astype(bf16)
            part = mm(lab[2 * g : 2 * g + 2].reshape(XB, XB).astype(bf16), select)
            total = part if total is None else total + part
        edge_out[0] = total[:, :XB]
        edge_out[1] = total[:, XB:]

    def tables():
        density = [jnp.full((8, XB), density_ref[n], f32) for n in range(LABELS)]
        speed = [jnp.full((8, XB), speed_ref[n], f32) for n in range(LABELS)]
        return [1.0 / d for d in density], [d * s * s for d, s in zip(density, speed)]

    def look_up(label, table):
        value = jnp.broadcast_to(table[0][None], label.shape)
        for n in range(1, LABELS):
            value = jnp.where(label == float(n), table[n][None], value)
        return value

    def fill_raw():
        buoyancy_of, modulus_of = tables()

        def plane(z, carry):
            label = lab[z].reshape(8, 8, XB)
            rows = pl.ds(pl.multiple_of(z * 2 * YB, 2 * YB), 2 * YB)
            raw[rows, :XB] = look_up(label, buoyancy_of).reshape(2 * YB, XB)
            raw[rows, XB:] = look_up(label, modulus_of).reshape(2 * YB, XB)
            return carry

        lax.fori_loop(0, NZ, plane, 0)

    def smooth():
        buoyancy_of, modulus_of = tables()
        edges = [edge_in[0].reshape(16, 8, XB), edge_in[1].reshape(16, 8, XB)]
        sides = [
            halves(jnp.concatenate([look_up(e, t).reshape(XB, XB) for e in edges], axis=1))
            for t in (buoyancy_of, modulus_of)
        ]
        group_of = ids((XB, XB), 0) // HALO

        def quarter(i, carry):
            rows = pl.ds(pl.multiple_of(i * 8 * YB, 8 * YB), 8 * YB)
            high, low_part = halves(raw[rows, :])
            main = mm(high, across[0]) + mm(low_part, across[0]) + mm(high, across[1])
            parts = []
            for g in range(2):
                inside = group_of == 2 * i + g
                parts.append(
                    jnp.concatenate(
                        [jnp.where(inside, edge_band[s], 0.0) for s in range(2)], axis=0
                    )
                )
            high, low_part = halves(jnp.concatenate(parts, axis=1))
            columns = []
            for side_high, side_low in sides:
                out = mm(side_high, high) + mm(side_low, high) + mm(side_high, low_part)
                columns.append(jnp.concatenate([out[:, :XB], out[:, XB:]], axis=0))
            high, low_part = halves(main + jnp.concatenate(columns, axis=1))
            out = mm(down[0], high) + mm(down[0], low_part) + mm(down[1], high)
            planes = pl.ds(i * 4, 4)
            coef[0, planes] = out[:, :XB].reshape(4, YB, XB)
            coef[1, planes] = out[:, XB:].reshape(4, YB, XB)
            return carry

        lax.fori_loop(0, 4, quarter, 0)

    tile_rows = lax.broadcasted_iota(jnp.int32, (8, XB), 0)
    one, zero = jnp.ones((8, XB), f32), jnp.zeros((8, XB), f32)
    top = jnp.where(tile_rows < SLOTS, one, zero)
    bottom = 1.0 - top
    flat = jnp.where(jnp.full((8, XB), j, jnp.int32) == 0, one, zero)
    deep = 1.0 - flat

    def slot_of(u):
        return u * CHUNK + q * SLOTS + tile_rows % SLOTS

    def first_of(u):
        return jnp.where(slot_of(u) == 0, one, zero)

    def turned(value):
        return pltpu.roll(value, SLOTS, 0)

    pi2 = np.float32(math.pi * math.pi)
    kz = jnp.full((8, XB), j, jnp.int32).astype(f32) * np.float32(2.0 * math.pi / NZ)

    def square_of(u):
        ky = slot_of(u).astype(f32) * np.float32(2.0 * math.pi / NY)
        return ky * ky + kz * kz + pi2 * bottom * (first_of(u) * deep + flat)

    squares = (square_of(0), pi2 + pi2 * bottom, square_of(1))
    scale = np.float32((0.5 * reference_speed * time_step) ** 2)

    def fill_kappa(kc, carry):
        kx2 = xt_ref[2, pl.ds(kc, 1), :]
        for g, part in enumerate(squares):
            v2 = scale * (kx2 + part)
            series = 1.0 + v2 * np.float32(-1.0 / 110.0)
            series = 1.0 + v2 * np.float32(-1.0 / 72.0) * series
            series = 1.0 + v2 * np.float32(-1.0 / 42.0) * series
            series = 1.0 + v2 * np.float32(-1.0 / 20.0) * series
            kappa[g, kc] = 1.0 + v2 * np.float32(-1.0 / 6.0) * series
        return carry

    loaded(2)
    lax.fori_loop(0, COLS, fill_kappa, 0)

    for edge in y_edges():
        edge.start()
    loaded(3, 4)
    fill_bands()
    fill_damping()

    def lines(ref, f):
        return ref[f].reshape(NY, XB)

    def put_col(f, values, add=None):
        span = NY // 2
        for u in range(2):
            rows = slice(u * span, (u + 1) * span)
            out = row_product(fy_ref[:, rows, :], [values])[0]
            if add is not None:
                out = out + add[rows]
            col_out[f, u] = out.reshape(2 * COLS, 2 * SLOTS, XB)
            send_col(f, u)

    def row_product(table, values):
        parts = [halves(v) for v in values]
        high = [part[0] for part in parts]
        low_part = [part[1] for part in parts]
        if len(values) == 1:
            both = mm(table[0], jnp.concatenate([high[0], low_part[0]], axis=1))
            return [both[:, :XB] + both[:, XB:] + mm(table[1], high[0])]
        high = jnp.concatenate(high, axis=1)
        low_part = jnp.concatenate(low_part, axis=1)
        result = mm(table[0], high) + mm(table[0], low_part) + mm(table[1], high)
        return [result[:, :XB], result[:, XB:]]

    def fill_slopes(n, carry):
        slots = n * SLOTS + tile_rows % SLOTS
        angle = slots.astype(f32) * np.float32(math.pi / NY)
        square = angle * angle
        sine, cosine = one, one
        for k in range(6, 0, -1):
            sine = 1.0 - square * np.float32(1.0 / (2 * k * (2 * k + 1))) * sine
        for k in range(7, 0, -1):
            cosine = 1.0 - square * np.float32(1.0 / (2 * k * (2 * k - 1))) * cosine
        same = -2.0 * square * sine
        edge = jnp.where(slots == 0, bottom * np.float32(math.pi), zero)
        yd_ref[0, n] = same - edge
        yd_ref[1, n] = 2.0 * angle * cosine * (bottom - top)
        return carry

    def y_derivative(value, sign):
        tiles = value.reshape(NY // 8, 8, XB)
        same = tiles * yd_ref[0]
        cross = pltpu.roll(tiles, SLOTS, 1) * yd_ref[1]
        return (cross + same if sign > 0 else cross - same).reshape(NY, XB)

    def x_forward(f, u):
        first, groups = first_of(u), 2 - u
        general = (1.0 - first) * deep
        rest = (1.0 - first) * flat
        lone = first * deep
        re_r, re_turned_r = top + bottom * lone, bottom * general
        re_i, re_turned_i = bottom * general, bottom * flat - top * general
        im_r, im_turned_r = -bottom * general, top * (general + rest)
        im_i, im_turned_i = top * general + lone + bottom * rest, bottom * general
        for n in range(COLS):
            tr, ti = col_in[f, u, n], col_in[f, u, COLS + n]
            rr, ri = turned(tr), turned(ti)
            xb[0, 0, n] = re_r * tr + re_turned_r * rr + re_i * ti + re_turned_i * ri
            xb[0, 1, n] = im_r * tr + im_turned_r * rr + im_i * ti + im_turned_i * ri
            if u == 0:
                xb[1, 0, n] = first * flat * (top * rr + bottom * ti)
                xb[1, 1, n] = zero

        def group(g, carry):
            values = [(xb[g, 0, n], xb[g, 1, n]) for n in range(COLS)]
            values = short_transform(values, -1.0)
            for kc in range(COLS):
                re, im = values[kc]
                cs, sn = xt_ref[0, kc : kc + 1, :], xt_ref[1, kc : kc + 1, :]
                xs[g, kc, :, :XB] = re * cs + im * sn
                xs[g, kc, :, XB:] = im * cs - re * sn
            return carry

        lax.fori_loop(0, groups, group, 0)
        high, low_part = halves(xs[:groups].reshape(groups * COLS * 8, 2 * XB))
        out = mm(high, wx_ref[0]) + mm(low_part, wx_ref[0]) + mm(high, wx_ref[1])
        return out.reshape(groups, COLS, 8, 2 * XB)

    def kappa_of(u):
        return kappa[0:2] if u == 0 else kappa[2:3]

    def x_derivative(re, im, sign):
        same = xt_ref[3][None, :, None, :]
        cross = xt_ref[4][None, :, None, :]
        if sign > 0:
            return -(re * same + im * cross), re * cross - im * same
        return re * same - im * cross, im * same + re * cross

    def x_inverse(value, f, u):
        first, groups = first_of(u), 2 - u
        high, low_part = halves(value.reshape(groups * COLS * 8, 2 * XB))
        out = mm(high, ux_ref[0]) + mm(low_part, ux_ref[0]) + mm(high, ux_ref[1])
        xs[:groups] = out.reshape(groups, COLS, 8, 2 * XB)

        def group(g, carry):
            values = []
            for kc in range(COLS):
                re, im = xs[g, kc, :, :XB], xs[g, kc, :, XB:]
                cs, sn = xt_ref[0, kc : kc + 1, :], xt_ref[1, kc : kc + 1, :]
                values.append((re * cs - im * sn, im * cs + re * sn))
            values = short_transform(values, 1.0)
            for n in range(COLS):
                xb[g, 0, n] = values[n][0]
                xb[g, 1, n] = values[n][1]
            return carry

        lax.fori_loop(0, groups, group, 0)
        half = 0.5 * (1.0 - first) * deep
        rest = (1.0 - first) * flat
        lone = first * deep
        r_re = top * half + top * flat + lone
        r_re_turned = top * half
        r_im, r_im_turned = -bottom * half, bottom * (half + rest)
        i_re, i_re_turned = bottom * half, top * flat - bottom * half
        i_im, i_im_turned = top * half + lone + bottom * rest, top * half
        for n in range(COLS):
            vr, vi = xb[0, 0, n], xb[0, 1, n]
            wr, wi = turned(vr), turned(vi)
            out_r = r_re * vr + r_re_turned * wr + r_im * vi + r_im_turned * wi
            out_i = i_re * vr + i_re_turned * wr + i_im * vi + i_im_turned * wi
            if u == 0:
                extra = first * flat * bottom
                out_r = out_r + extra * turned(xb[1, 0, n])
                out_i = out_i + extra * xb[1, 0, n]
            bcol_out[f, u, n] = out_r
            bcol_out[f, u, COLS + n] = out_i

    loaded(5)
    arrived("row", 0)
    put_col(0, lines(row_in, 0))

    for edge in y_edges():
        edge.wait_recv()
    pack_edges()
    for edge in x_edges():
        edge.start()
    loaded(7, 8)
    fill_raw()
    lax.fori_loop(0, NY // 8, fill_slopes, 0)

    loaded(6, 9)
    for u in range(2):
        arrived("col", 0, u)
        spectrum = x_forward(0, u)
        re, im = spectrum[..., :XB] * kappa_of(u), spectrum[..., XB:] * kappa_of(u)
        x_inverse(jnp.concatenate([re, im], axis=-1), 1, u)
        send_bcol(1, u)
        if u == 1:
            send_bcol(0, 0)
        dre, dim = x_derivative(re, im, 1)
        x_inverse(jnp.concatenate([dre, dim], axis=-1), 0, u)
    send_bcol(0, 1)

    for edge in x_edges():
        edge.wait_recv()
    smooth()
    loaded(10, 11, 12, 13)

    dx = damp[0:8]

    def rows_of_y(rows):
        return damp[pl.ds(pl.multiple_of(rows.start + 8, 8), 8), :]

    def update_x(rows):
        grad = depth_inverse(load(brow_in.at[0], rows))
        fresh = []
        for z in range(NZ):
            change = time_step * coef[0, z, rows, :] * grad[z]
            fresh.append(dx * (dx * vx_ref[z, rows, :] - change))
        store(vxo_ref, rows, fresh)
        store(row_out.at[1], rows, depth_forward(fresh))

    def update_y(rows):
        grad = depth_inverse(load(brow_in.at[1], rows))
        dy = rows_of_y(rows)
        fresh = []
        for z in range(NZ):
            change = time_step * coef[0, z, rows, :] * grad[z]
            fresh.append(dy * (dy * vy_ref[z, rows, :] - change))
        store(vyo_ref, rows, fresh)
        store(row_out.at[2], rows, depth_forward(fresh))

    def update_z(rows):
        grad = depth_inverse(depth_derivative(load(brow_in.at[2], rows), 1))
        fresh = []
        for z in range(NZ):
            fresh.append(vz_ref[z, rows, :] - time_step * coef[0, z, rows, :] * grad[z])
        store(vzo_ref, rows, fresh)
        store(row_out.at[3], rows, depth_derivative(depth_forward(fresh), -1))

    arrived("bcol", 1, 0)
    arrived("bcol", 1, 1)
    flow = lines(bcol_in, 1)
    plain, slope = row_product(gy_ref, [flow, y_derivative(flow, 1)])
    brow_out[1] = slope.reshape(ROWS, YB, XB)
    send_brow(1)
    brow_out[2] = plain.reshape(ROWS, YB, XB)
    send_brow(2)

    arrived("bcol", 0, 0)
    arrived("bcol", 0, 1)
    brow_out[0] = row_product(gy_ref, [lines(bcol_in, 0)])[0].reshape(ROWS, YB, XB)
    send_brow(0)

    arrived("brow", 1)
    chunks(update_y)
    send_row(2)
    arrived("brow", 2)
    chunks(update_z)
    send_row(3)
    arrived("brow", 0)
    chunks(update_x)
    send_row(1)

    arrived("row", 2)
    aside = y_derivative(row_product(fy_ref, [lines(row_in, 2)])[0], -1)
    arrived("row", 3)
    put_col(2, lines(row_in, 3), aside)
    arrived("row", 1)
    put_col(1, lines(row_in, 1))

    remains = []
    for u in range(2):
        arrived("col", 2, u)
        remains.append(x_forward(2, u))
    for u in range(2):
        arrived("col", 1, u)
        flow_x = x_forward(1, u)
        tre, tim = x_derivative(flow_x[..., :XB], flow_x[..., XB:], -1)
        tre = (tre + remains[u][..., :XB]) * kappa_of(u)
        tim = (tim + remains[u][..., XB:]) * kappa_of(u)
        x_inverse(jnp.concatenate([tre, tim], axis=-1), 2, u)
        send_bcol(2, u)

    arrived("bcol", 2, 0)
    arrived("bcol", 2, 1)
    brow_out[3] = row_product(gy_ref, [lines(bcol_in, 2)])[0].reshape(ROWS, YB, XB)
    send_brow(3)

    arrived("brow", 3)

    def update_p(rows):
        divergence = depth_inverse(load(brow_in.at[3], rows))
        both = dx * damp[pl.ds(pl.multiple_of(rows.start + 8, 8), 8), :]
        for z in range(NZ):
            change = time_step * coef[1, z, rows, :] * divergence[z]
            po_ref[z, rows, :] = both * (both * p_ref[z, rows, :] - change)

    chunks(update_p)

    for f in range(4):
        all_of("row", f).wait_send()
        all_of("brow", f).wait_send()
    for f in range(3):
        for u in range(2):
            all_of("col", f, u).wait_send()
            all_of("bcol", f, u).wait_send()
    for edge in y_edges() + x_edges():
        edge.wait_send()


def write_kernel(a, b, c, d, a_out, b_out, c_out, d_out, sem):
    pairs = ((a, a_out), (b, b_out), (c, c_out), (d, d_out))
    copies = [pltpu.make_async_copy(x, y, sem.at[n]) for n, (x, y) in enumerate(pairs)]
    for copy in copies:
        copy.start()
    for copy in copies:
        copy.wait()


def on_device(
    labels, pressure, velocity_x, velocity_y, velocity_z,
    speed_table, density_table, filter_taps, layer_width,
):
    fy, gy = row_tables()
    wx, ux, xt = column_tables()
    brick = jax.ShapeDtypeStruct(pressure.shape, f32)
    row_buffer = lambda n: pltpu.VMEM((n, ROWS, YB, XB), f32)
    col_buffer = lambda n: pltpu.VMEM((n, 2, 2 * COLS, 2 * SLOTS, XB), f32)
    hold = lambda t: pltpu.with_memory_space_constraint(t, pltpu.HBM)
    results = pl.pallas_call(
        step_kernel,
        out_shape=(brick,) * 4,
        in_specs=[pl.BlockSpec(memory_space=pl.ANY)] * 14,
        out_specs=(pl.BlockSpec(memory_space=pltpu.VMEM),) * 4,
        scratch_shapes=[
            row_buffer(4), row_buffer(4), col_buffer(3), col_buffer(3),
            col_buffer(3), col_buffer(3), row_buffer(4), row_buffer(4),
            pltpu.VMEM((3, COLS, 8, XB), f32),
            pltpu.VMEM((2, 2, COLS, 8, XB), f32),
            pltpu.VMEM((2, COLS, 8, 2 * XB), f32),
            pltpu.VMEM((2, NZ, YB, XB), f32),
            pltpu.VMEM((NZ, 2 * YB, XB), f32),
            pltpu.VMEM((2, XB, XB), f32),
            pltpu.VMEM((2, XB, XB), f32),
            pltpu.VMEM((NZ * 2 * YB, 2 * XB), f32),
            pltpu.VMEM((2, 2 * XB, 2 * XB), bf16),
            pltpu.VMEM((2, XB, XB), f32),
            pltpu.VMEM((2, 4 * YB, 8 * YB), bf16),
            pltpu.VMEM((8 + YB, XB), f32),
            pltpu.VMEM(labels.shape, jnp.int32),
            *[pltpu.VMEM(pressure.shape, f32)] * 4,
            pltpu.SMEM((LABELS,), f32), pltpu.SMEM((LABELS,), f32),
            pltpu.SMEM((TAPS,), f32), pltpu.SMEM((4,), jnp.int32),
            *[pltpu.VMEM(t.shape, t.dtype) for t in (fy, gy, wx, ux, xt)],
            pltpu.VMEM((2, NY // 8, 8, XB), f32),
            pltpu.SemaphoreType.DMA((24,)),
            pltpu.SemaphoreType.DMA((24,)),
            pltpu.SemaphoreType.DMA((14,)),
        ],
        compiler_params=pltpu.CompilerParams(
            collective_id=0, has_side_effects=True, vmem_limit_bytes=STEP_BYTES
        ),
    )(
        *[
            hold(t)
            for t in (
                labels, pressure, velocity_x, velocity_y, velocity_z,
                speed_table, density_table, filter_taps, layer_width,
                jnp.asarray(fy), jnp.asarray(gy),
                jnp.asarray(wx), jnp.asarray(ux), jnp.asarray(xt),
            )
        ]
    )
    return pl.pallas_call(
        write_kernel,
        out_shape=(brick,) * 4,
        in_specs=[pl.BlockSpec(memory_space=pltpu.VMEM)] * 4,
        out_specs=(pl.BlockSpec(memory_space=pl.ANY),) * 4,
        scratch_shapes=[pltpu.SemaphoreType.DMA((4,))],
        compiler_params=pltpu.CompilerParams(vmem_limit_bytes=WRITE_BYTES),
    )(*results)


def solution(mesh):
    brick = P(None, "row", "col")
    return jax.shard_map(
        on_device,
        mesh=mesh,
        in_specs=(brick,) * 5 + (P(),) * 4,
        out_specs=(brick,) * 4,
        check_vma=False,
    )
```
